128 devices in a mesh: gx: 8 (over y, core), gy: 4 (over z), gz: 4 (over x).
Axes of the slice: x: 4, y: 4, z: 4, core: 2. Of those that a mesh axis runs over, the one named last changes fastest.
Arguments:
- kappa_sq: float32 [128, 64, 512], P('gx', 'gz', 'gy'), may hold values from 0.004 to 0.4
- probe_bits: int32 [4, 128, 64, 512], P(None, 'gx', 'gz', 'gy'), may hold values from 0 to 1
Outputs:
- solution: float32 [4, 128, 64, 512], P(None, 'gx', 'gz', 'gy')
- relative_residual: float32 [4], replicated
The draws below stay inside these ranges and needn't reach their ends.
All inputs are finite; a program needn't handle non-finite values.
Results may differ from the reference program's by a relative error of at most 0.0001.
Values sent between devices are 32-bit elements; how exact they have to be, the bound alone decides.
A program may use at most 128 MiB of HBM per device.

```python
import math
import jax
import jax.numpy as jnp
from jax import lax

PROBES = 4
LEVELS = 3
COARSE_SWEEPS = 8
ITERS = 2
NX = 128
NZ = 64
NY = 512


def place_ends(array, own_key, smallest, top_value):
    place = [jax.random.randint(jax.random.fold_in(own_key, axis), (), 0, length) for axis, length in enumerate(array.shape)]
    main_axis = array.shape.index(max(array.shape))
    beside = place[:main_axis] + [(place[main_axis] + 1) % array.shape[main_axis]] + place[main_axis + 1:]
    return array.at[tuple(place)].set(smallest).at[tuple(beside)].set(top_value)


def shard_levels(stream_key, dims, cuts, low, high):
    def one(dim, shards_of):
        draws = jax.random.uniform(jax.random.fold_in(jax.random.fold_in(stream_key, 6), dim), (shards_of,), jnp.float32, low / len(cuts), high / len(cuts))
        return jnp.repeat(jnp.exp(draws), dims[dim] // shards_of).reshape((-1,) + (1,) * (len(dims) - dim - 1))

    level = one(*cuts[0])
    for cut in cuts[1:]:
        level = level * one(*cut)
    return level


def setup_inputs(seed: int = 0) -> dict:
    arg_keys = jax.random.split(jax.random.key(seed), 3)
    kappa_sq = jnp.clip(jnp.exp(math.log(0.4) - 4.6051702 * jax.random.uniform(arg_keys[0], (NX, NZ, NY), jnp.float32) ** shard_levels(arg_keys[0], (NX, NZ, NY), ((0, 8), (1, 4), (2, 4)), -0.2, 0.2)), 0.004, 0.4)
    probe_bits = place_ends(jax.random.randint(arg_keys[1], (PROBES, NX, NZ, NY), 0, 2), jax.random.fold_in(arg_keys[1], 1), 0, 1).astype(jnp.int32)
    return {"kappa_sq": kappa_sq, "probe_bits": probe_bits}


damping = 0.8

def neighbours(padded):
    along_first = padded[..., 2:, 1:-1, 1:-1] + padded[..., :-2, 1:-1, 1:-1]
    along_second = padded[..., 1:-1, 2:, 1:-1] + padded[..., 1:-1, :-2, 1:-1]
    along_third = padded[..., 1:-1, 1:-1, 2:] + padded[..., 1:-1, 1:-1, :-2]
    return along_first + along_second + along_third

def coarsen(field):
    leading = field.shape[:-3]
    cells_first, cells_second, cells_third = field.shape[-3:]
    grouped = field.reshape(leading + (cells_first // 2, 2, cells_second // 2, 2, cells_third // 2, 2))
    return lax.optimization_barrier(jnp.mean(grouped, axis=(-5, -3, -1)))

def refine(field):
    leading = field.shape[:-3]
    cells_first, cells_second, cells_third = field.shape[-3:]
    spread = field.reshape(leading + (cells_first, 1, cells_second, 1, cells_third, 1))
    spread = jnp.broadcast_to(spread, leading + (cells_first, 2, cells_second, 2, cells_third, 2))
    return spread.reshape(leading + (cells_first * 2, cells_second * 2, cells_third * 2))

def reference(kappa_sq, probe_bits):
    diagonals = []
    couplings = []
    coef_field = kappa_sq
    for grid_level in range(LEVELS + 1):
        if grid_level > 0:
            coef_field = coarsen(coef_field)
        coupling = 0.25 ** grid_level
        diagonals.append(coef_field + 6.0 * coupling)
        couplings.append(coupling)

    def operate(field, grid_level):
        return diagonals[grid_level] * field - couplings[grid_level] * neighbours(jnp.pad(field, 1))

    def jacobi_sweep(field, rhs_field, grid_level):
        return field + damping * (rhs_field - operate(field, grid_level)) / diagonals[grid_level]

    def vcycle(rhs_field, grid_level):
        field = damping * rhs_field / diagonals[grid_level]
        if grid_level == LEVELS:
            for sweep_index in range(COARSE_SWEEPS - 1):
                field = jacobi_sweep(field, rhs_field, grid_level)
            return field
        field = jacobi_sweep(field, rhs_field, grid_level)
        remainder = rhs_field - operate(field, grid_level)
        field = field + refine(vcycle(coarsen(remainder), grid_level + 1))
        field = jacobi_sweep(field, rhs_field, grid_level)
        return jacobi_sweep(field, rhs_field, grid_level)

    def solve_one(sign_bits):
        right_side = 2.0 * sign_bits.astype(jnp.float32) - 1.0
        solution = jnp.zeros_like(right_side)
        residual = right_side
        precond = vcycle(residual, 0)
        precond_dot = jnp.sum(residual * precond)
        search = precond
        for iteration in range(ITERS):
            operated = operate(search, 0)
            step_size = precond_dot / jnp.sum(search * operated)
            solution = solution + step_size * search
            residual = residual - step_size * operated
            if iteration + 1 < ITERS:
                precond = vcycle(residual, 0)
                next_dot = jnp.sum(residual * precond)
                search = precond + next_dot / precond_dot * search
                precond_dot = next_dot
        return (solution, jnp.sum(residual * residual))
    solution, squares = lax.map(solve_one, probe_bits)
    cell_total = probe_bits.shape[1] * probe_bits.shape[2] * probe_bits.shape[3]
    return (solution, jnp.sqrt(squares / cell_total))
```

```python
import functools

import jax
import jax.numpy as jnp
from jax import lax
from jax.experimental import pallas as pl
from jax.experimental.pallas import tpu as pltpu
from jax.sharding import PartitionSpec as P

LEVELS = 3
COARSE_SWEEPS = 8
PROBES = 4
LANES = 128
HALF = 4
MESH = pl.DeviceIdType.MESH
F32 = jnp.float32
HIGHEST = lax.Precision.HIGHEST


def lanes_of(shape):
    return lax.broadcasted_iota(jnp.int32, shape, len(shape) - 1)


def rows_of(shape):
    return lax.broadcasted_iota(jnp.int32, shape, len(shape) - 2)


def turn(value, shift):
    return pltpu.roll(value, shift, len(value.shape) - 1)


def swap_halves(value):
    return pltpu.roll(value, HALF, len(value.shape) - 2)


def kernel_body(
    sizes,
    counts,
    cells,
    kappa_ref,
    bits_ref,
    solution_ref,
    norm_ref,
    *scratch,
):
    names = scratch_names()
    s = dict(zip(names, scratch))
    axes = ("gx", "gz", "gy")
    me = {a: lax.axis_index(a) for a in axes}

    barrier = pltpu.get_barrier_semaphore()
    greeted = 0
    for a in axes:
        for o in range(1, counts[a]):
            pl.semaphore_signal(
                barrier, inc=1, device_id={a: lax.rem(me[a] + o, counts[a])}, device_id_type=MESH
            )
            greeted += 1

    def loop(count, body, init=0, unroll=1):
        return lax.fori_loop(0, count, body, init, unroll=unroll)

    def load_x(x, carry):
        for p in range(PROBES):
            for h in range(2):
                row = h * PROBES + p
                s["flip"][x, pl.ds(row, 8, stride=8), :] = (
                    2.0 * bits_ref[p, x, pl.ds(8 * h, 8), :].astype(F32) - 1.0
                )
        return carry

    loop(16, load_x)

    def take_x(x, carry):
        s["b0"][x] = s["flip"][x].reshape(8, 8, LANES)
        return carry

    loop(16, take_x)

    def kappa_x(x, carry):
        for p in range(PROBES):
            for h in range(2):
                row = h * PROBES + p
                s["flip"][x, pl.ds(row, 8, stride=8), :] = kappa_ref[x, pl.ds(8 * h, 8), :]
        return carry

    loop(16, kappa_x)

    def diag_x(x, carry):
        diag = s["flip"][x].reshape(8, 8, LANES)
        s["d0"][x] = diag + 6.0
        s["w0"][x] = 0.8 / (diag + 6.0)
        return carry

    loop(16, diag_x)

    def coarse_of(field, level):
        xs, zs = field.shape[0] // 2, field.shape[1] // 2
        split = field.reshape(xs, 2, zs, 2, 8, LANES)
        total = (split[:, 0, :, 0] + split[:, 0, :, 1]) + (split[:, 1, :, 0] + split[:, 1, :, 1])
        width = 2**level
        odd = (lanes_of(total.shape) // width) % 2 == 1
        other = jnp.where(odd, turn(total, width), turn(total, LANES - width))
        return 0.125 * (total + other)

    def kappa_coarse(x, carry):
        a = s["flip"][2 * x].reshape(8, 8, LANES)
        b = s["flip"][2 * x + 1].reshape(8, 8, LANES)
        s["e1"][x] = coarse_of(jnp.stack([a, b]), 0)[0]
        return carry

    loop(8, kappa_coarse)
    for level in (1, 2, 3):
        kappa_l = s[f"e{level}"][...]
        s[f"d{level}"][...] = kappa_l + 6.0 * 0.25**level
        s[f"w{level}"][...] = 0.8 / (kappa_l + 6.0 * 0.25**level)
        if level < 3:
            s[f"e{level + 1}"][...] = coarse_of(kappa_l, level)

    for name in names:
        if name[0] in "vr" and name[1] in "0123":
            ref = s[name]
            if name[0] == "v":

                def clear(x, carry, ref=ref):
                    ref[x] = jnp.zeros(ref.shape[1:], F32)
                    return carry

                loop(ref.shape[0], clear)
            else:
                ref[...] = jnp.zeros(ref.shape, F32)
    s["gva"][...] = jnp.zeros(s["gva"].shape, F32)
    s["gvb"][...] = jnp.zeros(s["gvb"].shape, F32)

    pl.semaphore_wait(barrier, greeted)

    def neighbour(a, step):
        return {a: me[a] + step}

    def exchange(level, which):
        xs, zs = sizes[level]
        v = s[f"v{level}{which}"]
        near = s[f"r{level}{which}"]
        pack = s[f"p{level}{which}"]
        yin = s[f"r{level}{which}y"]
        yout = s[f"p{level}{which}y"]
        half = xs // 2
        slot = "abc".index(which)

        first = v[pl.ds(1, xs), 1]
        last = v[pl.ds(1, xs), zs]
        low_rows = rows_of((half, 8, LANES)) < HALF
        pack[0] = jnp.where(low_rows, first[:half], swap_halves(first[half:]))
        pack[1] = jnp.where(low_rows, swap_halves(last[:half]), last[half:])

        def copy(n, src, dst, to):
            return pltpu.make_async_remote_copy(
                src_ref=src,
                dst_ref=dst,
                send_sem=s["send"].at[slot, n],
                recv_sem=s["recv"].at[slot, n],
                device_id=to,
                device_id_type=MESH,
            )

        inner = pl.ds(1, zs)
        plan = []
        for n, (a, step, src, dst) in enumerate(
            (
                ("gz", -1, pack.at[0], near.at[1]),
                ("gz", 1, pack.at[1], near.at[0]),
                ("gx", -1, v.at[1, inner], v.at[xs + 1, inner]),
                ("gx", 1, v.at[xs, inner], v.at[0, inner]),
                ("gy", -1, yout.at[0], yin.at[1]),
                ("gy", 1, yout.at[1], yin.at[0]),
            )
        ):
            there = me[a] > 0 if step < 0 else me[a] < counts[a] - 1
            back = me[a] < counts[a] - 1 if step < 0 else me[a] > 0
            plan.append((there, back, copy(n, src, dst, neighbour(a, step))))
        for there, _, c in plan:
            pl.when(there)(c.start)
        for there, back, c in plan:
            pl.when(back)(c.wait_recv)
        for there, back, c in plan:
            pl.when(there)(c.wait_send)
        low, high = near[0], near[1]
        v[pl.ds(1, half), 0] = jnp.where(low_rows, low, swap_halves(last[:half]))
        v[pl.ds(1 + half, half), 0] = swap_halves(jnp.where(low_rows, last[half:], low))
        v[pl.ds(1, half), zs + 1] = swap_halves(jnp.where(low_rows, high, first[:half]))
        v[pl.ds(1 + half, half), zs + 1] = jnp.where(low_rows, swap_halves(first[half:]), high)

    def y_pack(level, fields, x, carry):
        zs = sizes[level][1]
        width = 2**level
        low, high = carry
        lane = lanes_of((8, LANES))
        for z in range(zs):
            at = (x * zs + z) * width
            moved = turn(fields[z], at)
            low = jnp.where((lane >= at) & (lane < at + width), moved, low)
            before = lax.rem(at + LANES - width, LANES)
            high = jnp.where((lane >= before) & (lane < before + width), moved, high)
        return low, high

    def neighbours(level, which, x):
        xs, zs = sizes[level]
        width = 2**level
        v = s[f"v{level}{which}"]
        yin = s[f"r{level}{which}y"]
        here = v[x + 1, pl.ds(1, zs)]
        total = v[x, pl.ds(1, zs)] + v[x + 2, pl.ds(1, zs)]
        total = total + (v[x + 1, pl.ds(0, zs)] + v[x + 1, pl.ds(2, zs)])
        low, high = yin[0], yin[1]
        lows, highs = [], []
        for z in range(zs):
            at = (x * zs + z) * width
            lows.append(turn(low, lax.rem(2 * LANES + width - at, LANES)))
            highs.append(turn(high, lax.rem(2 * LANES - width - at, LANES)))
        lane = lanes_of((zs, 8, LANES))
        before = jnp.where(lane < width, jnp.stack(lows), turn(here, width))
        after = jnp.where(lane >= LANES - width, jnp.stack(highs), turn(here, LANES - width))
        return here, total + (before + after)

    def unrolled(level):
        return {0: 2, 1: 4, 2: 4}[level]

    def put(level, which, row):
        xs, zs = sizes[level]
        v = s[f"v{level}{which}"]

        def body(x, carry):
            value = row(x)
            v[x + 1, pl.ds(1, zs)] = value
            return y_pack(level, value, x, carry)

        zero = jnp.zeros((8, LANES), F32)
        low, high = loop(xs, body, (zero, zero), unrolled(level))
        s[f"p{level}{which}y"][0] = low
        s[f"p{level}{which}y"][1] = high
        exchange(level, which)

    def swept(level, which):
        coupling = 0.25**level

        def row(x):
            here, around = neighbours(level, which, x)
            b, w = s[f"b{level}"][x], s[f"w{level}"][x]
            return 0.2 * here + w * (b + coupling * around)

        return row

    lane = lanes_of((8, LANES))
    to_lane = lanes_of((LANES, LANES))
    from_lane = rows_of((LANES, LANES))

    def all_along(a, buffer, n, base):
        count = counts[a]
        copies = []
        for o in range(1, count):
            to = lax.rem(me[a] + o, count)
            copies.append(
                pltpu.make_async_remote_copy(
                    src_ref=buffer.at[me[a]],
                    dst_ref=buffer.at[me[a]],
                    send_sem=s["gsend"].at[n, base + o],
                    recv_sem=s["grecv"].at[n, base + o],
                    device_id={a: to},
                    device_id_type=MESH,
                )
            )
        for c in copies:
            c.start()
        for c in copies:
            c.wait_recv()
        for c in copies:
            c.wait_send()

    def gather_coarse(field, n):
        packed = jnp.zeros((8, LANES), F32)
        for x in range(2):
            place = (to_lane == 64 * x + 16 * me["gy"] + from_lane // 8) & (from_lane % 8 == 0)
            packed = packed + jnp.dot(
                field[x, 0], place.astype(F32), precision=HIGHEST, preferred_element_type=F32
            )
        s["g1"][n, me["gy"]] = packed
        all_along("gy", s["g1"].at[n], n, 0)
        parts = s["g1"][n]
        s["g2"][n, me["gz"]] = (parts[0] + parts[1]) + (parts[2] + parts[3])
        all_along("gz", s["g2"].at[n], n, 4)
        s["g3"][n, me["gx"]] = s["g2"][n]
        all_along("gx", s["g3"].at[n], n, 8)

    def coarsest(n):
        coupling = 0.25**LEVELS
        nx, nz = counts["gx"], counts["gz"]
        va, vb = s["gva"], s["gvb"]
        va[pl.ds(1, nx), pl.ds(1, nz)] = s["gw"][...] * s["g3"][n]
        shape = (nz, 8, LANES)
        glane, grow = lanes_of(shape), rows_of(shape)

        def sweep(src, dst):
            def body(x, carry):
                here = src[x + 1, pl.ds(1, nz)]
                along_x = turn(
                    here
                    + jnp.where(glane >= 64, src[x, pl.ds(1, nz)], src[x + 2, pl.ds(1, nz)]),
                    64,
                )
                along_z = swap_halves(
                    here
                    + jnp.where(
                        grow >= HALF, src[x + 1, pl.ds(0, nz)], src[x + 1, pl.ds(2, nz)]
                    )
                )
                before = jnp.where(glane % 64 == 0, 0.0, turn(here, 1))
                after = jnp.where(glane % 64 == 63, 0.0, turn(here, LANES - 1))
                around = (along_x + along_z) + (before + after)
                dst[x + 1, pl.ds(1, nz)] = 0.2 * here + s["gw"][x] * (
                    s["g3"][n, x] + coupling * around
                )
                return carry

            loop(nx, body, 0, 4)

        for i in range(COARSE_SWEEPS - 1):
            sweep(*((va, vb) if i % 2 == 0 else (vb, va)))
        done = vb if (COARSE_SWEEPS - 1) % 2 else va
        mine = done[1 + me["gx"], 1 + me["gz"]]
        for x in range(2):
            place = from_lane == 64 * x + 16 * me["gy"] + to_lane // 8
            s["e3"][x, 0] = jnp.dot(
                mine, place.astype(F32), precision=HIGHEST, preferred_element_type=F32
            )

    def down(level):
        xs, zs = sizes[level]
        coupling = 0.25**level
        put(level, "a", lambda x: s[f"w{level}"][x] * s[f"b{level}"][x])
        put(level, "b", swept(level, "a"))

        def remainder(x):
            here, around = neighbours(level, "b", x)
            return s[f"b{level}"][x] - (s[f"d{level}"][x] * here - coupling * around)

        def body(x, carry):
            fine = jnp.stack([remainder(2 * x), remainder(2 * x + 1)])
            s[f"b{level + 1}"][x] = coarse_of(fine, level)[0]
            return carry

        loop(xs // 2, body)

    def up(level):
        xs, zs = sizes[level]
        v = s[f"v{level}b"]

        def corrected(x):
            e = s[f"e{level + 1}"][x // 2]
            e = jnp.stack([e, e], axis=1).reshape(zs, 8, LANES)
            return v[x + 1, pl.ds(1, zs)] + e

        put(level, "a", corrected)
        put(level, "b", swept(level, "a"))

    def cycle(n):
        for level in range(LEVELS):
            down(level)
        gather_coarse(s["b3"][...], n + 1)
        coarsest(n + 1)
        for level in (2, 1):
            up(level)
            row = swept(level, "b")

            def body(x, carry, level=level, row=row):
                s[f"e{level}"][x] = row(x)
                return carry

            loop(sizes[level][0], body, 0, unrolled(level))
        up(0)
        put(0, "c", swept(0, "b"))

    gather_coarse(s["d3"][...], 0)
    gdiag = s["g3"][0]
    s["gw"][...] = 0.8 / gdiag

    def iterate(n, carry):
        cycle(n)

        def apply(x, c):
            here, around = neighbours(0, "c", x)
            q = s["d0"][x] * here - around
            s["z"][n, x] = here
            s["q"][n, x] = q

            @pl.when(n == 0)
            def _():
                s["flip"][x] = s["b0"][x].reshape(64, LANES)

            s["b0"][x] = q
            return c

        loop(16, apply)
        return carry

    loop(2, iterate)

    def reduce_all(dots, n):
        packed = jnp.zeros((8, LANES), F32)
        for j, d in enumerate(dots):
            total = jnp.sum(d, axis=-1, keepdims=True)
            packed = jnp.where(lane == j, total, packed)
        packed = packed + swap_halves(packed)
        s["a1"][n, me["gy"]] = packed
        all_along("gy", s["a1"].at[n], n, 16)
        parts = s["a1"][n]
        s["a2"][n, me["gz"]] = (parts[0] + parts[1]) + (parts[2] + parts[3])
        all_along("gz", s["a2"].at[n], n, 20)
        parts = s["a2"][n]
        s["a3"][n, me["gx"]] = (parts[0] + parts[1]) + (parts[2] + parts[3])
        all_along("gx", s["a3"].at[n], n, 24)
        parts = s["a3"][n]
        parts = (parts[:4] + parts[4:])
        total = (parts[0] + parts[1]) + (parts[2] + parts[3])
        return [total[:, j : j + 1] for j in range(len(dots))]

    zero = jnp.zeros((8, LANES), F32)

    def folded(value):
        while value.shape[0] > 1:
            value = value[: value.shape[0] // 2] + value[value.shape[0] // 2 :]
        return value[0]

    def dots_first(x, c):
        b = s["flip"][x].reshape(8, 8, LANES)
        z = s["z"][0, x]
        return c[0] + folded(b * z), c[1] + folded(z * s["q"][0, x])

    rz, zq = reduce_all(loop(16, dots_first, (zero, zero)), 0)
    step = jnp.broadcast_to(rz / zq, (8, LANES))

    def dots_second(x, c):
        q0 = s["q"][0, x]
        z0 = s["z"][0, x]
        r1 = s["flip"][x].reshape(8, 8, LANES) - step * q0
        z1 = z0 - step * s["z"][1, x]
        q1 = q0 - step * s["q"][1, x]
        s["z"][1, x] = z1
        pairs = ((r1, z1), (z1, q1), (z1, q0), (z0, q1), (r1, r1), (r1, q1), (r1, q0), (q1, q1), (q1, q0), (q0, q0))
        return tuple(t + folded(u * v) for t, (u, v) in zip(c, pairs))

    r1z1, z1q1, z1q0, z0q1, r1r1, r1q1, r1q0, q1q1, q1q0, q0q0 = reduce_all(
        loop(16, dots_second, (zero,) * 10), 1
    )
    ratio = r1z1 / rz
    step2 = r1z1 / (z1q1 + ratio * (z1q0 + z0q1) + ratio * ratio * zq)
    squares = (
        r1r1
        - 2.0 * step2 * (r1q1 + ratio * r1q0)
        + step2 * step2 * (q1q1 + 2.0 * ratio * q1q0 + ratio * ratio * q0q0)
    )
    norm = jnp.sqrt(jnp.maximum(squares, 0.0) * (1.0 / cells))
    norm_ref[...] = jnp.broadcast_to(norm, (8, LANES))
    along_z0 = jnp.broadcast_to(step + step2 * ratio, (8, LANES))
    along_z1 = jnp.broadcast_to(step2, (8, LANES))

    def finish(x, c):
        value = along_z0 * s["z"][0, x] + along_z1 * s["z"][1, x]
        s["flip"][x] = value.reshape(64, LANES)
        return c

    loop(16, finish)

    def write(x, c):
        for p in range(PROBES):
            for h in range(2):
                row = h * PROBES + p
                solution_ref[p, x, pl.ds(8 * h, 8), :] = s["flip"][x, pl.ds(row, 8, stride=8), :]
        return c

    loop(16, write)


SIZES = ((16, 8), (8, 4), (4, 2), (2, 1))


def scratch_list():
    out = {"flip": pltpu.VMEM((16, 64, LANES), F32)}
    for level, (xs, zs) in enumerate(SIZES):
        for name in "bdwe":
            out[f"{name}{level}"] = pltpu.VMEM((xs, zs, 8, LANES), F32)
        if level == LEVELS:
            continue
        for which in "abc" if level == 0 else "ab":
            out[f"v{level}{which}"] = pltpu.VMEM((xs + 2, zs + 2, 8, LANES), F32)
            out[f"r{level}{which}"] = pltpu.VMEM((2, xs // 2, 8, LANES), F32)
            out[f"p{level}{which}"] = pltpu.VMEM((2, xs // 2, 8, LANES), F32)
            out[f"r{level}{which}y"] = pltpu.VMEM((2, 8, LANES), F32)
            out[f"p{level}{which}y"] = pltpu.VMEM((2, 8, LANES), F32)
    out["z"] = pltpu.VMEM((2, 16, 8, 8, LANES), F32)
    out["q"] = pltpu.VMEM((2, 16, 8, 8, LANES), F32)
    out["g1"] = pltpu.VMEM((3, 4, 8, LANES), F32)
    out["g2"] = pltpu.VMEM((3, 4, 8, LANES), F32)
    out["g3"] = pltpu.VMEM((3, 8, 4, 8, LANES), F32)
    out["a1"] = pltpu.VMEM((2, 4, 8, LANES), F32)
    out["a2"] = pltpu.VMEM((2, 4, 8, LANES), F32)
    out["a3"] = pltpu.VMEM((2, 8, 8, LANES), F32)
    out["gw"] = pltpu.VMEM((8, 4, 8, LANES), F32)
    out["gva"] = pltpu.VMEM((10, 6, 8, LANES), F32)
    out["gvb"] = pltpu.VMEM((10, 6, 8, LANES), F32)
    out["send"] = pltpu.SemaphoreType.DMA((3, 6))
    out["recv"] = pltpu.SemaphoreType.DMA((3, 6))
    out["gsend"] = pltpu.SemaphoreType.DMA((3, 32))
    out["grecv"] = pltpu.SemaphoreType.DMA((3, 32))
    return out


def scratch_names():
    return list(scratch_list())


def solution(mesh):
    counts = {a: mesh.shape[a] for a in ("gx", "gy", "gz")}

    def step(kappa_sq, probe_bits):
        cells = probe_bits[0].size * counts["gx"] * counts["gy"] * counts["gz"]
        whole, norms = pl.pallas_call(
            functools.partial(kernel_body, SIZES, counts, cells),
            out_shape=(
                jax.ShapeDtypeStruct(probe_bits.shape, F32),
                jax.ShapeDtypeStruct((8, LANES), F32),
            ),
            in_specs=[pl.BlockSpec(memory_space=pltpu.VMEM)] * 2,
            out_specs=(pl.BlockSpec(memory_space=pltpu.VMEM),) * 2,
            scratch_shapes=list(scratch_list().values()),
            compiler_params=pltpu.CompilerParams(
                collective_id=0, has_side_effects=True, vmem_limit_bytes=40 * 2**20
            ),
            name="solve",
        )(kappa_sq, probe_bits)
        return whole, norms[:PROBES, 0]

    return jax.shard_map(
        step,
        mesh=mesh,
        in_specs=(P("gx", "gz", "gy"), P(None, "gx", "gz", "gy")),
        out_specs=(P(None, "gx", "gz", "gy"), P()),
        check_vma=False,
    )
```

```python
import functools

import jax
import jax.numpy as jnp
from jax import lax
from jax.experimental import pallas as pl
from jax.experimental.pallas import tpu as pltpu
from jax.sharding import PartitionSpec as P

LEVELS = 3
COARSE_SWEEPS = 8
PROBES = 4
LANES = 128
HALF = 4
MESH = pl.DeviceIdType.MESH
F32 = jnp.float32
HIGHEST = lax.Precision.HIGHEST

OWN = {1: 32, 2: 48, 3: 24}
REACH = {1: 3, 2: 4}


def lanes_of(shape):
    return lax.broadcasted_iota(jnp.int32, shape, len(shape) - 1)


def rows_of(shape):
    return lax.broadcasted_iota(jnp.int32, shape, len(shape) - 2)


def turn(value, shift):
    return pltpu.roll(value, shift, len(value.shape) - 1)


def swap_halves(value):
    return pltpu.roll(value, HALF, len(value.shape) - 2)


def kernel_body(counts, cells, kappa_ref, bits_ref, solution_ref, norm_ref, *scratch):
    s = dict(zip(scratch_list(), scratch))
    axes = ("gx", "gz", "gy")
    me = {a: lax.axis_index(a) for a in axes}
    nx, nz = counts["gx"], counts["gz"]
    lane = lanes_of((8, LANES))

    def loop(count, body, init=0, unroll=1):
        return lax.fori_loop(0, count, body, init, unroll=unroll)

    def exists(steps):
        ok = None
        for a, d in zip(axes, steps):
            if d:
                one = me[a] > 0 if d < 0 else me[a] < counts[a] - 1
                ok = one if ok is None else ok & one
        return ok

    def device(steps):
        return {a: me[a] + d for a, d in zip(axes, steps)}

    around_me = [
        (i, j, k) for i in (-1, 0, 1) for j in (-1, 0, 1) for k in (-1, 0, 1) if (i, j, k) != (0, 0, 0)
    ]

    for which in "abc":
        ref = s[f"v0{which}"]
        for x in (0, 17):
            ref[x] = jnp.zeros(ref.shape[1:], F32)
        for name in (f"r0{which}", f"r0{which}y"):
            s[name][...] = jnp.zeros(s[name].shape, F32)
    for name in ("m1", "y1", "m2"):
        ref = s[name]

        def clear(i, carry, ref=ref):
            for j in range(3):
                ref[i // 3, lax.rem(i, 3), j] = jnp.zeros(ref.shape[3:], F32)
            return carry

        loop(9, clear)
    for name in ("gva", "gvb"):
        s[name][...] = jnp.zeros(s[name].shape, F32)

    barrier = pltpu.get_barrier_semaphore()

    def greet(to):
        pl.semaphore_signal(barrier, inc=1, device_id=to, device_id_type=MESH)

    def plane_peer(o):
        i, j = o // nz, lax.rem(o, nz)
        return {"gx": lax.rem(me["gx"] + i, nx), "gz": lax.rem(me["gz"] + j, nz)}

    def greet_plane(o, carry):
        greet(plane_peer(o + 1))
        return carry

    loop(nx * nz - 1, greet_plane)
    for o in range(1, counts["gy"]):
        greet({"gy": lax.rem(me["gy"] + o, counts["gy"])})
    for steps in around_me:
        if steps[2] and steps[:2] != (0, 0):
            pl.when(exists(steps))(functools.partial(greet, device(steps)))
    near = {
        a: (me[a] > 0).astype(jnp.int32) + (me[a] < counts[a] - 1).astype(jnp.int32) for a in axes
    }
    greeted = (
        nx * nz - 1 + counts["gy"] - 1 + ((near["gx"] + 1) * (near["gz"] + 1) - 1) * near["gy"]
    )

    row_at = rows_of((LANES, LANES))
    col_at = lanes_of((LANES, LANES))

    def halved(value):
        return (value + 256) // 2 - 128

    def keep(name, where, weight):
        s["lanes"][MATRICES.index(name)] = jnp.where(where, weight, 0.0)

    keep("c01", col_at == 32 + row_at // 2, 0.125)
    keep("c12", (col_at == 48 + halved(row_at - 32)) & (row_at >= 32) & (row_at < 96), 0.125)
    inside = (row_at >= 18) & (row_at < 110)
    keep("p10", row_at == 32 + col_at // 2, 1.0)
    keep("p21", row_at == 48 + halved(col_at - 32), 1.0)
    for i in range(2):
        keep(f"c23{i}", (col_at == 64 * i + 24 + halved(row_at - 48)) & inside, 0.125)
        keep(f"p32{i}", row_at == 64 * i + 24 + halved(col_at - 48), 1.0)

    def moved(value, name):
        shape = value.shape
        flat = jnp.dot(
            value.reshape(-1, LANES),
            s["lanes"][MATRICES.index(name)],
            precision=HIGHEST,
            preferred_element_type=F32,
        )
        return flat.reshape(shape)

    def load_x(x, carry):
        for p in range(PROBES):
            for h in range(2):
                row = h * PROBES + p
                s["flip"][x, pl.ds(row, 8, stride=8), :] = (
                    2.0 * bits_ref[p, x, pl.ds(8 * h, 8), :].astype(F32) - 1.0
                )
        return carry

    def take_x(x, carry):
        s["b0"][x] = s["flip"][x].reshape(8, 8, LANES)
        return carry

    def kappa_x(x, carry):
        for p in range(PROBES):
            for h in range(2):
                row = h * PROBES + p
                s["flip"][x, pl.ds(row, 8, stride=8), :] = kappa_ref[x, pl.ds(8 * h, 8), :]
        return carry

    def pair_sum(field):
        xs, zs = field.shape[0] // 2, field.shape[1] // 2
        split = field.reshape(xs, 2, zs, 2, 8, LANES)
        return (split[:, 0, :, 0] + split[:, 0, :, 1]) + (split[:, 1, :, 0] + split[:, 1, :, 1])

    def diag_x(x, carry):
        kappas = [s["flip"][2 * x + i].reshape(8, 8, LANES) for i in range(2)]
        for i in range(2):
            s["d0"][2 * x + i] = kappas[i] + 6.0
            s["w0"][2 * x + i] = 0.8 / (kappas[i] + 6.0)
        s["t1"][x] = pair_sum(jnp.stack(kappas))[0]
        return carry

    loop(16, load_x)
    loop(16, take_x)
    loop(16, kappa_x)
    loop(8, diag_x)

    def exchange(which):
        v = s[f"v0{which}"]
        got = s[f"r0{which}"]
        pack = s[f"p0{which}"]
        yin = s[f"r0{which}y"]
        yout = s[f"p0{which}y"]
        slot = "abc".index(which)
        first = v[pl.ds(1, 16), 1]
        last = v[pl.ds(1, 16), 8]
        low_rows = rows_of((8, 8, LANES)) < HALF
        pack[0] = jnp.where(low_rows, first[:8], swap_halves(first[8:]))
        pack[1] = jnp.where(low_rows, swap_halves(last[:8]), last[8:])
        inner = pl.ds(1, 8)
        plan = []
        for n, (steps, src, dst) in enumerate(
            (
                ((0, -1, 0), pack.at[0], got.at[1]),
                ((0, 1, 0), pack.at[1], got.at[0]),
                ((-1, 0, 0), v.at[1, inner], v.at[17, inner]),
                ((1, 0, 0), v.at[16, inner], v.at[0, inner]),
                ((0, 0, -1), yout.at[0], yin.at[1]),
                ((0, 0, 1), yout.at[1], yin.at[0]),
            )
        ):
            c = pltpu.make_async_remote_copy(
                src_ref=src,
                dst_ref=dst,
                send_sem=s["send"].at[slot, n],
                recv_sem=s["recv"].at[slot, n],
                device_id=device(steps),
                device_id_type=MESH,
            )
            plan.append((exists(steps), exists(tuple(-d for d in steps)), c))
        for there, _, c in plan:
            pl.when(there)(c.start)
        for _, back, c in plan:
            pl.when(back)(c.wait_recv)
        for there, _, c in plan:
            pl.when(there)(c.wait_send)
        low, high = got[0], got[1]
        v[pl.ds(1, 8), 0] = jnp.where(low_rows, low, swap_halves(last[:8]))
        v[pl.ds(9, 8), 0] = swap_halves(jnp.where(low_rows, last[8:], low))
        v[pl.ds(1, 8), 9] = swap_halves(jnp.where(low_rows, high, first[:8]))
        v[pl.ds(9, 8), 9] = jnp.where(low_rows, swap_halves(first[8:]), high)

    def y_pack(fields, x, carry):
        low, high = carry
        for z in range(8):
            at = x * 8 + z
            turned = turn(fields[z], at)
            low = jnp.where(lane == at, turned, low)
            high = jnp.where(lane == lax.rem(at + LANES - 1, LANES), turned, high)
        return low, high

    def neighbours(which, x):
        v = s[f"v0{which}"]
        yin = s[f"r0{which}y"]
        here = v[x + 1, pl.ds(1, 8)]
        total = v[x, pl.ds(1, 8)] + v[x + 2, pl.ds(1, 8)]
        total = total + (v[x + 1, pl.ds(0, 8)] + v[x + 1, pl.ds(2, 8)])
        low, high = yin[0], yin[1]
        lows, highs = [], []
        for z in range(8):
            at = x * 8 + z
            lows.append(turn(low, lax.rem(2 * LANES + 1 - at, LANES)))
            highs.append(turn(high, lax.rem(2 * LANES - 1 - at, LANES)))
        at_lane = lanes_of((8, 8, LANES))
        before = jnp.where(at_lane < 1, jnp.stack(lows), turn(here, 1))
        after = jnp.where(at_lane >= LANES - 1, jnp.stack(highs), turn(here, LANES - 1))
        return here, total + (before + after)

    def put(which, row):
        v = s[f"v0{which}"]

        def body(x, carry):
            value = row(x)
            v[x + 1, pl.ds(1, 8)] = value
            return y_pack(value, x, carry)

        zero = jnp.zeros((8, LANES), F32)
        low, high = loop(16, body, (zero, zero), 2)
        s[f"p0{which}y"][0] = low
        s[f"p0{which}y"][1] = high
        exchange(which)

    def swept(which):
        def row(x):
            here, around = neighbours(which, x)
            return 0.2 * here + s["w0"][x] * (s["b0"][x] + around)

        return row

    def start_exchange(level, n, field):
        if level == 1:
            pack = s["m1"].at[n, 1, 1]
            pairs = field.reshape(4, 2, 4, 8, LANES)
            pack[...] = turn(pairs[:, 0], LANES - 32) + turn(pairs[:, 1], 32)
            low = high = jnp.zeros((8, LANES), F32)
            for x in range(8):
                for z in range(4):
                    at = 4 * (4 * x + z)
                    slot = (lane >= at) & (lane < at + 4)
                    low = jnp.where(slot, turn(field[x, z], (at + 2 * LANES - 32) % LANES), low)
                    high = jnp.where(slot, turn(field[x, z], (at + 2 * LANES - 92) % LANES), high)
            s["y1out"][n, 0] = high
            s["y1out"][n, 1] = low
        else:
            pack = s["m2"].at[n, 1, 1, 1]
            total = turn(field[0], LANES - 48)
            for x in range(1, 4):
                total = total + turn(field[x], (32 * x + LANES - 48) % LANES)
            pack[...] = total
        plan = exchange_plan(level, n)
        for there, _, c in plan:
            pl.when(there)(c.start)
        return plan

    def exchange_plan(level, n):
        plan = []
        for steps in around_me:
            i, j, k = steps
            if level == 2:
                src = s["m2"].at[n, 1, 1, 1]
                dst = s["m2"].at[n, 1 - i, 1 - j, 1 - k]
            elif k:
                side = 0 if k > 0 else 1
                src = s["y1out"].at[n, side]
                dst = s["y1"].at[n, 1 - i, 1 - j, side]
            else:
                if j == 0:
                    part = (pl.ds(0 if i < 0 else 2, 2),)
                elif i == 0:
                    part = (slice(None), pl.ds(0 if j < 0 else 1, 3))
                else:
                    part = (pl.ds(0 if i < 0 else 3, 1), pl.ds(0 if j < 0 else 2, 2))
                src = s["m1"].at[(n, 1, 1, *part)]
                dst = s["m1"].at[(n, 1 - i, 1 - j, *part)]
            at = 9 * (i + 1) + 3 * (j + 1) + (k + 1)
            c = pltpu.make_async_remote_copy(
                src_ref=src,
                dst_ref=dst,
                send_sem=s["xsend"].at[level - 1, n, at],
                recv_sem=s["xrecv"].at[level - 1, n, at],
                device_id=device(steps),
                device_id_type=MESH,
            )
            plan.append((exists(steps), exists(tuple(-d for d in steps)), c))
        return plan

    def finish_exchange(level, n, plan, out):
        for _, back, c in plan:
            pl.when(back)(c.wait_recv)
        for there, _, c in plan:
            pl.when(there)(c.wait_send)
        low_rows = rows_of((8, LANES)) < HALF
        reach = REACH[level]
        xs, zs = (8, 4) if level == 1 else (4, 2)

        def body(x, carry):
            far = (x + xs - reach) // xs
            at_x = lax.rem(x + xs - reach, xs)

            def source(j, z):
                if level == 1:
                    mid = turn(
                        s["m1"][n, far, j, at_x // 2, z], 32 + 64 * lax.rem(at_x, 2)
                    )
                    at = 4 * (4 * at_x + z)
                    left = turn(s["y1"][n, far, j, 0], lax.rem(28 - at + 2 * LANES, LANES))
                    right = turn(s["y1"][n, far, j, 1], lax.rem(96 - at + 2 * LANES, LANES))
                    value = jnp.where((lane >= 28) & (lane < 32), left, 0.0)
                    value = jnp.where((lane >= 96) & (lane < 100), right, value)
                    return jnp.where((lane >= 32) & (lane < 96), mid, value)
                value = jnp.zeros((8, LANES), F32)
                for k in range(3):
                    start = 16 + 32 * k
                    part = turn(
                        s["m2"][n, far, j, k, z], lax.rem(start + 2 * LANES - 32 * at_x, LANES)
                    )
                    value = jnp.where((lane >= start) & (lane < start + 32), part, value)
                return value

            mine = [source(1, z) for z in range(zs)]
            if level == 1:
                down = [None] + [source(0, z) for z in (1, 2, 3)]
                over = [source(2, z) for z in (0, 1, 2)]
                below = [(down[z], mine[z]) for z in (1, 2, 3)]
                above = [(over[z], mine[z]) for z in (0, 1, 2)]
                outer_low, outer_high = [], []
            else:
                outer_low = [source(0, z) for z in range(2)]
                outer_high = [source(2, z) for z in range(2)]
                below = list(zip(outer_low, mine))
                above = list(zip(outer_high, mine))
            values = list(outer_low)
            values += [swap_halves(jnp.where(low_rows, own, other)) for other, own in below]
            values += mine
            values += [swap_halves(jnp.where(low_rows, other, own)) for other, own in above]
            values += outer_high
            out[x] = jnp.stack(values)
            return carry

        loop(xs + 2 * reach, body)

    def held_row(src, x, z0, z1):
        inner = pl.ds(z0, z1 - z0)
        here = src[x, inner]
        total = (src[x - 1, inner] + src[x + 1, inner]) + (
            src[x, pl.ds(z0 - 1, z1 - z0)] + src[x, pl.ds(z0 + 1, z1 - z0)]
        )
        return here, total + (turn(here, 1) + turn(here, LANES - 1))

    def held_sweep(level, src, dst, margin, into=0):
        xs, zs = s[f"b{level}"].shape[:2]
        coupling = 0.25**level
        z0, z1 = margin, zs - margin

        def body(i, carry):
            x = i + margin
            here, around = held_row(src, x, z0, z1)
            inner = pl.ds(z0, z1 - z0)
            value = 0.2 * here + s[f"w{level}"][x, inner] * (
                s[f"b{level}"][x, inner] + coupling * around
            )
            if into:
                dst[i] = value
            else:
                dst[x, inner] = value
            return carry

        loop(xs - 2 * margin, body, 0, 2)

    def held_down(level):
        xs, zs = s[f"b{level}"].shape[:2]
        reach = REACH[level]
        coupling = 0.25**level

        def begin(x, carry):
            s[f"v{level}a"][x] = s[f"w{level}"][x] * s[f"b{level}"][x]
            return carry

        loop(xs, begin)
        held_sweep(level, s[f"v{level}a"], s[f"v{level}b"], 1)
        z0, z1 = reach, zs - reach
        own = []
        for x in range(reach, xs - reach):
            here, around = held_row(s[f"v{level}b"], x, z0, z1)
            inner = pl.ds(z0, z1 - z0)
            own.append(
                s[f"b{level}"][x, inner] - (s[f"d{level}"][x - reach] * here - coupling * around)
            )
        return jnp.stack(own)

    def held_up(level, coarse, spread, out, last_margin):
        xs, zs = s[f"b{level}"].shape[:2]

        def add(i, carry):
            x = i + 1
            picked = jnp.stack([coarse[spread(x), spread(z)] for z in range(1, zs - 1)])
            s[f"v{level}a"][x, pl.ds(1, zs - 2)] = s[f"v{level}b"][x, pl.ds(1, zs - 2)] + picked
            return carry

        loop(xs - 2, add)
        held_sweep(level, s[f"v{level}a"], s[f"v{level}b"], 2)
        held_sweep(level, s[f"v{level}b"], out, 3, into=1)

    def own_of(level, ref):
        reach = REACH[level]
        xs, zs = ref.shape[:2]
        return ref[pl.ds(reach, xs - 2 * reach), pl.ds(reach, zs - 2 * reach)]

    def coefficients(level, kappa):
        coupling = 6.0 * 0.25**level
        s[f"d{level}"][...] = own_of(level, kappa) + coupling

        def body(x, carry):
            k = kappa[x]
            s[f"w{level}"][x] = jnp.where(k > 0.0, 0.8 / (k + coupling), 0.0)
            return carry

        loop(kappa.shape[0], body)

    def plane_copies(ref, sems, o):
        at = ref.at[me["gx"], me["gz"]]
        return pltpu.make_async_remote_copy(
            src_ref=at,
            dst_ref=at,
            send_sem=s["gsend"].at[sems, o],
            recv_sem=s["grecv"].at[sems, o],
            device_id=plane_peer(o),
            device_id_type=MESH,
        )

    def plane_start(ref, sems):
        def body(o, carry):
            plane_copies(ref, sems, o + 1).start()
            return carry

        loop(nx * nz - 1, body)

    def plane_finish(ref, sems):
        def body(o, carry):
            plane_copies(ref, sems, o + 1).wait_recv()
            return carry

        loop(nx * nz - 1, body)

        def body_send(o, carry):
            plane_copies(ref, sems, o + 1).wait_send()
            return carry

        loop(nx * nz - 1, body_send)

    def gather_start(n, field):
        pairs = pair_sum(field)
        s["g3"][n, me["gx"], me["gz"]] = moved(pairs[0, 0], "c230") + moved(pairs[1, 0], "c231")
        plane_start(s["g3"].at[n], n)

    def gather_finish(n):
        plane_finish(s["g3"].at[n], n)

    def coarsest(n):
        coupling = 0.25**LEVELS
        va, vb = s["gva"], s["gvb"]
        va[pl.ds(1, nx), pl.ds(1, nz)] = s["gw"][...] * s["g3"][n]
        glane, grow = lanes_of((nz, 8, LANES)), rows_of((nz, 8, LANES))
        inner = pl.ds(1, nz)

        def sweep(src, dst):
            def body(x, carry):
                here = src[x + 1, inner]
                along_x = turn(
                    here + jnp.where(glane >= 64, src[x, inner], src[x + 2, inner]), 64
                )
                along_z = swap_halves(
                    here
                    + jnp.where(grow >= HALF, src[x + 1, pl.ds(0, nz)], src[x + 1, pl.ds(2, nz)])
                )
                around = (along_x + along_z) + (turn(here, 1) + turn(here, LANES - 1))
                dst[x + 1, inner] = 0.2 * here + s["gw"][x] * (s["g3"][n, x] + coupling * around)
                return carry

            loop(nx, body, 0, 4)

        for i in range(COARSE_SWEEPS - 1):
            sweep(*((va, vb) if i % 2 == 0 else (vb, va)))
        done = vb if (COARSE_SWEEPS - 1) % 2 else va
        low_rows = rows_of((8, LANES)) < HALF
        near_me = []
        for i in range(3):
            below, mine, above = (done[i + me["gx"], j + me["gz"]] for j in range(3))
            near_me += [
                below,
                swap_halves(jnp.where(low_rows, mine, below)),
                mine,
                swap_halves(jnp.where(low_rows, above, mine)),
                above,
            ]
        near_me = jnp.stack(near_me)
        for i in range(2):
            spread = moved(near_me, f"p32{i}")
            for x in range(3):
                s["e3"][2 * x + i] = spread[5 * x : 5 * x + 5]

    def sum_start(dots, n):
        packed = jnp.zeros((8, LANES), F32)
        for j, d in enumerate(dots):
            packed = jnp.where(lane == j, jnp.sum(d, axis=-1, keepdims=True), packed)
        s["a1"][n, me["gx"], me["gz"]] = packed + swap_halves(packed)
        plane_start(s["a1"].at[n], 3 + n)

    def gy_copies(n):
        at = s["a2"].at[n, me["gy"]]
        return [
            pltpu.make_async_remote_copy(
                src_ref=at,
                dst_ref=at,
                send_sem=s["gsend"].at[5 + n, o],
                recv_sem=s["grecv"].at[5 + n, o],
                device_id={"gy": lax.rem(me["gy"] + o, counts["gy"])},
                device_id_type=MESH,
            )
            for o in range(1, counts["gy"])
        ]

    def folded(value):
        while value.shape[0] > 1:
            value = value[: value.shape[0] // 2] + value[value.shape[0] // 2 :]
        return value[0]

    def sum_middle(n):
        plane_finish(s["a1"].at[n], 3 + n)
        s["a2"][n, me["gy"]] = folded(s["a1"][n].reshape(nx * nz, 8, LANES))
        for c in gy_copies(n):
            c.start()

    def sum_finish(n, count):
        for c in gy_copies(n):
            c.wait_recv()
        for c in gy_copies(n):
            c.wait_send()
        total = folded(s["a2"][n])
        return [total[:, j : j + 1] for j in range(count)]

    kappa_1 = moved(s["t1"][...], "c01")
    kappa_2 = moved(pair_sum(kappa_1), "c12")
    pl.semaphore_wait(barrier, greeted)
    kappa_plans = {1: start_exchange(1, 0, kappa_1), 2: start_exchange(2, 0, kappa_2)}

    def cycle(n, meanwhile_1, meanwhile_2):
        put("a", lambda x: s["w0"][x] * s["b0"][x])
        put("b", swept("a"))

        def remainder(x):
            here, around = neighbours("b", x)
            return s["b0"][x] - (s["d0"][x] * here - around)

        def body(x, carry):
            s["t1"][x] = pair_sum(jnp.stack([remainder(2 * x), remainder(2 * x + 1)]))[0]
            return carry

        loop(8, body)
        plan = start_exchange(1, n, moved(s["t1"][...], "c01"))
        meanwhile_1()
        finish_exchange(1, n, plan, s["b1"])
        plan = start_exchange(2, n, moved(pair_sum(held_down(1)), "c12"))
        meanwhile_2()
        finish_exchange(2, n, plan, s["b2"])
        gather_start(n, held_down(2))
        if n == 1:
            gather_finish(0)
            kappa_3 = s["g3"][0]
            s["gw"][...] = jnp.where(kappa_3 > 0.0, 0.8 / (kappa_3 + 6.0 * 0.25**LEVELS), 0.0)
        gather_finish(n)
        coarsest(n)
        held_up(2, s["e3"], lambda i: i // 2, s["e2"], 3)
        s["t2"][...] = moved(s["e2"][...], "p21")
        held_up(1, s["t2"], lambda i: (i - 1) // 2, s["e1"], 3)
        s["t1"][...] = moved(s["e1"][...], "p10")

        def corrected(x):
            e = s["t1"][x // 2]
            return s["v0b"][x + 1, pl.ds(1, 8)] + jnp.stack([e, e], axis=1).reshape(8, 8, LANES)

        put("a", corrected)
        put("b", swept("a"))
        put("c", swept("b"))

        def apply(x, c):
            here, around = neighbours("c", x)
            q = s["d0"][x] * here - around
            s["z"][n - 1, x] = here
            s["q"][n - 1, x] = q
            b = s["b0"][x]
            if n == 1:
                s["flip"][x] = b.reshape(64, LANES)
                s["b0"][x] = q
            return c[0] + folded(b * here), c[1] + folded(here * q)

        return loop(16, apply, (jnp.zeros((8, LANES), F32),) * 2)

    def kappa_held_1():
        finish_exchange(1, 0, kappa_plans[1], s["v1a"])
        coefficients(1, s["v1a"])
        finish_exchange(2, 0, kappa_plans[2], s["v2a"])
        coefficients(2, s["v2a"])
        gather_start(0, own_of(2, s["v2a"]))

    sum_start(cycle(1, kappa_held_1, lambda: None), 0)
    cycle(2, lambda: sum_middle(0), lambda: None)
    rz, zq = sum_finish(0, 2)
    step = jnp.broadcast_to(rz / zq, (8, LANES))
    zero = jnp.zeros((8, LANES), F32)

    def dots_second(x, c):
        q0 = s["q"][0, x]
        z0 = s["z"][0, x]
        r1 = s["flip"][x].reshape(8, 8, LANES) - step * q0
        z1 = z0 - step * s["z"][1, x]
        q1 = q0 - step * s["q"][1, x]
        s["z"][1, x] = z1
        pairs = (
            (r1, z1),
            (z1, q1),
            (z1, q0),
            (z0, q1),
            (r1, r1),
            (r1, q1),
            (r1, q0),
            (q1, q1),
            (q1, q0),
            (q0, q0),
        )
        return tuple(t + folded(u * v) for t, (u, v) in zip(c, pairs))

    sum_start(loop(16, dots_second, (zero,) * 10), 1)
    sum_middle(1)
    r1z1, z1q1, z1q0, z0q1, r1r1, r1q1, r1q0, q1q1, q1q0, q0q0 = sum_finish(1, 10)
    ratio = r1z1 / rz
    step2 = r1z1 / (z1q1 + ratio * (z1q0 + z0q1) + ratio * ratio * zq)
    squares = (
        r1r1
        - 2.0 * step2 * (r1q1 + ratio * r1q0)
        + step2 * step2 * (q1q1 + 2.0 * ratio * q1q0 + ratio * ratio * q0q0)
    )
    norm = jnp.sqrt(jnp.maximum(squares, 0.0) * (1.0 / cells))
    norm_ref[...] = jnp.broadcast_to(norm, (8, LANES))
    along_z0 = jnp.broadcast_to(step + step2 * ratio, (8, LANES))
    along_z1 = jnp.broadcast_to(step2, (8, LANES))

    def finish(x, c):
        value = along_z0 * s["z"][0, x] + along_z1 * s["z"][1, x]
        s["flip"][x] = value.reshape(64, LANES)
        return c

    loop(16, finish)

    def write(x, c):
        for p in range(PROBES):
            for h in range(2):
                row = h * PROBES + p
                solution_ref[p, x, pl.ds(8 * h, 8), :] = s["flip"][x, pl.ds(row, 8, stride=8), :]
        return c

    loop(16, write)


MATRICES = ("c01", "c12", "p10", "p21", "c230", "c231", "p320", "p321")


def scratch_list():
    def fields(*lead):
        return pltpu.VMEM((*lead, 8, LANES), F32)

    out = {"flip": pltpu.VMEM((16, 64, LANES), F32), "lanes": pltpu.VMEM((8, LANES, LANES), F32)}
    for name in ("b0", "d0", "w0"):
        out[name] = fields(16, 8)
    for which in "abc":
        out[f"v0{which}"] = fields(18, 10)
        out[f"r0{which}"] = fields(2, 8)
        out[f"p0{which}"] = fields(2, 8)
        out[f"r0{which}y"] = fields(2)
        out[f"p0{which}y"] = fields(2)
    for level, xs, zs in ((1, 8, 4), (2, 4, 2)):
        reach = REACH[level]
        for name in (f"b{level}", f"w{level}", f"v{level}a", f"v{level}b"):
            out[name] = fields(xs + 2 * reach, zs + 2 * reach)
        out[f"d{level}"] = fields(xs, zs)
    out["e1"] = fields(8, 4)
    out["t1"] = fields(8, 4)
    out["e2"] = fields(6, 4)
    out["t2"] = fields(6, 4)
    out["e3"] = fields(6, 5)
    out["m1"] = fields(3, 3, 3, 4, 4)
    out["y1"] = fields(3, 3, 3, 2)
    out["y1out"] = fields(3, 2)
    out["m2"] = fields(3, 3, 3, 3, 2)
    out["z"] = fields(2, 16, 8)
    out["q"] = fields(2, 16, 8)
    out["g3"] = fields(3, 8, 4)
    out["a1"] = fields(2, 8, 4)
    out["a2"] = fields(2, 4)
    out["gw"] = fields(8, 4)
    out["gva"] = fields(10, 6)
    out["gvb"] = fields(10, 6)
    out["send"] = pltpu.SemaphoreType.DMA((3, 6))
    out["recv"] = pltpu.SemaphoreType.DMA((3, 6))
    out["xsend"] = pltpu.SemaphoreType.DMA((2, 3, 27))
    out["xrecv"] = pltpu.SemaphoreType.DMA((2, 3, 27))
    out["gsend"] = pltpu.SemaphoreType.DMA((7, 32))
    out["grecv"] = pltpu.SemaphoreType.DMA((7, 32))
    return out


def solution(mesh):
    counts = {a: mesh.shape[a] for a in ("gx", "gy", "gz")}

    def step(kappa_sq, probe_bits):
        cells = probe_bits[0].size * counts["gx"] * counts["gy"] * counts["gz"]
        whole, norms = pl.pallas_call(
            functools.partial(kernel_body, counts, cells),
            out_shape=(
                jax.ShapeDtypeStruct(probe_bits.shape, F32),
                jax.ShapeDtypeStruct((8, LANES), F32),
            ),
            in_specs=[pl.BlockSpec(memory_space=pltpu.VMEM)] * 2,
            out_specs=(pl.BlockSpec(memory_space=pltpu.VMEM),) * 2,
            scratch_shapes=list(scratch_list().values()),
            compiler_params=pltpu.CompilerParams(
                collective_id=0, has_side_effects=True, vmem_limit_bytes=40 * 2**20
            ),
            name="solve",
        )(kappa_sq, probe_bits)
        return whole, norms[:PROBES, 0]

    return jax.shard_map(
        step,
        mesh=mesh,
        in_specs=(P("gx", "gz", "gy"), P(None, "gx", "gz", "gy")),
        out_specs=(P(None, "gx", "gz", "gy"), P()),
        check_vma=False,
    )
```

```python
import functools

import jax
import jax.numpy as jnp
from jax import lax
from jax.experimental import pallas as pl
from jax.experimental.pallas import tpu as pltpu
from jax.sharding import PartitionSpec as P

LEVELS = 3
COARSE_SWEEPS = 8
PROBES = 4
LANES = 128
HALF = 4
MESH = pl.DeviceIdType.MESH
F32 = jnp.float32

OWN = {1: 32, 2: 48, 3: 24}
REACH = {1: 3, 2: 4}
HELD = {1: (14, 10), 2: (12, 10)}
CORE = {1: (8, 4), 2: (4, 2)}


def lanes_of(shape):
    return lax.broadcasted_iota(jnp.int32, shape, len(shape) - 1)


def rows_of(shape):
    return lax.broadcasted_iota(jnp.int32, shape, len(shape) - 2)


def turn(value, shift):
    return pltpu.roll(value, shift, len(value.shape) - 1)


def swap_halves(value):
    return pltpu.roll(value, HALF, len(value.shape) - 2)


def kernel_body(counts, cells, kappa_ref, bits_ref, solution_ref, norm_ref, *scratch):
    s = dict(zip(scratch_list(), scratch))
    axes = ("gx", "gz", "gy")
    me = {a: lax.axis_index(a) for a in axes}
    nx, nz = counts["gx"], counts["gz"]
    lane = lanes_of((8, LANES))

    def loop(count, body, init=0, unroll=1):
        return lax.fori_loop(0, count, body, init, unroll=count)

    def exists(steps):
        ok = None
        for a, d in zip(axes, steps):
            if d:
                one = me[a] > 0 if d < 0 else me[a] < counts[a] - 1
                ok = one if ok is None else ok & one
        return ok

    def device(steps):
        return {a: me[a] + d for a, d in zip(axes, steps)}

    around_me = [
        (i, j, k) for i in (-1, 0, 1) for j in (-1, 0, 1) for k in (-1, 0, 1) if (i, j, k) != (0, 0, 0)
    ]

    def clear_faces(i, carry):
        for x in (0, 17):
            s["v0"][i, x] = jnp.zeros(s["v0"].shape[2:], F32)
        for name in ("r0", "r0y"):
            s[name][i] = jnp.zeros(s[name].shape[1:], F32)
        return carry

    loop(3, clear_faces)
    for name in ("m1", "y1", "m2"):
        ref = s[name]

        def clear(i, carry, ref=ref):
            for j in range(3):
                ref[i // 3, lax.rem(i, 3), j] = jnp.zeros(ref.shape[3:], F32)
            return carry

        loop(9, clear)

    def clear_coarse(i, carry):
        s["gv"][i // 10, lax.rem(i, 10)] = jnp.zeros(s["gv"].shape[2:], F32)
        return carry

    loop(20, clear_coarse)

    barrier = pltpu.get_barrier_semaphore()

    def greet(to):
        pl.semaphore_signal(barrier, inc=1, device_id=to, device_id_type=MESH)

    def wrapped(a, step):
        to = me[a] + step
        return jnp.where(to >= counts[a], to - counts[a], to)

    def plane_peer(i, j):
        return {"gx": wrapped("gx", i), "gz": wrapped("gz", j)}

    plane_offsets = sorted(
        ((i, j) for i in range(nx) for j in range(nz) if (i, j) != (0, 0)),
        key=lambda at: -min(at[0], nx - at[0]) - 2 * min(at[1], nz - at[1]),
    )
    for i, j in plane_offsets:
        greet(plane_peer(i, j))
    for o in range(1, counts["gy"]):
        greet({"gy": lax.rem(me["gy"] + o, counts["gy"])})
    for steps in around_me:
        if steps[2] and steps[:2] != (0, 0):
            pl.when(exists(steps))(functools.partial(greet, device(steps)))
    near = {
        a: (me[a] > 0).astype(jnp.int32) + (me[a] < counts[a] - 1).astype(jnp.int32) for a in axes
    }
    greeted = (
        nx * nz - 1 + counts["gy"] - 1 + ((near["gx"] + 1) * (near["gz"] + 1) - 1) * near["gy"]
    )

    row_at = rows_of((LANES, LANES))
    col_at = lanes_of((LANES, LANES))

    def halved(value):
        return (value + 256) // 2 - 128

    def keep(name, where, weight):
        s["lanes"][MATRICES.index(name)] = jnp.where(where, weight, 0.0).astype(jnp.bfloat16)

    keep("c01", col_at == 32 + row_at // 2, 0.125)
    keep("c12", (col_at == 48 + halved(row_at - 32)) & (row_at >= 32) & (row_at < 96), 0.125)
    inside = (row_at >= 18) & (row_at < 110)
    keep("p10", row_at == 32 + col_at // 2, 1.0)
    keep("p21", row_at == 48 + halved(col_at - 32), 1.0)
    for i in range(2):
        keep(f"c23{i}", (col_at == 64 * i + 24 + halved(row_at - 48)) & inside, 0.125)
        keep(f"p32{i}", row_at == 64 * i + 24 + halved(col_at - 48), 1.0)

    def moved(value, name):
        shape = value.shape
        rest = value.reshape(-1, LANES)
        matrix = s["lanes"][MATRICES.index(name)]
        total = None
        for _ in range(3):
            part = rest.astype(jnp.bfloat16)
            rest = rest - part.astype(F32)
            product = jnp.dot(part, matrix, preferred_element_type=F32)
            total = product if total is None else total + product
        return total.reshape(shape)

    def moved_rows(source, target, name, rows):
        def body(i, carry):
            at = pl.ds(i * rows, rows)
            target[at] = moved(source[at], name)
            return carry

        loop(source.shape[0] // rows, body)

    def load_x(x, carry):
        for p in range(PROBES):
            for h in range(2):
                row = h * PROBES + p
                s["flip"][x, pl.ds(row, 8, stride=8), :] = (
                    2.0 * bits_ref[p, x, pl.ds(8 * h, 8), :].astype(F32) - 1.0
                )
        return carry

    def take_x(x, carry):
        s["b0"][x] = s["flip"][x].reshape(8, 8, LANES)
        return carry

    def kappa_x(x, carry):
        for p in range(PROBES):
            for h in range(2):
                row = h * PROBES + p
                s["flip"][x, pl.ds(row, 8, stride=8), :] = kappa_ref[x, pl.ds(8 * h, 8), :]
        return carry

    def pair_sum(field):
        xs, zs = field.shape[0] // 2, field.shape[1] // 2
        split = field.reshape(xs, 2, zs, 2, 8, LANES)
        return (split[:, 0, :, 0] + split[:, 0, :, 1]) + (split[:, 1, :, 0] + split[:, 1, :, 1])

    def diag_x(x, carry):
        kappas = [s["flip"][2 * x + i].reshape(8, 8, LANES) for i in range(2)]
        for i in range(2):
            s["d0"][2 * x + i] = kappas[i] + 6.0
            s["w0"][2 * x + i] = 0.8 / (kappas[i] + 6.0)
        s["t1"][x] = pair_sum(jnp.stack(kappas))[0]
        return carry

    loop(16, load_x)
    loop(16, take_x)
    loop(16, kappa_x)
    loop(8, diag_x)

    def wait_for(count, send, recv):
        ref = s["count"].at[pl.ds(0, count)]
        c = pltpu.make_async_remote_copy(
            src_ref=ref,
            dst_ref=ref,
            send_sem=send,
            recv_sem=recv,
            device_id={"gx": lax.rem(me["gx"] + 1, nx)},
            device_id_type=MESH,
        )
        c.wait_recv()
        c.wait_send()

    def wait_near(count_of, send, recv):
        for x in (1, 2):
            for z in (1, 2):
                for y in (1, 2):
                    here = (near["gx"] == x) & (near["gz"] == z) & (near["gy"] == y)
                    pl.when(here)(functools.partial(wait_for, count_of(x, z, y), send, recv))

    def exchange(which):
        v = s["v0"].at[which]
        got = s["r0"].at[which]
        pack = s["p0"].at[which]
        yin = s["r0y"].at[which]
        yout = s["p0y"].at[which]
        low_rows = rows_of((8, LANES)) < HALF

        def pack_z(x, carry):
            pack[0, x] = jnp.where(low_rows, v[x + 1, 1], swap_halves(v[x + 9, 1]))
            pack[1, x] = jnp.where(low_rows, swap_halves(v[x + 1, 8]), v[x + 9, 8])
            return carry

        loop(8, pack_z, 0, 4)

        group = ((lane + 1) & (LANES - 1)) // 16

        def pack_y(x, carry):
            low, high = carry
            ends = v[x + 1, 1]
            for z in range(1, 8):
                ends = jnp.where(group == z, turn(v[x + 1, 1 + z], 16 * z), ends)
            ends = turn(ends, x)
            low = jnp.where((lane & 15) == x, ends, low)
            high = jnp.where((lane & 15) == ((x + 15) & 15), ends, high)
            return low, high

        zero = jnp.zeros((8, LANES), F32)
        yout[0], yout[1] = loop(16, pack_y, (zero, zero), 8)
        inner = pl.ds(1, 8)
        for steps, src, dst in (
            ((0, -1, 0), pack.at[0], got.at[1]),
            ((0, 1, 0), pack.at[1], got.at[0]),
            ((-1, 0, 0), v.at[1, inner], v.at[17, inner]),
            ((1, 0, 0), v.at[16, inner], v.at[0, inner]),
            ((0, 0, -1), yout.at[0], yin.at[1]),
            ((0, 0, 1), yout.at[1], yin.at[0]),
        ):
            c = pltpu.make_async_remote_copy(
                src_ref=src,
                dst_ref=dst,
                send_sem=s["send"].at[which],
                recv_sem=s["recv"].at[which],
                device_id=device(steps),
                device_id_type=MESH,
            )
            pl.when(exists(steps))(c.start)
        wait_near(lambda x, z, y: 8 * (x + z) + y, s["send"].at[which], s["recv"].at[which])

        def unpack_z(x, carry):
            low, high = got[0, x], got[1, x]
            v[x + 1, 0] = jnp.where(low_rows, low, swap_halves(v[x + 1, 8]))
            v[x + 9, 0] = swap_halves(jnp.where(low_rows, v[x + 9, 8], low))
            v[x + 1, 9] = swap_halves(jnp.where(low_rows, high, v[x + 1, 1]))
            v[x + 9, 9] = jnp.where(low_rows, swap_halves(v[x + 9, 1]), high)
            return carry

        loop(8, unpack_z, 0, 4)

        def unpack_y(x, carry):
            before = turn(yin[0], (LANES + 1 - x) & (LANES - 1))
            after = turn(yin[1], LANES - 1 - x)
            s["ends"][x, 0] = jnp.where((lane & 15) == 0, before, after)
            return carry

        loop(16, unpack_y, 0, 8)

    def neighbours(which, x):
        v = s["v0"].at[which]
        here = v[x + 1, pl.ds(1, 8)]
        total = v[x, pl.ds(1, 8)] + v[x + 2, pl.ds(1, 8)]
        total = total + (v[x + 1, pl.ds(0, 8)] + v[x + 1, pl.ds(2, 8)])
        ends = s["ends"][x, 0]
        ends = jnp.stack([ends] + [turn(ends, LANES - 16 * z) for z in range(1, 8)])
        at_lane = lanes_of((8, 8, LANES))
        before = jnp.where(at_lane == 0, ends, turn(here, 1))
        after = jnp.where(at_lane == LANES - 1, ends, turn(here, LANES - 1))
        return here, total + (before + after)

    def put(which, row, unroll):
        def body(x, carry):
            s["v0"][which, x + 1, pl.ds(1, 8)] = row(x)
            return carry

        loop(16, body, 0, unroll)

    def sweep(which, into):
        def row(x):
            here, around = neighbours(which, x)
            return 0.2 * here + s["w0"][x] * (s["b0"][x] + around)

        put(into, row, 4)

    def start_exchange(level, n, field):
        if level == 1:

            def pack_x(i, carry):
                s["m1"][n, 1, 1, i] = turn(field[2 * i], LANES - 32) + turn(field[2 * i + 1], 32)
                return carry

            loop(4, pack_x, 0, 2)

            def pack_y(x, carry):
                low, high = carry
                for z in range(4):
                    at = 16 * x + 4 * z
                    slot = (lane >> 2) == 4 * x + z
                    value = field[x, z]
                    low = jnp.where(slot, turn(value, (at + LANES - 32) & (LANES - 1)), low)
                    high = jnp.where(slot, turn(value, (at + LANES - 92) & (LANES - 1)), high)
                return low, high

            zero = jnp.zeros((8, LANES), F32)
            low, high = loop(8, pack_y, (zero, zero), 2)
            s["y1out"][n, 0] = high
            s["y1out"][n, 1] = low
        else:
            both = pl.ds(0, 2)
            total = turn(field[0, both], LANES - 48)
            for x in range(1, 4):
                total = total + turn(field[x, both], (32 * x + LANES - 48) % LANES)
            s["m2"][n, 1, 1, 1, both] = total
        for steps in around_me:
            i, j, k = steps
            if level == 2:
                src = s["m2"].at[n, 1, 1, 1, pl.ds(0, 2)]
                dst = s["m2"].at[n, 1 - i, 1 - j, 1 - k, pl.ds(0, 2)]
            elif k:
                side = 0 if k > 0 else 1
                src = s["y1out"].at[n, side]
                dst = s["y1"].at[n, 1 - i, 1 - j, side]
            else:
                if j == 0:
                    part = (pl.ds(0 if i < 0 else 2, 2),)
                elif i == 0:
                    part = (slice(None), pl.ds(0 if j < 0 else 1, 3))
                else:
                    part = (pl.ds(0 if i < 0 else 3, 1), pl.ds(0 if j < 0 else 2, 2))
                src = s["m1"].at[(n, 1, 1, *part)]
                dst = s["m1"].at[(n, 1 - i, 1 - j, *part)]
            c = pltpu.make_async_remote_copy(
                src_ref=src,
                dst_ref=dst,
                send_sem=s["xsend"].at[level - 1, n],
                recv_sem=s["xrecv"].at[level - 1, n],
                device_id=device(steps),
                device_id_type=MESH,
            )
            pl.when(exists(steps))(c.start)

    def finish_exchange(level, n, out):
        def count_of(x, z, y):
            if level == 2:
                return 2 * ((x + 1) * (z + 1) * (y + 1) - 1)
            return 8 * x + 12 * z + 2 * x * z + (x + 1) * (z + 1) * y

        wait_near(count_of, s["xsend"].at[level - 1, n], s["xrecv"].at[level - 1, n])
        low_rows = rows_of((8, LANES)) < HALF
        reach = REACH[level]
        xs, zs = (8, 4) if level == 1 else (4, 2)

        def body(x, carry):
            far = (x + xs - reach) // xs
            at_x = lax.rem(x + xs - reach, xs)

            def source(j, z):
                if level == 1:
                    mid = turn(
                        s["m1"][n, far, j, at_x // 2, z], 32 + 64 * lax.rem(at_x, 2)
                    )
                    at = 4 * (4 * at_x + z)
                    left = turn(s["y1"][n, far, j, 0], lax.rem(28 - at + 2 * LANES, LANES))
                    right = turn(s["y1"][n, far, j, 1], lax.rem(96 - at + 2 * LANES, LANES))
                    value = jnp.where((lane >= 28) & (lane < 32), left, 0.0)
                    value = jnp.where((lane >= 96) & (lane < 100), right, value)
                    return jnp.where((lane >= 32) & (lane < 96), mid, value)
                value = jnp.zeros((8, LANES), F32)
                for k in range(3):
                    start = 16 + 32 * k
                    part = turn(
                        s["m2"][n, far, j, k, z], lax.rem(start + 2 * LANES - 32 * at_x, LANES)
                    )
                    value = jnp.where((lane >= start) & (lane < start + 32), part, value)
                return value

            mine = [source(1, z) for z in range(zs)]
            if level == 1:
                down = [None] + [source(0, z) for z in (1, 2, 3)]
                over = [source(2, z) for z in (0, 1, 2)]
                below = [(down[z], mine[z]) for z in (1, 2, 3)]
                above = [(over[z], mine[z]) for z in (0, 1, 2)]
                outer_low, outer_high = [], []
            else:
                outer_low = [source(0, z) for z in range(2)]
                outer_high = [source(2, z) for z in range(2)]
                below = list(zip(outer_low, mine))
                above = list(zip(outer_high, mine))
            values = list(outer_low)
            values += [swap_halves(jnp.where(low_rows, own, other)) for other, own in below]
            values += mine
            values += [swap_halves(jnp.where(low_rows, other, own)) for other, own in above]
            values += outer_high
            out[x, pl.ds(0, len(values))] = jnp.stack(values)
            return carry

        loop(xs + 2 * reach, body, 0, 2)

    def held_row(src, x, z0, z1):
        inner = pl.ds(z0, z1 - z0)
        here = src[x, inner]
        total = (src[x - 1, inner] + src[x + 1, inner]) + (
            src[x, pl.ds(z0 - 1, z1 - z0)] + src[x, pl.ds(z0 + 1, z1 - z0)]
        )
        return here, total + (turn(here, 1) + turn(here, LANES - 1))

    def held_sweep(level, src, dst, margin, into=0):
        xs, zs = HELD[level]
        coupling = 0.25**level
        z0, z1 = margin, zs - margin

        def body(i, carry):
            x = i + margin
            here, around = held_row(src, x, z0, z1)
            inner = pl.ds(z0, z1 - z0)
            value = 0.2 * here + s[f"w{level}"][x, inner] * (
                s[f"b{level}"][x, inner] + coupling * around
            )
            if into:
                dst[i] = value
            else:
                dst[x, inner] = value
            return carry

        loop(xs - 2 * margin, body, 0, 2)

    def held_down(level):
        xs, zs = HELD[level]
        reach = REACH[level]
        coupling = 0.25**level

        def begin(x, carry):
            s[f"v{level}a"][x] = s[f"w{level}"][x] * s[f"b{level}"][x]
            return carry

        loop(xs, begin)
        held_sweep(level, s[f"v{level}a"], s[f"v{level}b"], 1)
        z0, z1 = reach, zs - reach
        inner = pl.ds(z0, z1 - z0)

        def remainder(x):
            here, around = held_row(s[f"v{level}b"], x + reach, z0, z1)
            return s[f"b{level}"][x + reach, inner] - (
                s[f"d{level}"][x, pl.ds(0, CORE[level][1])] * here - coupling * around
            )

        def body(x, carry):
            pair = pair_sum(jnp.stack([remainder(2 * x), remainder(2 * x + 1)]))[0]
            s[f"f{level + 1}"][x, pl.ds(0, CORE[level][1] // 2)] = pair
            return carry

        loop((xs - 2 * reach) // 2, body, 0, 2)

    def held_up(level, coarse, spread, out, last_margin):
        xs, zs = HELD[level]

        def add(i, carry):
            x = i + 1
            picked = jnp.stack([coarse[spread(x), spread(z)] for z in range(1, zs - 1)])
            s[f"v{level}a"][x, pl.ds(1, zs - 2)] = s[f"v{level}b"][x, pl.ds(1, zs - 2)] + picked
            return carry

        loop(xs - 2, add)
        held_sweep(level, s[f"v{level}a"], s[f"v{level}b"], 2)
        held_sweep(level, s[f"v{level}b"], out, 3, into=1)

    def own_of(level, ref):
        reach = REACH[level]
        xs, zs = HELD[level]
        return ref[pl.ds(reach, xs - 2 * reach), pl.ds(reach, zs - 2 * reach)]

    def coefficients(level, kappa):
        coupling = 6.0 * 0.25**level
        s[f"d{level}"][:, pl.ds(0, CORE[level][1])] = own_of(level, kappa) + coupling

        def body(x, carry):
            k = kappa[x]
            s[f"w{level}"][x] = jnp.where(k > 0.0, 0.8 / (k + coupling), 0.0)
            return carry

        loop(kappa.shape[0], body)

    def plane_start(ref, sems):
        at = ref.at[me["gx"], me["gz"]]
        for i, j in plane_offsets:
            pltpu.make_async_remote_copy(
                src_ref=at,
                dst_ref=at,
                send_sem=s["gsend"].at[sems],
                recv_sem=s["grecv"].at[sems],
                device_id=plane_peer(i, j),
                device_id_type=MESH,
            ).start()

    def plane_finish(sems):
        wait_for(nx * nz - 1, s["gsend"].at[sems], s["grecv"].at[sems])

    def gather_start(n):
        s["g3"][n, me["gx"], me["gz"]] = moved(s["f3"][0, 0], "c230") + moved(s["f3"][1, 0], "c231")
        plane_start(s["g3"].at[n], n)

    def gather_finish(n):
        plane_finish(n)

    def coarsest(n):
        coupling = 0.25**LEVELS
        inner = pl.ds(1, nz)
        s["gv"][0, pl.ds(1, nx), inner] = s["gw"][...] * s["g3"][n]
        glane, grow = lanes_of((nz, 8, LANES)), rows_of((nz, 8, LANES))

        def coarse_sweep(src, dst):
            def body(x, carry):
                here = src[x + 1, inner]
                along_x = turn(
                    here + jnp.where(glane >= 64, src[x, inner], src[x + 2, inner]), 64
                )
                along_z = swap_halves(
                    here
                    + jnp.where(grow >= HALF, src[x + 1, pl.ds(0, nz)], src[x + 1, pl.ds(2, nz)])
                )
                around = (along_x + along_z) + (turn(here, 1) + turn(here, LANES - 1))
                dst[x + 1, inner] = 0.2 * here + s["gw"][x] * (s["g3"][n, x] + coupling * around)
                return carry

            loop(nx, body, 0, nx)

        for i in range(COARSE_SWEEPS - 1):
            coarse_sweep(s["gv"].at[i % 2], s["gv"].at[1 - i % 2])
        done = s["gv"].at[(COARSE_SWEEPS - 1) % 2]
        low_rows = rows_of((8, LANES)) < HALF
        near_me = []
        for i in range(3):
            below, mine, above = (done[i + me["gx"], j + me["gz"]] for j in range(3))
            near_me += [
                below,
                swap_halves(jnp.where(low_rows, mine, below)),
                mine,
                swap_halves(jnp.where(low_rows, above, mine)),
                above,
            ]
        near_me = jnp.stack(near_me)
        for i in range(2):
            spread = moved(near_me, f"p32{i}")
            for x in range(3):
                s["e3"][2 * x + i, pl.ds(0, 5)] = spread[5 * x : 5 * x + 5]

    def sum_start(dots, n):
        packed = jnp.zeros((8, LANES), F32)
        for j, d in enumerate(dots):
            packed = jnp.where(lane == j, jnp.sum(d, axis=-1, keepdims=True), packed)
        s["a1"][n, me["gx"], me["gz"]] = packed + swap_halves(packed)
        plane_start(s["a1"].at[n], 3 + n)

    def folded(value):
        while value.shape[0] > 1:
            value = value[: value.shape[0] // 2] + value[value.shape[0] // 2 :]
        return value[0]

    def sum_middle(n):
        plane_finish(3 + n)
        s["a2"][n, me["gy"]] = folded(s["a1"][n].reshape(nx * nz, 8, LANES))
        at = s["a2"].at[n, me["gy"]]
        for o in range(1, counts["gy"]):
            pltpu.make_async_remote_copy(
                src_ref=at,
                dst_ref=at,
                send_sem=s["gsend"].at[5 + n],
                recv_sem=s["grecv"].at[5 + n],
                device_id={"gy": wrapped("gy", o)},
                device_id_type=MESH,
            ).start()

    def sum_finish(n, count):
        wait_for(counts["gy"] - 1, s["gsend"].at[5 + n], s["grecv"].at[5 + n])
        total = folded(s["a2"][n])
        return [total[:, j : j + 1] for j in range(count)]

    moved_rows(s["t1"], s["f1"], "c01", 4)

    def pair_up(x, carry):
        s["f2"][x, pl.ds(0, 2)] = pair_sum(s["f1"][pl.ds(2 * x, 2)])[0]
        return carry

    loop(4, pair_up)
    pl.semaphore_wait(barrier, greeted)
    start_exchange(1, 0, s["f1"])
    s["t3"][:, pl.ds(0, 2)] = moved(s["f2"][:, pl.ds(0, 2)], "c12")
    start_exchange(2, 0, s["t3"])

    def coefficients_held():
        finish_exchange(1, 0, s["v1a"])
        coefficients(1, s["v1a"])
        finish_exchange(2, 0, s["v2a"])
        coefficients(2, s["v2a"])
        s["f3"][:, pl.ds(0, 1)] = pair_sum(own_of(2, s["v2a"]))
        gather_start(0)

    def coarse_coefficients():
        gather_finish(0)
        kappa_3 = s["g3"][0]
        s["gw"][...] = jnp.where(kappa_3 > 0.0, 0.8 / (kappa_3 + 6.0 * 0.25**LEVELS), 0.0)

    def below(n):
        def remainder(x):
            here, around = neighbours(1, x)
            return s["b0"][x] - (s["d0"][x] * here - around)

        def body(x, carry):
            s["t1"][x] = pair_sum(jnp.stack([remainder(2 * x), remainder(2 * x + 1)]))[0]
            return carry

        loop(8, body, 0, 2)
        moved_rows(s["t1"], s["f1"], "c01", 4)
        start_exchange(1, n, s["f1"])
        pl.when(n == 1)(coefficients_held)
        pl.when(n == 2)(lambda: sum_middle(0))
        finish_exchange(1, n, s["b1"])
        held_down(1)
        s["t3"][:, pl.ds(0, 2)] = moved(s["f2"][:, pl.ds(0, 2)], "c12")
        start_exchange(2, n, s["t3"])
        finish_exchange(2, n, s["b2"])
        held_down(2)
        pl.when(n == 1)(coarse_coefficients)
        gather_start(n)
        gather_finish(n)
        coarsest(n)
        held_up(2, s["e3"], lambda i: i // 2, s["e2"], 3)
        moved_rows(s["e2"], s["t2"], "p21", 3)
        held_up(1, s["t2"], lambda i: (i - 1) // 2, s["e1"], 3)
        moved_rows(s["e1"], s["t1"], "p10", 4)

    def corrected(x):
        e = s["t1"][x // 2]
        return s["v0"][1, x + 1, pl.ds(1, 8)] + jnp.stack([e, e], axis=1).reshape(8, 8, LANES)

    def cycle(n, carry):
        put(0, lambda x: s["w0"][x] * s["b0"][x], 2)
        exchange(0)
        sweep(0, 1)
        exchange(1)
        below(n)
        put(0, corrected, 2)
        exchange(0)
        sweep(0, 1)
        exchange(1)
        sweep(1, 2)
        exchange(2)

        def apply(x, c):
            here, around = neighbours(2, x)
            q = s["d0"][x] * here - around
            s["z"][n - 1, x] = here
            s["q"][n - 1, x] = q
            b = s["b0"][x]

            @pl.when(n == 1)
            def _():
                s["flip"][x] = b.reshape(64, LANES)
                s["b0"][x] = q

            return c[0] + folded(b * here), c[1] + folded(here * q)

        dots = loop(16, apply, (jnp.zeros((8, LANES), F32),) * 2, 2)
        pl.when(n == 1)(lambda: sum_start(dots, 0))
        return carry

    lax.fori_loop(1, 3, cycle, 0)
    rz, zq = sum_finish(0, 2)
    step = jnp.broadcast_to(rz / zq, (8, LANES))
    zero = jnp.zeros((8, LANES), F32)

    def dots_second(x, c):
        q0 = s["q"][0, x]
        z0 = s["z"][0, x]
        r1 = s["flip"][x].reshape(8, 8, LANES) - step * q0
        z1 = z0 - step * s["z"][1, x]
        q1 = q0 - step * s["q"][1, x]
        s["z"][1, x] = z1
        pairs = (
            (r1, z1),
            (z1, q1),
            (z1, q0),
            (z0, q1),
            (r1, r1),
            (r1, q1),
            (r1, q0),
            (q1, q1),
            (q1, q0),
            (q0, q0),
        )
        return tuple(t + folded(u * v) for t, (u, v) in zip(c, pairs))

    sum_start(loop(16, dots_second, (zero,) * 10), 1)
    sum_middle(1)
    r1z1, z1q1, z1q0, z0q1, r1r1, r1q1, r1q0, q1q1, q1q0, q0q0 = sum_finish(1, 10)
    ratio = r1z1 / rz
    step2 = r1z1 / (z1q1 + ratio * (z1q0 + z0q1) + ratio * ratio * zq)
    squares = (
        r1r1
        - 2.0 * step2 * (r1q1 + ratio * r1q0)
        + step2 * step2 * (q1q1 + 2.0 * ratio * q1q0 + ratio * ratio * q0q0)
    )
    norm = jnp.sqrt(jnp.maximum(squares, 0.0) * (1.0 / cells))
    norm_ref[...] = jnp.broadcast_to(norm, (8, LANES))
    along_z0 = jnp.broadcast_to(step + step2 * ratio, (8, LANES))
    along_z1 = jnp.broadcast_to(step2, (8, LANES))

    def finish(x, c):
        value = along_z0 * s["z"][0, x] + along_z1 * s["z"][1, x]
        s["flip"][x] = value.reshape(64, LANES)
        return c

    loop(16, finish)

    def write(x, c):
        for p in range(PROBES):
            for h in range(2):
                row = h * PROBES + p
                solution_ref[p, x, pl.ds(8 * h, 8), :] = s["flip"][x, pl.ds(row, 8, stride=8), :]
        return c

    loop(16, write)


MATRICES = ("c01", "c12", "p10", "p21", "c230", "c231", "p320", "p321")


def scratch_list():
    def fields(*lead):
        return pltpu.VMEM((*lead[:-1], (lead[-1] + 3) // 4 * 4, 8, LANES), F32)

    out = {"flip": pltpu.VMEM((16, 64, LANES), F32), "lanes": pltpu.VMEM((8, LANES, LANES), jnp.bfloat16)}
    for name in ("b0", "d0", "w0"):
        out[name] = fields(16, 8)
    out["v0"] = fields(3, 18, 10)
    out["r0"] = fields(3, 2, 8)
    out["p0"] = fields(3, 2, 8)
    out["r0y"] = fields(3, 2)
    out["p0y"] = fields(3, 2)
    out["ends"] = fields(16, 1)
    out["f1"] = fields(8, 4)
    out["f2"] = fields(4, 2)
    out["f3"] = fields(2, 1)
    out["t3"] = fields(4, 2)
    for level in (1, 2):
        for name in (f"b{level}", f"w{level}", f"v{level}a", f"v{level}b"):
            out[name] = fields(*HELD[level])
        out[f"d{level}"] = fields(*CORE[level])
    out["e1"] = fields(8, 4)
    out["t1"] = fields(8, 4)
    out["e2"] = fields(6, 4)
    out["t2"] = fields(6, 4)
    out["e3"] = fields(6, 5)
    out["m1"] = fields(3, 3, 3, 4, 4)
    out["y1"] = fields(3, 3, 3, 2)
    out["y1out"] = fields(3, 2)
    out["m2"] = fields(3, 3, 3, 3, 2)
    out["z"] = fields(2, 16, 8)
    out["q"] = fields(2, 16, 8)
    out["g3"] = fields(3, 8, 4)
    out["a1"] = fields(2, 8, 4)
    out["a2"] = fields(2, 4)
    out["gw"] = fields(8, 4)
    out["gv"] = fields(2, 10, 6)
    out["count"] = fields(72)
    out["send"] = pltpu.SemaphoreType.DMA((3,))
    out["recv"] = pltpu.SemaphoreType.DMA((3,))
    out["xsend"] = pltpu.SemaphoreType.DMA((2, 3))
    out["xrecv"] = pltpu.SemaphoreType.DMA((2, 3))
    out["gsend"] = pltpu.SemaphoreType.DMA((7,))
    out["grecv"] = pltpu.SemaphoreType.DMA((7,))
    return out


def solution(mesh):
    counts = {a: mesh.shape[a] for a in ("gx", "gy", "gz")}

    def step(kappa_sq, probe_bits):
        cells = probe_bits[0].size * counts["gx"] * counts["gy"] * counts["gz"]
        whole, norms = pl.pallas_call(
            functools.partial(kernel_body, counts, cells),
            out_shape=(
                jax.ShapeDtypeStruct(probe_bits.shape, F32),
                jax.ShapeDtypeStruct((8, LANES), F32),
            ),
            in_specs=[pl.BlockSpec(memory_space=pltpu.VMEM)] * 2,
            out_specs=(pl.BlockSpec(memory_space=pltpu.VMEM),) * 2,
            scratch_shapes=list(scratch_list().values()),
            compiler_params=pltpu.CompilerParams(
                collective_id=0, has_side_effects=True, vmem_limit_bytes=40 * 2**20
            ),
            name="solve",
        )(kappa_sq, probe_bits)
        return whole, norms[:PROBES, 0]

    return jax.shard_map(
        step,
        mesh=mesh,
        in_specs=(P("gx", "gz", "gy"), P(None, "gx", "gz", "gy")),
        out_specs=(P(None, "gx", "gz", "gy"), P()),
        check_vma=False,
    )
```

```python
import functools

import jax
import jax.numpy as jnp
from jax import lax
from jax.experimental import pallas as pl
from jax.experimental.pallas import tpu as pltpu
from jax.sharding import PartitionSpec as P

LEVELS = 3
COARSE_SWEEPS = 8
PROBES = 4
LANES = 128
HALF = 4
MESH = pl.DeviceIdType.MESH
F32 = jnp.float32

OWN = {1: 32, 2: 48, 3: 24}
REACH = {1: 3, 2: 4}
HELD = {1: (14, 10), 2: (12, 10)}
CORE = {1: (8, 4), 2: (4, 2)}


def lanes_of(shape):
    return lax.broadcasted_iota(jnp.int32, shape, len(shape) - 1)


def rows_of(shape):
    return lax.broadcasted_iota(jnp.int32, shape, len(shape) - 2)


def turn(value, shift):
    return pltpu.roll(value, shift, len(value.shape) - 1)


def swap_halves(value):
    return pltpu.roll(value, HALF, len(value.shape) - 2)


def kernel_body(counts, cells, kappa_ref, bits_ref, solution_ref, norm_ref, *scratch):
    s = dict(zip(scratch_list(), scratch))
    axes = ("gx", "gz", "gy")
    me = {a: lax.axis_index(a) for a in axes}
    nx, nz = counts["gx"], counts["gz"]
    lane = lanes_of((8, LANES))

    def loop(count, body, init=0, unroll=1):
        return lax.fori_loop(0, count, body, init, unroll=count)

    def exists(steps):
        ok = None
        for a, d in zip(axes, steps):
            if d:
                one = me[a] > 0 if d < 0 else me[a] < counts[a] - 1
                ok = one if ok is None else ok & one
        return ok

    def device(steps):
        return {a: me[a] + d for a, d in zip(axes, steps)}

    around_me = [
        (i, j, k) for i in (-1, 0, 1) for j in (-1, 0, 1) for k in (-1, 0, 1) if (i, j, k) != (0, 0, 0)
    ]

    def clear_faces(i, carry):
        for x in (0, 17):
            s["v0"][i, x] = jnp.zeros(s["v0"].shape[2:], F32)
        for name in ("r0", "r0y"):
            s[name][i] = jnp.zeros(s[name].shape[1:], F32)
        return carry

    loop(3, clear_faces)
    for name in ("m1", "y1", "m2"):
        ref = s[name]

        def clear(i, carry, ref=ref):
            for j in range(3):
                ref[i // 3, lax.rem(i, 3), j] = jnp.zeros(ref.shape[3:], F32)
            return carry

        loop(9, clear)

    def clear_coarse(i, carry):
        s["gv"][i // 10, lax.rem(i, 10)] = jnp.zeros(s["gv"].shape[2:], F32)
        return carry

    loop(20, clear_coarse)

    barrier = pltpu.get_barrier_semaphore()

    def greet(to):
        pl.semaphore_signal(barrier, inc=1, device_id=to, device_id_type=MESH)

    def wrapped(a, step):
        to = me[a] + step
        return jnp.where(to >= counts[a], to - counts[a], to)

    def plane_peer(i, j):
        return {"gx": wrapped("gx", i), "gz": wrapped("gz", j)}

    plane_offsets = sorted(
        ((i, j) for i in range(nx) for j in range(nz) if (i, j) != (0, 0)),
        key=lambda at: -min(at[0], nx - at[0]) - 2 * min(at[1], nz - at[1]),
    )
    for i, j in plane_offsets:
        greet(plane_peer(i, j))
    for o in range(1, counts["gy"]):
        greet({"gy": lax.rem(me["gy"] + o, counts["gy"])})
    for steps in around_me:
        if steps[2] and steps[:2] != (0, 0):
            pl.when(exists(steps))(functools.partial(greet, device(steps)))
    near = {
        a: (me[a] > 0).astype(jnp.int32) + (me[a] < counts[a] - 1).astype(jnp.int32) for a in axes
    }
    greeted = (
        nx * nz - 1 + counts["gy"] - 1 + ((near["gx"] + 1) * (near["gz"] + 1) - 1) * near["gy"]
    )

    row_at = rows_of((LANES, LANES))
    col_at = lanes_of((LANES, LANES))

    def halved(value):
        return (value + 256) // 2 - 128

    def keep(name, where, weight):
        s["lanes"][MATRICES.index(name)] = jnp.where(where, weight, 0.0).astype(jnp.bfloat16)

    keep("c01", col_at == 32 + row_at // 2, 0.125)
    keep("c12", (col_at == 48 + halved(row_at - 32)) & (row_at >= 32) & (row_at < 96), 0.125)
    inside = (row_at >= 18) & (row_at < 110)
    keep("p10", row_at == 32 + col_at // 2, 1.0)
    keep("p21", row_at == 48 + halved(col_at - 32), 1.0)
    for i in range(2):
        keep(f"c23{i}", (col_at == 64 * i + 24 + halved(row_at - 48)) & inside, 0.125)
        keep(f"p32{i}", row_at == 64 * i + 24 + halved(col_at - 48), 1.0)

    def moved(value, name):
        shape = value.shape
        rest = value.reshape(-1, LANES)
        matrix = s["lanes"][MATRICES.index(name)]
        total = None
        for _ in range(3):
            part = rest.astype(jnp.bfloat16)
            rest = rest - part.astype(F32)
            product = jnp.dot(part, matrix, preferred_element_type=F32)
            total = product if total is None else total + product
        return total.reshape(shape)

    def moved_rows(source, target, name, rows):
        def body(i, carry):
            at = pl.ds(i * rows, rows)
            target[at] = moved(source[at], name)
            return carry

        loop(source.shape[0] // rows, body)

    def load_x(x, carry):
        for p in range(PROBES):
            for h in range(2):
                row = h * PROBES + p
                s["flip"][x, pl.ds(row, 8, stride=8), :] = (
                    2.0 * bits_ref[p, x, pl.ds(8 * h, 8), :].astype(F32) - 1.0
                )
        return carry

    def take_x(x, carry):
        s["b0"][x] = s["flip"][x].reshape(8, 8, LANES)
        return carry

    def kappa_x(x, carry):
        for p in range(PROBES):
            for h in range(2):
                row = h * PROBES + p
                s["flip"][x, pl.ds(row, 8, stride=8), :] = kappa_ref[x, pl.ds(8 * h, 8), :]
        return carry

    def pair_sum(field):
        xs, zs = field.shape[0] // 2, field.shape[1] // 2
        split = field.reshape(xs, 2, zs, 2, 8, LANES)
        return (split[:, 0, :, 0] + split[:, 0, :, 1]) + (split[:, 1, :, 0] + split[:, 1, :, 1])

    def diag_x(x, carry):
        kappas = [s["flip"][2 * x + i].reshape(8, 8, LANES) for i in range(2)]
        for i in range(2):
            s["d0"][2 * x + i] = kappas[i] + 6.0
            s["w0"][2 * x + i] = 0.8 / (kappas[i] + 6.0)
        s["t1"][x] = pair_sum(jnp.stack(kappas))[0]
        return carry

    loop(16, load_x)
    loop(16, take_x)
    loop(16, kappa_x)
    loop(8, diag_x)

    def wait_for(count, send, recv):
        ref = s["count"].at[pl.ds(0, count)]
        c = pltpu.make_async_remote_copy(
            src_ref=ref,
            dst_ref=ref,
            send_sem=send,
            recv_sem=recv,
            device_id={"gx": lax.rem(me["gx"] + 1, nx)},
            device_id_type=MESH,
        )
        c.wait_recv()
        c.wait_send()

    def wait_near(count_of, send, recv):
        for x in (1, 2):
            for z in (1, 2):
                for y in (1, 2):
                    here = (near["gx"] == x) & (near["gz"] == z) & (near["gy"] == y)
                    pl.when(here)(functools.partial(wait_for, count_of(x, z, y), send, recv))

    def exchange(which, cell, meanwhile=None):
        v = s["v0"].at[which]
        got = s["r0"].at[which]
        pack = s["p0"].at[which]
        yin = s["r0y"].at[which]
        yout = s["p0y"].at[which]
        low_rows = rows_of((8, LANES)) < HALF
        inner = pl.ds(1, 8)

        def send(steps, src, dst):
            c = pltpu.make_async_remote_copy(
                src_ref=src,
                dst_ref=dst,
                send_sem=s["send"].at[which],
                recv_sem=s["recv"].at[which],
                device_id=device(steps),
                device_id_type=MESH,
            )
            pl.when(exists(steps))(c.start)

        def fill_z(x, carry):
            v[x + 1, pl.ds(1, 1)] = cell(x, 0, 1)
            v[x + 1, pl.ds(8, 1)] = cell(x, 7, 8)
            return carry

        loop(16, fill_z)

        def pack_z(x, carry):
            pack[0, x] = jnp.where(low_rows, v[x + 1, 1], swap_halves(v[x + 9, 1]))
            pack[1, x] = jnp.where(low_rows, swap_halves(v[x + 1, 8]), v[x + 9, 8])
            return carry

        loop(8, pack_z)
        send((0, -1, 0), pack.at[0], got.at[1])
        send((0, 1, 0), pack.at[1], got.at[0])
        for x in (0, 15):
            v[x + 1, pl.ds(2, 6)] = cell(x, 1, 7)
        send((-1, 0, 0), v.at[1, inner], v.at[17, inner])
        send((1, 0, 0), v.at[16, inner], v.at[0, inner])

        group = ((lane + 1) & (LANES - 1)) // 16

        def fill(x, carry):
            v[x + 2, pl.ds(2, 6)] = cell(x + 1, 1, 7)
            return carry

        loop(14, fill)

        def pack_y(x, carry):
            low, high = carry
            ends = v[x + 1, 1]
            for z in range(1, 8):
                ends = jnp.where(group == z, turn(v[x + 1, 1 + z], 16 * z), ends)
            ends = turn(ends, x)
            low = jnp.where((lane & 15) == x, ends, low)
            high = jnp.where((lane & 15) == ((x + 15) & 15), ends, high)
            return low, high

        zero = jnp.zeros((8, LANES), F32)
        yout[0], yout[1] = loop(16, pack_y, (zero, zero))
        send((0, 0, -1), yout.at[0], yin.at[1])
        send((0, 0, 1), yout.at[1], yin.at[0])
        if meanwhile is not None:
            meanwhile()
        wait_near(lambda x, z, y: 8 * (x + z) + y, s["send"].at[which], s["recv"].at[which])

        def unpack_z(x, carry):
            low, high = got[0, x], got[1, x]
            v[x + 1, 0] = jnp.where(low_rows, low, swap_halves(v[x + 1, 8]))
            v[x + 9, 0] = swap_halves(jnp.where(low_rows, v[x + 9, 8], low))
            v[x + 1, 9] = swap_halves(jnp.where(low_rows, high, v[x + 1, 1]))
            v[x + 9, 9] = jnp.where(low_rows, swap_halves(v[x + 9, 1]), high)
            return carry

        loop(8, unpack_z, 0, 4)

        def unpack_y(x, carry):
            before = turn(yin[0], (LANES + 1 - x) & (LANES - 1))
            after = turn(yin[1], LANES - 1 - x)
            s["ends"][x, 0] = jnp.where((lane & 15) == 0, before, after)
            return carry

        loop(16, unpack_y, 0, 8)

    def neighbours(which, x, z0=0, z1=8):
        v = s["v0"].at[which]
        inner = pl.ds(1 + z0, z1 - z0)
        here = v[x + 1, inner]
        total = v[x, inner] + v[x + 2, inner]
        total = total + (v[x + 1, pl.ds(z0, z1 - z0)] + v[x + 1, pl.ds(z0 + 2, z1 - z0)])
        ends = s["ends"][x, 0]
        ends = jnp.stack([turn(ends, LANES - 16 * z) if z else ends for z in range(z0, z1)])
        at_lane = lanes_of((z1 - z0, 8, LANES))
        before = jnp.where(at_lane == 0, ends, turn(here, 1))
        after = jnp.where(at_lane == LANES - 1, ends, turn(here, LANES - 1))
        return here, total + (before + after)

    def swept(which):
        def cell(x, z0, z1):
            inner = pl.ds(z0, z1 - z0)
            here, around = neighbours(which, x, z0, z1)
            return 0.2 * here + s["w0"][x, inner] * (s["b0"][x, inner] + around)

        return cell

    def start_exchange(level, n, field):
        if level == 1:

            def pack_x(i, carry):
                s["m1"][n, 1, 1, i] = turn(field[2 * i], LANES - 32) + turn(field[2 * i + 1], 32)
                return carry

            loop(4, pack_x, 0, 2)

            def pack_y(x, carry):
                low, high = carry
                for z in range(4):
                    at = 16 * x + 4 * z
                    slot = (lane >> 2) == 4 * x + z
                    value = field[x, z]
                    low = jnp.where(slot, turn(value, (at + LANES - 32) & (LANES - 1)), low)
                    high = jnp.where(slot, turn(value, (at + LANES - 92) & (LANES - 1)), high)
                return low, high

            zero = jnp.zeros((8, LANES), F32)
            low, high = loop(8, pack_y, (zero, zero), 2)
            s["y1out"][n, 0] = high
            s["y1out"][n, 1] = low
        else:
            both = pl.ds(0, 2)
            total = turn(field[0, both], LANES - 48)
            for x in range(1, 4):
                total = total + turn(field[x, both], (32 * x + LANES - 48) % LANES)
            s["m2"][n, 1, 1, 1, both] = total
        for steps in around_me:
            i, j, k = steps
            if level == 2:
                src = s["m2"].at[n, 1, 1, 1, pl.ds(0, 2)]
                dst = s["m2"].at[n, 1 - i, 1 - j, 1 - k, pl.ds(0, 2)]
            elif k:
                side = 0 if k > 0 else 1
                src = s["y1out"].at[n, side]
                dst = s["y1"].at[n, 1 - i, 1 - j, side]
            else:
                if j == 0:
                    part = (pl.ds(0 if i < 0 else 2, 2),)
                elif i == 0:
                    part = (slice(None), pl.ds(0 if j < 0 else 1, 3))
                else:
                    part = (pl.ds(0 if i < 0 else 3, 1), pl.ds(0 if j < 0 else 2, 2))
                src = s["m1"].at[(n, 1, 1, *part)]
                dst = s["m1"].at[(n, 1 - i, 1 - j, *part)]
            c = pltpu.make_async_remote_copy(
                src_ref=src,
                dst_ref=dst,
                send_sem=s["xsend"].at[level - 1, n],
                recv_sem=s["xrecv"].at[level - 1, n],
                device_id=device(steps),
                device_id_type=MESH,
            )
            pl.when(exists(steps))(c.start)

    def finish_exchange(level, n, out):
        def count_of(x, z, y):
            if level == 2:
                return 2 * ((x + 1) * (z + 1) * (y + 1) - 1)
            return 8 * x + 12 * z + 2 * x * z + (x + 1) * (z + 1) * y

        wait_near(count_of, s["xsend"].at[level - 1, n], s["xrecv"].at[level - 1, n])
        low_rows = rows_of((8, LANES)) < HALF
        reach = REACH[level]
        xs, zs = (8, 4) if level == 1 else (4, 2)

        def body(x, carry):
            far = (x + xs - reach) // xs
            at_x = lax.rem(x + xs - reach, xs)

            def source(j, z):
                if level == 1:
                    mid = turn(
                        s["m1"][n, far, j, at_x // 2, z], 32 + 64 * lax.rem(at_x, 2)
                    )
                    at = 4 * (4 * at_x + z)
                    left = turn(s["y1"][n, far, j, 0], lax.rem(28 - at + 2 * LANES, LANES))
                    right = turn(s["y1"][n, far, j, 1], lax.rem(96 - at + 2 * LANES, LANES))
                    value = jnp.where((lane >= 28) & (lane < 32), left, 0.0)
                    value = jnp.where((lane >= 96) & (lane < 100), right, value)
                    return jnp.where((lane >= 32) & (lane < 96), mid, value)
                value = jnp.zeros((8, LANES), F32)
                for k in range(3):
                    start = 16 + 32 * k
                    part = turn(
                        s["m2"][n, far, j, k, z], lax.rem(start + 2 * LANES - 32 * at_x, LANES)
                    )
                    value = jnp.where((lane >= start) & (lane < start + 32), part, value)
                return value

            mine = [source(1, z) for z in range(zs)]
            if level == 1:
                down = [None] + [source(0, z) for z in (1, 2, 3)]
                over = [source(2, z) for z in (0, 1, 2)]
                below = [(down[z], mine[z]) for z in (1, 2, 3)]
                above = [(over[z], mine[z]) for z in (0, 1, 2)]
                outer_low, outer_high = [], []
            else:
                outer_low = [source(0, z) for z in range(2)]
                outer_high = [source(2, z) for z in range(2)]
                below = list(zip(outer_low, mine))
                above = list(zip(outer_high, mine))
            values = list(outer_low)
            values += [swap_halves(jnp.where(low_rows, own, other)) for other, own in below]
            values += mine
            values += [swap_halves(jnp.where(low_rows, other, own)) for other, own in above]
            values += outer_high
            out[x, pl.ds(0, len(values))] = jnp.stack(values)
            return carry

        loop(xs + 2 * reach, body, 0, 2)

    def held_row(src, x, z0, z1):
        inner = pl.ds(z0, z1 - z0)
        here = src[x, inner]
        total = (src[x - 1, inner] + src[x + 1, inner]) + (
            src[x, pl.ds(z0 - 1, z1 - z0)] + src[x, pl.ds(z0 + 1, z1 - z0)]
        )
        return here, total + (turn(here, 1) + turn(here, LANES - 1))

    def held_sweep(level, src, dst, margin, into=0):
        xs, zs = HELD[level]
        coupling = 0.25**level
        z0, z1 = margin, zs - margin

        def body(i, carry):
            x = i + margin
            here, around = held_row(src, x, z0, z1)
            inner = pl.ds(z0, z1 - z0)
            value = 0.2 * here + s[f"w{level}"][x, inner] * (
                s[f"b{level}"][x, inner] + coupling * around
            )
            if into:
                dst[i] = value
            else:
                dst[x, inner] = value
            return carry

        loop(xs - 2 * margin, body, 0, 2)

    def held_down(level):
        xs, zs = HELD[level]
        reach = REACH[level]
        coupling = 0.25**level

        def begin(x, carry):
            s[f"v{level}a"][x] = s[f"w{level}"][x] * s[f"b{level}"][x]
            return carry

        loop(xs, begin)
        held_sweep(level, s[f"v{level}a"], s[f"v{level}b"], 1)
        z0, z1 = reach, zs - reach
        inner = pl.ds(z0, z1 - z0)

        def remainder(x):
            here, around = held_row(s[f"v{level}b"], x + reach, z0, z1)
            return s[f"b{level}"][x + reach, inner] - (
                s[f"d{level}"][x, pl.ds(0, CORE[level][1])] * here - coupling * around
            )

        def body(x, carry):
            pair = pair_sum(jnp.stack([remainder(2 * x), remainder(2 * x + 1)]))[0]
            s[f"f{level + 1}"][x, pl.ds(0, CORE[level][1] // 2)] = pair
            return carry

        loop((xs - 2 * reach) // 2, body, 0, 2)

    def held_up(level, coarse, spread, out, last_margin):
        xs, zs = HELD[level]

        def add(i, carry):
            x = i + 1
            picked = jnp.stack([coarse[spread(x), spread(z)] for z in range(1, zs - 1)])
            s[f"v{level}a"][x, pl.ds(1, zs - 2)] = s[f"v{level}b"][x, pl.ds(1, zs - 2)] + picked
            return carry

        loop(xs - 2, add)
        held_sweep(level, s[f"v{level}a"], s[f"v{level}b"], 2)
        held_sweep(level, s[f"v{level}b"], out, 3, into=1)

    def own_of(level, ref):
        reach = REACH[level]
        xs, zs = HELD[level]
        return ref[pl.ds(reach, xs - 2 * reach), pl.ds(reach, zs - 2 * reach)]

    def coefficients(level, kappa):
        coupling = 6.0 * 0.25**level
        s[f"d{level}"][:, pl.ds(0, CORE[level][1])] = own_of(level, kappa) + coupling

        def body(x, carry):
            k = kappa[x]
            s[f"w{level}"][x] = jnp.where(k > 0.0, 0.8 / (k + coupling), 0.0)
            return carry

        loop(kappa.shape[0], body)

    def plane_start(ref, sems):
        at = ref.at[me["gx"], me["gz"]]
        for i, j in plane_offsets:
            pltpu.make_async_remote_copy(
                src_ref=at,
                dst_ref=at,
                send_sem=s["gsend"].at[sems],
                recv_sem=s["grecv"].at[sems],
                device_id=plane_peer(i, j),
                device_id_type=MESH,
            ).start()

    def plane_finish(sems):
        wait_for(nx * nz - 1, s["gsend"].at[sems], s["grecv"].at[sems])

    def gather_start(n):
        s["g3"][n, me["gx"], me["gz"]] = moved(s["f3"][0, 0], "c230") + moved(s["f3"][1, 0], "c231")
        plane_start(s["g3"].at[n], n)

    def gather_finish(n):
        plane_finish(n)

    def coarsest(n):
        coupling = 0.25**LEVELS
        inner = pl.ds(1, nz)
        s["gv"][0, pl.ds(1, nx), inner] = s["gw"][...] * s["g3"][n]
        glane, grow = lanes_of((nz, 8, LANES)), rows_of((nz, 8, LANES))

        def coarse_sweep(src, dst):
            def body(x, carry):
                here = src[x + 1, inner]
                along_x = turn(
                    here + jnp.where(glane >= 64, src[x, inner], src[x + 2, inner]), 64
                )
                along_z = swap_halves(
                    here
                    + jnp.where(grow >= HALF, src[x + 1, pl.ds(0, nz)], src[x + 1, pl.ds(2, nz)])
                )
                around = (along_x + along_z) + (turn(here, 1) + turn(here, LANES - 1))
                dst[x + 1, inner] = 0.2 * here + s["gw"][x] * (s["g3"][n, x] + coupling * around)
                return carry

            loop(nx, body, 0, nx)

        for i in range(COARSE_SWEEPS - 1):
            coarse_sweep(s["gv"].at[i % 2], s["gv"].at[1 - i % 2])
        done = s["gv"].at[(COARSE_SWEEPS - 1) % 2]
        low_rows = rows_of((8, LANES)) < HALF
        near_me = []
        for i in range(3):
            below, mine, above = (done[i + me["gx"], j + me["gz"]] for j in range(3))
            near_me += [
                below,
                swap_halves(jnp.where(low_rows, mine, below)),
                mine,
                swap_halves(jnp.where(low_rows, above, mine)),
                above,
            ]
        near_me = jnp.stack(near_me)
        for i in range(2):
            spread = moved(near_me, f"p32{i}")
            for x in range(3):
                s["e3"][2 * x + i, pl.ds(0, 5)] = spread[5 * x : 5 * x + 5]

    def sum_start(dots, n):
        packed = jnp.zeros((8, LANES), F32)
        for j, d in enumerate(dots):
            packed = jnp.where(lane == j, jnp.sum(d, axis=-1, keepdims=True), packed)
        s["a1"][n, me["gx"], me["gz"]] = packed + swap_halves(packed)
        plane_start(s["a1"].at[n], 3 + n)

    def folded(value):
        while value.shape[0] > 1:
            value = value[: value.shape[0] // 2] + value[value.shape[0] // 2 :]
        return value[0]

    def sum_middle(n):
        plane_finish(3 + n)
        s["a2"][n, me["gy"]] = folded(s["a1"][n].reshape(nx * nz, 8, LANES))
        at = s["a2"].at[n, me["gy"]]
        for o in range(1, counts["gy"]):
            pltpu.make_async_remote_copy(
                src_ref=at,
                dst_ref=at,
                send_sem=s["gsend"].at[5 + n],
                recv_sem=s["grecv"].at[5 + n],
                device_id={"gy": wrapped("gy", o)},
                device_id_type=MESH,
            ).start()

    def sum_finish(n, count):
        wait_for(counts["gy"] - 1, s["gsend"].at[5 + n], s["grecv"].at[5 + n])
        total = folded(s["a2"][n])
        return [total[:, j : j + 1] for j in range(count)]

    pl.semaphore_wait(barrier, greeted)

    def coefficients_held():
        finish_exchange(1, 0, s["v1a"])
        coefficients(1, s["v1a"])
        finish_exchange(2, 0, s["v2a"])
        coefficients(2, s["v2a"])
        s["f3"][:, pl.ds(0, 1)] = pair_sum(own_of(2, s["v2a"]))
        gather_start(0)

    def coarse_coefficients():
        gather_finish(0)
        kappa_3 = s["g3"][0]
        s["gw"][...] = jnp.where(kappa_3 > 0.0, 0.8 / (kappa_3 + 6.0 * 0.25**LEVELS), 0.0)

    def below(n):
        def remainder(x):
            here, around = neighbours(1, x)
            return s["b0"][x] - (s["d0"][x] * here - around)

        def body(x, carry):
            s["t1"][x] = pair_sum(jnp.stack([remainder(2 * x), remainder(2 * x + 1)]))[0]
            return carry

        loop(8, body, 0, 2)
        moved_rows(s["t1"], s["f1"], "c01", 4)
        start_exchange(1, n, s["f1"])
        pl.when(n == 1)(coefficients_held)
        pl.when(n == 2)(lambda: sum_middle(0))
        finish_exchange(1, n, s["b1"])
        held_down(1)
        s["t3"][:, pl.ds(0, 2)] = moved(s["f2"][:, pl.ds(0, 2)], "c12")
        start_exchange(2, n, s["t3"])
        finish_exchange(2, n, s["b2"])
        held_down(2)
        pl.when(n == 1)(coarse_coefficients)
        gather_start(n)
        gather_finish(n)
        coarsest(n)
        held_up(2, s["e3"], lambda i: i // 2, s["e2"], 3)
        moved_rows(s["e2"], s["t2"], "p21", 3)
        held_up(1, s["t2"], lambda i: (i - 1) // 2, s["e1"], 3)
        moved_rows(s["e1"], s["t1"], "p10", 4)

    def begun(x, z0, z1):
        inner = pl.ds(z0, z1 - z0)
        return s["w0"][x, inner] * s["b0"][x, inner]

    def corrected(x, z0, z1):
        e = s["t1"].at[x // 2]
        e = jnp.stack([e[z // 2] for z in range(z0, z1)])
        return s["v0"][1, x + 1, pl.ds(1 + z0, z1 - z0)] + e

    def coarse_kappa():
        moved_rows(s["t1"], s["f1"], "c01", 4)

        def pair_up(x, carry):
            s["f2"][x, pl.ds(0, 2)] = pair_sum(s["f1"][pl.ds(2 * x, 2)])[0]
            return carry

        loop(4, pair_up)
        start_exchange(1, 0, s["f1"])
        s["t3"][:, pl.ds(0, 2)] = moved(s["f2"][:, pl.ds(0, 2)], "c12")
        start_exchange(2, 0, s["t3"])

    def first_sums():
        def body(x, c):
            z = s["z"][0, x]
            b = s["flip"][x].reshape(8, 8, LANES)
            return c[0] + folded(b * z), c[1] + folded(z * s["q"][0, x])

        sum_start(loop(16, body, (jnp.zeros((8, LANES), F32),) * 2), 0)

    def cycle(n, carry):
        def meanwhile():
            pl.when(n == 1)(coarse_kappa)
            pl.when(n == 2)(first_sums)

        exchange(0, begun, meanwhile)
        exchange(1, swept(0))
        below(n)
        exchange(0, corrected)
        exchange(1, swept(0))
        exchange(2, swept(1))

        def apply(x, c):
            here, around = neighbours(2, x)
            q = s["d0"][x] * here - around
            s["z"][n - 1, x] = here
            s["q"][n - 1, x] = q
            return c

        loop(16, apply)

        @pl.when(n == 1)
        def _():
            def shift(x, c):
                s["flip"][x] = s["b0"][x].reshape(64, LANES)
                s["b0"][x] = s["q"][0, x]
                return c

            loop(16, shift)

        return carry

    lax.fori_loop(1, 3, cycle, 0)
    rz, zq = sum_finish(0, 2)
    step = jnp.broadcast_to(rz / zq, (8, LANES))
    zero = jnp.zeros((8, LANES), F32)

    def dots_second(x, c):
        q0 = s["q"][0, x]
        z0 = s["z"][0, x]
        r1 = s["flip"][x].reshape(8, 8, LANES) - step * q0
        z1 = z0 - step * s["z"][1, x]
        q1 = q0 - step * s["q"][1, x]
        s["z"][1, x] = z1
        pairs = (
            (r1, z1),
            (z1, q1),
            (z1, q0),
            (z0, q1),
            (r1, r1),
            (r1, q1),
            (r1, q0),
            (q1, q1),
            (q1, q0),
            (q0, q0),
        )
        return tuple(t + folded(u * v) for t, (u, v) in zip(c, pairs))

    sum_start(loop(16, dots_second, (zero,) * 10), 1)
    sum_middle(1)
    r1z1, z1q1, z1q0, z0q1, r1r1, r1q1, r1q0, q1q1, q1q0, q0q0 = sum_finish(1, 10)
    ratio = r1z1 / rz
    step2 = r1z1 / (z1q1 + ratio * (z1q0 + z0q1) + ratio * ratio * zq)
    squares = (
        r1r1
        - 2.0 * step2 * (r1q1 + ratio * r1q0)
        + step2 * step2 * (q1q1 + 2.0 * ratio * q1q0 + ratio * ratio * q0q0)
    )
    norm = jnp.sqrt(jnp.maximum(squares, 0.0) * (1.0 / cells))
    norm_ref[...] = jnp.broadcast_to(norm, (8, LANES))
    along_z0 = jnp.broadcast_to(step + step2 * ratio, (8, LANES))
    along_z1 = jnp.broadcast_to(step2, (8, LANES))

    def finish(x, c):
        value = along_z0 * s["z"][0, x] + along_z1 * s["z"][1, x]
        s["flip"][x] = value.reshape(64, LANES)
        return c

    loop(16, finish)

    def write(x, c):
        for p in range(PROBES):
            for h in range(2):
                row = h * PROBES + p
                solution_ref[p, x, pl.ds(8 * h, 8), :] = s["flip"][x, pl.ds(row, 8, stride=8), :]
        return c

    loop(16, write)


MATRICES = ("c01", "c12", "p10", "p21", "c230", "c231", "p320", "p321")


def scratch_list():
    def fields(*lead):
        return pltpu.VMEM((*lead[:-1], (lead[-1] + 3) // 4 * 4, 8, LANES), F32)

    out = {"flip": pltpu.VMEM((16, 64, LANES), F32), "lanes": pltpu.VMEM((8, LANES, LANES), jnp.bfloat16)}
    for name in ("b0", "d0", "w0"):
        out[name] = fields(16, 8)
    out["v0"] = fields(3, 18, 10)
    out["r0"] = fields(3, 2, 8)
    out["p0"] = fields(3, 2, 8)
    out["r0y"] = fields(3, 2)
    out["p0y"] = fields(3, 2)
    out["ends"] = fields(16, 1)
    out["f1"] = fields(8, 4)
    out["f2"] = fields(4, 2)
    out["f3"] = fields(2, 1)
    out["t3"] = fields(4, 2)
    for level in (1, 2):
        for name in (f"b{level}", f"w{level}", f"v{level}a", f"v{level}b"):
            out[name] = fields(*HELD[level])
        out[f"d{level}"] = fields(*CORE[level])
    out["e1"] = fields(8, 4)
    out["t1"] = fields(8, 4)
    out["e2"] = fields(6, 4)
    out["t2"] = fields(6, 4)
    out["e3"] = fields(6, 5)
    out["m1"] = fields(3, 3, 3, 4, 4)
    out["y1"] = fields(3, 3, 3, 2)
    out["y1out"] = fields(3, 2)
    out["m2"] = fields(3, 3, 3, 3, 2)
    out["z"] = fields(2, 16, 8)
    out["q"] = fields(2, 16, 8)
    out["g3"] = fields(3, 8, 4)
    out["a1"] = fields(2, 8, 4)
    out["a2"] = fields(2, 4)
    out["gw"] = fields(8, 4)
    out["gv"] = fields(2, 10, 6)
    out["count"] = fields(72)
    out["send"] = pltpu.SemaphoreType.DMA((3,))
    out["recv"] = pltpu.SemaphoreType.DMA((3,))
    out["xsend"] = pltpu.SemaphoreType.DMA((2, 3))
    out["xrecv"] = pltpu.SemaphoreType.DMA((2, 3))
    out["gsend"] = pltpu.SemaphoreType.DMA((7,))
    out["grecv"] = pltpu.SemaphoreType.DMA((7,))
    return out


def solution(mesh):
    counts = {a: mesh.shape[a] for a in ("gx", "gy", "gz")}

    def step(kappa_sq, probe_bits):
        cells = probe_bits[0].size * counts["gx"] * counts["gy"] * counts["gz"]
        whole, norms = pl.pallas_call(
            functools.partial(kernel_body, counts, cells),
            out_shape=(
                jax.ShapeDtypeStruct(probe_bits.shape, F32),
                jax.ShapeDtypeStruct((8, LANES), F32),
            ),
            in_specs=[pl.BlockSpec(memory_space=pltpu.VMEM)] * 2,
            out_specs=(pl.BlockSpec(memory_space=pltpu.VMEM),) * 2,
            scratch_shapes=list(scratch_list().values()),
            compiler_params=pltpu.CompilerParams(
                collective_id=0, has_side_effects=True, vmem_limit_bytes=40 * 2**20
            ),
            name="solve",
        )(kappa_sq, probe_bits)
        return whole, norms[:PROBES, 0]

    return jax.shard_map(
        step,
        mesh=mesh,
        in_specs=(P("gx", "gz", "gy"), P(None, "gx", "gz", "gy")),
        out_specs=(P(None, "gx", "gz", "gy"), P()),
        check_vma=False,
    )
```

```python
import functools

import jax
import jax.numpy as jnp
from jax import lax
from jax.experimental import pallas as pl
from jax.experimental.pallas import tpu as pltpu
from jax.sharding import PartitionSpec as P

LEVELS = 3
COARSE_SWEEPS = 8
PROBES = 4
LANES = 128
HALF = 4
MESH = pl.DeviceIdType.MESH
F32 = jnp.float32

OWN = {1: 32, 2: 48, 3: 24}
REACH = {1: 3, 2: 4}
HELD = {1: (14, 10), 2: (12, 10)}
CORE = {1: (8, 4), 2: (4, 2)}


def lanes_of(shape):
    return lax.broadcasted_iota(jnp.int32, shape, len(shape) - 1)


def rows_of(shape):
    return lax.broadcasted_iota(jnp.int32, shape, len(shape) - 2)


def turn(value, shift):
    return pltpu.roll(value, shift, len(value.shape) - 1)


def swap_halves(value):
    return pltpu.roll(value, HALF, len(value.shape) - 2)


def kernel_body(counts, cells, kappa_ref, bits_ref, solution_ref, norm_ref, *scratch):
    s = dict(zip(scratch_list(), scratch))
    axes = ("gx", "gz", "gy")
    me = {a: lax.axis_index(a) for a in axes}
    nx, nz = counts["gx"], counts["gz"]
    lane = lanes_of((8, LANES))

    def loop(count, body, init=0, unroll=1):
        return lax.fori_loop(0, count, body, init, unroll=count)

    def exists(steps):
        ok = None
        for a, d in zip(axes, steps):
            if d:
                one = me[a] > 0 if d < 0 else me[a] < counts[a] - 1
                ok = one if ok is None else ok & one
        return ok

    def device(steps):
        return {a: me[a] + d for a, d in zip(axes, steps)}

    around_me = sorted(
        (
            (i, j, k)
            for i in (-1, 0, 1)
            for j in (-1, 0, 1)
            for k in (-1, 0, 1)
            if (i, j, k) != (0, 0, 0)
        ),
        key=lambda steps: -sum(d * d for d in steps),
    )

    def clear_faces(i, carry):
        for x in (0, 17):
            s["v0"][i, x] = jnp.zeros(s["v0"].shape[2:], F32)
        for name in ("r0", "r0y"):
            s[name][i] = jnp.zeros(s[name].shape[1:], F32)
        return carry

    loop(3, clear_faces)
    for name in ("m1", "z1", "y1", "m2"):
        ref = s[name]

        def clear(i, carry, ref=ref):
            for j in range(ref.shape[2]):
                ref[i // 3, lax.rem(i, 3), j] = jnp.zeros(ref.shape[3:], F32)
            return carry

        loop(9, clear)

    def clear_coarse(i, carry):
        s["gv"][i // 10, lax.rem(i, 10)] = jnp.zeros(s["gv"].shape[2:], F32)
        return carry

    loop(20, clear_coarse)

    barrier = pltpu.get_barrier_semaphore()

    def greet(to):
        pl.semaphore_signal(barrier, inc=1, device_id=to, device_id_type=MESH)

    def wrapped(a, step):
        to = me[a] + step
        return jnp.where(to >= counts[a], to - counts[a], to)

    def plane_peer(i, j):
        return {"gx": wrapped("gx", i), "gz": wrapped("gz", j)}

    plane_offsets = sorted(
        ((i, j) for i in range(nx) for j in range(nz) if (i, j) != (0, 0)),
        key=lambda at: -min(at[0], nx - at[0]) - 2 * min(at[1], nz - at[1]),
    )
    for i, j in plane_offsets:
        greet(plane_peer(i, j))
    for o in range(1, counts["gy"]):
        greet({"gy": lax.rem(me["gy"] + o, counts["gy"])})
    for steps in around_me:
        if steps[2] and steps[:2] != (0, 0):
            pl.when(exists(steps))(functools.partial(greet, device(steps)))
    near = {
        a: (me[a] > 0).astype(jnp.int32) + (me[a] < counts[a] - 1).astype(jnp.int32) for a in axes
    }
    greeted = (
        nx * nz - 1 + counts["gy"] - 1 + ((near["gx"] + 1) * (near["gz"] + 1) - 1) * near["gy"]
    )

    row_at = rows_of((LANES, LANES))
    col_at = lanes_of((LANES, LANES))

    def halved(value):
        return (value + 256) // 2 - 128

    def keep(name, where, weight):
        s["lanes"][MATRICES.index(name)] = jnp.where(where, weight, 0.0).astype(jnp.bfloat16)

    keep("c01", col_at == 32 + row_at // 2, 0.125)
    keep("c12", (col_at == 48 + halved(row_at - 32)) & (row_at >= 32) & (row_at < 96), 0.125)
    inside = (row_at >= 18) & (row_at < 110)
    keep("p10", row_at == 32 + col_at // 2, 1.0)
    keep("p21", row_at == 48 + halved(col_at - 32), 1.0)
    for i in range(2):
        keep(f"c23{i}", (col_at == 64 * i + 24 + halved(row_at - 48)) & inside, 0.125)
        keep(f"p32{i}", row_at == 64 * i + 24 + halved(col_at - 48), 1.0)

    def moved(value, name):
        shape = value.shape
        rest = value.reshape(-1, LANES)
        matrix = s["lanes"][MATRICES.index(name)]
        total = None
        for _ in range(3):
            part = rest.astype(jnp.bfloat16)
            rest = rest - part.astype(F32)
            product = jnp.dot(part, matrix, preferred_element_type=F32)
            total = product if total is None else total + product
        return total.reshape(shape)

    def moved_rows(source, target, name, rows):
        def body(i, carry):
            at = pl.ds(i * rows, rows)
            target[at] = moved(source[at], name)
            return carry

        loop(source.shape[0] // rows, body)

    def load_x(x, carry):
        for p in range(PROBES):
            for h in range(2):
                row = h * PROBES + p
                s["flip"][x, pl.ds(row, 8, stride=8), :] = (
                    2.0 * bits_ref[p, x, pl.ds(8 * h, 8), :].astype(F32) - 1.0
                )
        return carry

    def take_x(x, carry):
        s["b0"][x] = s["flip"][x].reshape(8, 8, LANES)
        return carry

    def kappa_x(x, carry):
        for p in range(PROBES):
            for h in range(2):
                row = h * PROBES + p
                s["flip"][x, pl.ds(row, 8, stride=8), :] = kappa_ref[x, pl.ds(8 * h, 8), :]
        return carry

    def pair_sum(field):
        xs, zs = field.shape[0] // 2, field.shape[1] // 2
        split = field.reshape(xs, 2, zs, 2, 8, LANES)
        return (split[:, 0, :, 0] + split[:, 0, :, 1]) + (split[:, 1, :, 0] + split[:, 1, :, 1])

    def diag_x(x, carry):
        kappas = [s["flip"][2 * x + i].reshape(8, 8, LANES) for i in range(2)]
        for i in range(2):
            s["d0"][2 * x + i] = kappas[i] + 6.0
            s["w0"][2 * x + i] = 0.8 / (kappas[i] + 6.0)
        s["t1"][x] = pair_sum(jnp.stack(kappas))[0]
        return carry

    loop(16, load_x)
    loop(16, take_x)
    loop(16, kappa_x)
    loop(8, diag_x)

    def wait_for(count, send, recv):
        ref = s["count"].at[pl.ds(0, count)]
        c = pltpu.make_async_remote_copy(
            src_ref=ref,
            dst_ref=ref,
            send_sem=send,
            recv_sem=recv,
            device_id={"gx": lax.rem(me["gx"] + 1, nx)},
            device_id_type=MESH,
        )
        c.wait_recv()
        c.wait_send()

    def wait_near(count_of, send, recv):
        for x in (1, 2):
            for z in (1, 2):
                for y in (1, 2):
                    here = (near["gx"] == x) & (near["gz"] == z) & (near["gy"] == y)
                    pl.when(here)(functools.partial(wait_for, count_of(x, z, y), send, recv))

    def exchange(which, cell, meanwhile=None):
        v = s["v0"].at[which]
        got = s["r0"].at[which]
        pack = s["p0"].at[which]
        yin = s["r0y"].at[which]
        yout = s["p0y"].at[which]
        low_rows = rows_of((8, LANES)) < HALF
        inner = pl.ds(1, 8)

        def send(steps, src, dst):
            c = pltpu.make_async_remote_copy(
                src_ref=src,
                dst_ref=dst,
                send_sem=s["send"].at[which],
                recv_sem=s["recv"].at[which],
                device_id=device(steps),
                device_id_type=MESH,
            )
            pl.when(exists(steps))(c.start)

        def fill_z(x, carry):
            v[x + 1, pl.ds(1, 1)] = cell(x, 0, 1)
            v[x + 1, pl.ds(8, 1)] = cell(x, 7, 8)
            return carry

        loop(16, fill_z)

        def pack_z(x, carry):
            pack[0, x] = jnp.where(low_rows, v[x + 1, 1], swap_halves(v[x + 9, 1]))
            pack[1, x] = jnp.where(low_rows, swap_halves(v[x + 1, 8]), v[x + 9, 8])
            return carry

        loop(8, pack_z)
        send((0, -1, 0), pack.at[0], got.at[1])
        send((0, 1, 0), pack.at[1], got.at[0])
        for x in (0, 15):
            v[x + 1, pl.ds(2, 6)] = cell(x, 1, 7)
        send((-1, 0, 0), v.at[1, inner], v.at[17, inner])
        send((1, 0, 0), v.at[16, inner], v.at[0, inner])

        group = ((lane + 1) & (LANES - 1)) // 16

        def fill(x, carry):
            v[x + 2, pl.ds(2, 6)] = cell(x + 1, 1, 7)
            return carry

        loop(14, fill)

        def pack_y(x, carry):
            low, high = carry
            ends = v[x + 1, 1]
            for z in range(1, 8):
                ends = jnp.where(group == z, turn(v[x + 1, 1 + z], 16 * z), ends)
            ends = turn(ends, x)
            low = jnp.where((lane & 15) == x, ends, low)
            high = jnp.where((lane & 15) == ((x + 15) & 15), ends, high)
            return low, high

        zero = jnp.zeros((8, LANES), F32)
        yout[0], yout[1] = loop(16, pack_y, (zero, zero))
        send((0, 0, -1), yout.at[0], yin.at[1])
        send((0, 0, 1), yout.at[1], yin.at[0])
        if meanwhile is not None:
            meanwhile()
        wait_near(lambda x, z, y: 8 * (x + z) + y, s["send"].at[which], s["recv"].at[which])

        def unpack_z(x, carry):
            low, high = got[0, x], got[1, x]
            v[x + 1, 0] = jnp.where(low_rows, low, swap_halves(v[x + 1, 8]))
            v[x + 9, 0] = swap_halves(jnp.where(low_rows, v[x + 9, 8], low))
            v[x + 1, 9] = swap_halves(jnp.where(low_rows, high, v[x + 1, 1]))
            v[x + 9, 9] = jnp.where(low_rows, swap_halves(v[x + 9, 1]), high)
            return carry

        loop(8, unpack_z, 0, 4)

        def unpack_y(x, carry):
            before = turn(yin[0], (LANES + 1 - x) & (LANES - 1))
            after = turn(yin[1], LANES - 1 - x)
            s["ends"][x, 0] = jnp.where((lane & 15) == 0, before, after)
            return carry

        loop(16, unpack_y, 0, 8)

    def neighbours(which, x, z0=0, z1=8):
        v = s["v0"].at[which]
        inner = pl.ds(1 + z0, z1 - z0)
        here = v[x + 1, inner]
        total = v[x, inner] + v[x + 2, inner]
        total = total + (v[x + 1, pl.ds(z0, z1 - z0)] + v[x + 1, pl.ds(z0 + 2, z1 - z0)])
        ends = s["ends"][x, 0]
        ends = jnp.stack([turn(ends, LANES - 16 * z) if z else ends for z in range(z0, z1)])
        at_lane = lanes_of((z1 - z0, 8, LANES))
        before = jnp.where(at_lane == 0, ends, turn(here, 1))
        after = jnp.where(at_lane == LANES - 1, ends, turn(here, LANES - 1))
        return here, total + (before + after)

    def swept(which):
        def cell(x, z0, z1):
            inner = pl.ds(z0, z1 - z0)
            here, around = neighbours(which, x, z0, z1)
            return 0.2 * here + s["w0"][x, inner] * (s["b0"][x, inner] + around)

        return cell

    def start_exchange(level, n, field):
        if level == 1:

            def pack_x(i, carry):
                s["m1"][n, 1, 1, i] = turn(field[2 * i], LANES - 32) + turn(field[2 * i + 1], 32)
                return carry

            loop(4, pack_x, 0, 2)

            low_rows = rows_of((3, 8, LANES)) < HALF
            for i in range(2):
                one, two = (s["m1"].at[n, 1, 1, i + 2 * k] for k in range(2))
                s["z1out"][n, 0, i, pl.ds(0, 3)] = jnp.where(
                    low_rows, one[pl.ds(0, 3)], swap_halves(two[pl.ds(0, 3)])
                )
                s["z1out"][n, 1, i, pl.ds(0, 3)] = jnp.where(
                    low_rows, swap_halves(one[pl.ds(1, 3)]), two[pl.ds(1, 3)]
                )

            def pack_y(x, carry):
                low, high = carry
                for z in range(4):
                    at = 16 * x + 4 * z
                    slot = (lane >> 2) == 4 * x + z
                    value = field[x, z]
                    low = jnp.where(slot, turn(value, (at + LANES - 32) & (LANES - 1)), low)
                    high = jnp.where(slot, turn(value, (at + LANES - 92) & (LANES - 1)), high)
                return low, high

            zero = jnp.zeros((8, LANES), F32)
            low, high = loop(8, pack_y, (zero, zero), 2)
            s["y1out"][n, 0] = high
            s["y1out"][n, 1] = low
        else:
            both = pl.ds(0, 2)
            total = turn(field[0, both], LANES - 48)
            for x in range(1, 4):
                total = total + turn(field[x, both], (32 * x + LANES - 48) % LANES)
            s["m2"][n, 1, 1, 1, both] = total
        for steps in around_me:
            i, j, k = steps
            if level == 2:
                src = s["m2"].at[n, 1, 1, 1, pl.ds(0, 2)]
                dst = s["m2"].at[n, 1 - i, 1 - j, 1 - k, pl.ds(0, 2)]
            elif k:
                side = 0 if k > 0 else 1
                src = s["y1out"].at[n, side]
                dst = s["y1"].at[n, 1 - i, 1 - j, side]
            else:
                if j == 0:
                    part = pl.ds(0 if i < 0 else 2, 2)
                    src = s["m1"].at[n, 1, 1, part]
                    dst = s["m1"].at[n, 1 - i, 1 - j, part]
                else:
                    side = 0 if j < 0 else 1
                    if i == 0:
                        part = (slice(None), pl.ds(0, 3))
                    else:
                        part = (pl.ds(0 if i < 0 else 1, 1), pl.ds(0 if j < 0 else 1, 2))
                    src = s["z1out"].at[(n, side, *part)]
                    dst = s["z1"].at[(n, 1 - i, 1 - side, *part)]
            c = pltpu.make_async_remote_copy(
                src_ref=src,
                dst_ref=dst,
                send_sem=s["xsend"].at[level - 1, n],
                recv_sem=s["xrecv"].at[level - 1, n],
                device_id=device(steps),
                device_id_type=MESH,
            )
            pl.when(exists(steps))(c.start)

    def finish_exchange(level, n, out):
        def count_of(x, z, y):
            if level == 2:
                return 2 * ((x + 1) * (z + 1) * (y + 1) - 1)
            return 8 * x + 6 * z + 2 * x * z + (x + 1) * (z + 1) * y

        wait_near(count_of, s["xsend"].at[level - 1, n], s["xrecv"].at[level - 1, n])
        low_rows = rows_of((8, LANES)) < HALF
        reach = REACH[level]
        xs, zs = (8, 4) if level == 1 else (4, 2)

        def body(x, carry):
            far = (x + xs - reach) // xs
            at_x = lax.rem(x + xs - reach, xs)

            def source(j, z):
                if level == 1:
                    pair = at_x // 2
                    if j == 1:
                        mid = s["m1"][n, far, 1, pair, z]
                    else:
                        mid = s["z1"][n, far, j // 2, lax.rem(pair, 2), z - 1 if j == 0 else z]
                        there = (pair < 2) if j == 0 else (pair >= 2)
                        mid = jnp.where(there, swap_halves(mid), mid)
                    mid = turn(mid, 32 + 64 * lax.rem(at_x, 2))
                    at = 4 * (4 * at_x + z)
                    left = turn(s["y1"][n, far, j, 0], lax.rem(28 - at + 2 * LANES, LANES))
                    right = turn(s["y1"][n, far, j, 1], lax.rem(96 - at + 2 * LANES, LANES))
                    value = jnp.where((lane >= 28) & (lane < 32), left, 0.0)
                    value = jnp.where((lane >= 96) & (lane < 100), right, value)
                    return jnp.where((lane >= 32) & (lane < 96), mid, value)
                value = jnp.zeros((8, LANES), F32)
                for k in range(3):
                    start = 16 + 32 * k
                    part = turn(
                        s["m2"][n, far, j, k, z], lax.rem(start + 2 * LANES - 32 * at_x, LANES)
                    )
                    value = jnp.where((lane >= start) & (lane < start + 32), part, value)
                return value

            mine = [source(1, z) for z in range(zs)]
            if level == 1:
                down = [None] + [source(0, z) for z in (1, 2, 3)]
                over = [source(2, z) for z in (0, 1, 2)]
                below = [(down[z], mine[z]) for z in (1, 2, 3)]
                above = [(over[z], mine[z]) for z in (0, 1, 2)]
                outer_low, outer_high = [], []
            else:
                outer_low = [source(0, z) for z in range(2)]
                outer_high = [source(2, z) for z in range(2)]
                below = list(zip(outer_low, mine))
                above = list(zip(outer_high, mine))
            values = list(outer_low)
            values += [swap_halves(jnp.where(low_rows, own, other)) for other, own in below]
            values += mine
            values += [swap_halves(jnp.where(low_rows, other, own)) for other, own in above]
            values += outer_high
            out[x, pl.ds(0, len(values))] = jnp.stack(values)
            return carry

        loop(xs + 2 * reach, body, 0, 2)

    def held_row(src, x, z0, z1):
        inner = pl.ds(z0, z1 - z0)
        here = src[x, inner]
        total = (src[x - 1, inner] + src[x + 1, inner]) + (
            src[x, pl.ds(z0 - 1, z1 - z0)] + src[x, pl.ds(z0 + 1, z1 - z0)]
        )
        return here, total + (turn(here, 1) + turn(here, LANES - 1))

    def held_sweep(level, src, dst, margin, into=0):
        xs, zs = HELD[level]
        coupling = 0.25**level
        z0, z1 = margin, zs - margin

        def body(i, carry):
            x = i + margin
            here, around = held_row(src, x, z0, z1)
            inner = pl.ds(z0, z1 - z0)
            value = 0.2 * here + s[f"w{level}"][x, inner] * (
                s[f"b{level}"][x, inner] + coupling * around
            )
            if into:
                dst[i] = value
            else:
                dst[x, inner] = value
            return carry

        loop(xs - 2 * margin, body, 0, 2)

    def held_down(level):
        xs, zs = HELD[level]
        reach = REACH[level]
        coupling = 0.25**level

        def begin(x, carry):
            s[f"v{level}a"][x] = s[f"w{level}"][x] * s[f"b{level}"][x]
            return carry

        loop(xs, begin)
        held_sweep(level, s[f"v{level}a"], s[f"v{level}b"], 1)
        z0, z1 = reach, zs - reach
        inner = pl.ds(z0, z1 - z0)

        def remainder(x):
            here, around = held_row(s[f"v{level}b"], x + reach, z0, z1)
            return s[f"b{level}"][x + reach, inner] - (
                s[f"d{level}"][x, pl.ds(0, CORE[level][1])] * here - coupling * around
            )

        def body(x, carry):
            pair = pair_sum(jnp.stack([remainder(2 * x), remainder(2 * x + 1)]))[0]
            s[f"f{level + 1}"][x, pl.ds(0, CORE[level][1] // 2)] = pair
            return carry

        loop((xs - 2 * reach) // 2, body, 0, 2)

    def held_up(level, coarse, spread, out, last_margin):
        xs, zs = HELD[level]

        def add(i, carry):
            x = i + 1
            picked = jnp.stack([coarse[spread(x), spread(z)] for z in range(1, zs - 1)])
            s[f"v{level}a"][x, pl.ds(1, zs - 2)] = s[f"v{level}b"][x, pl.ds(1, zs - 2)] + picked
            return carry

        loop(xs - 2, add)
        held_sweep(level, s[f"v{level}a"], s[f"v{level}b"], 2)
        held_sweep(level, s[f"v{level}b"], out, 3, into=1)

    def own_of(level, ref):
        reach = REACH[level]
        xs, zs = HELD[level]
        return ref[pl.ds(reach, xs - 2 * reach), pl.ds(reach, zs - 2 * reach)]

    def coefficients(level, kappa):
        coupling = 6.0 * 0.25**level
        s[f"d{level}"][:, pl.ds(0, CORE[level][1])] = own_of(level, kappa) + coupling

        def body(x, carry):
            k = kappa[x]
            s[f"w{level}"][x] = jnp.where(k > 0.0, 0.8 / (k + coupling), 0.0)
            return carry

        loop(kappa.shape[0], body)

    def plane_start(ref, sems):
        at = ref.at[me["gx"], me["gz"]]
        for i, j in plane_offsets:
            pltpu.make_async_remote_copy(
                src_ref=at,
                dst_ref=at,
                send_sem=s["gsend"].at[sems],
                recv_sem=s["grecv"].at[sems],
                device_id=plane_peer(i, j),
                device_id_type=MESH,
            ).start()

    def plane_finish(sems):
        wait_for(nx * nz - 1, s["gsend"].at[sems], s["grecv"].at[sems])

    def gather_start(n):
        s["g3"][n, me["gx"], me["gz"]] = moved(s["f3"][0, 0], "c230") + moved(s["f3"][1, 0], "c231")
        plane_start(s["g3"].at[n], n)

    def gather_finish(n):
        plane_finish(n)

    def coarsest(n):
        coupling = 0.25**LEVELS
        inner = pl.ds(1, nz)
        s["gv"][0, pl.ds(1, nx), inner] = s["gw"][...] * s["g3"][n]
        glane, grow = lanes_of((nz, 8, LANES)), rows_of((nz, 8, LANES))

        def coarse_sweep(src, dst):
            def body(x, carry):
                here = src[x + 1, inner]
                along_x = turn(
                    here + jnp.where(glane >= 64, src[x, inner], src[x + 2, inner]), 64
                )
                along_z = swap_halves(
                    here
                    + jnp.where(grow >= HALF, src[x + 1, pl.ds(0, nz)], src[x + 1, pl.ds(2, nz)])
                )
                around = (along_x + along_z) + (turn(here, 1) + turn(here, LANES - 1))
                dst[x + 1, inner] = 0.2 * here + s["gw"][x] * (s["g3"][n, x] + coupling * around)
                return carry

            loop(nx, body, 0, nx)

        for i in range(COARSE_SWEEPS - 1):
            coarse_sweep(s["gv"].at[i % 2], s["gv"].at[1 - i % 2])
        done = s["gv"].at[(COARSE_SWEEPS - 1) % 2]
        low_rows = rows_of((8, LANES)) < HALF
        near_me = []
        for i in range(3):
            below, mine, above = (done[i + me["gx"], j + me["gz"]] for j in range(3))
            near_me += [
                below,
                swap_halves(jnp.where(low_rows, mine, below)),
                mine,
                swap_halves(jnp.where(low_rows, above, mine)),
                above,
            ]
        near_me = jnp.stack(near_me)
        for i in range(2):
            spread = moved(near_me, f"p32{i}")
            for x in range(3):
                s["e3"][2 * x + i, pl.ds(0, 5)] = spread[5 * x : 5 * x + 5]

    def sum_start(dots, n):
        packed = jnp.zeros((8, LANES), F32)
        for j, d in enumerate(dots):
            packed = jnp.where(lane == j, jnp.sum(d, axis=-1, keepdims=True), packed)
        s["a1"][n, me["gx"], me["gz"]] = packed + swap_halves(packed)
        plane_start(s["a1"].at[n], 3 + n)

    def folded(value):
        while value.shape[0] > 1:
            value = value[: value.shape[0] // 2] + value[value.shape[0] // 2 :]
        return value[0]

    def sum_middle(n):
        plane_finish(3 + n)
        s["a2"][n, me["gy"]] = folded(s["a1"][n].reshape(nx * nz, 8, LANES))
        at = s["a2"].at[n, me["gy"]]
        for o in range(1, counts["gy"]):
            pltpu.make_async_remote_copy(
                src_ref=at,
                dst_ref=at,
                send_sem=s["gsend"].at[5 + n],
                recv_sem=s["grecv"].at[5 + n],
                device_id={"gy": wrapped("gy", o)},
                device_id_type=MESH,
            ).start()

    def sum_finish(n, count):
        wait_for(counts["gy"] - 1, s["gsend"].at[5 + n], s["grecv"].at[5 + n])
        total = folded(s["a2"][n])
        return [total[:, j : j + 1] for j in range(count)]

    pl.semaphore_wait(barrier, greeted)

    def coefficients_held():
        finish_exchange(1, 0, s["v1a"])
        coefficients(1, s["v1a"])
        finish_exchange(2, 0, s["v2a"])
        coefficients(2, s["v2a"])
        s["f3"][:, pl.ds(0, 1)] = pair_sum(own_of(2, s["v2a"]))
        gather_start(0)

    def coarse_coefficients():
        gather_finish(0)
        kappa_3 = s["g3"][0]
        s["gw"][...] = jnp.where(kappa_3 > 0.0, 0.8 / (kappa_3 + 6.0 * 0.25**LEVELS), 0.0)

    def below(n):
        def remainder(x):
            here, around = neighbours(1, x)
            return s["b0"][x] - (s["d0"][x] * here - around)

        def body(x, carry):
            s["t1"][x] = pair_sum(jnp.stack([remainder(2 * x), remainder(2 * x + 1)]))[0]
            return carry

        loop(8, body, 0, 2)
        moved_rows(s["t1"], s["f1"], "c01", 4)
        start_exchange(1, n, s["f1"])
        pl.when(n == 1)(coefficients_held)
        pl.when(n == 2)(lambda: sum_middle(0))
        finish_exchange(1, n, s["b1"])
        held_down(1)
        s["t3"][:, pl.ds(0, 2)] = moved(s["f2"][:, pl.ds(0, 2)], "c12")
        start_exchange(2, n, s["t3"])
        finish_exchange(2, n, s["b2"])
        held_down(2)
        pl.when(n == 1)(coarse_coefficients)
        gather_start(n)
        gather_finish(n)
        coarsest(n)
        held_up(2, s["e3"], lambda i: i // 2, s["e2"], 3)
        moved_rows(s["e2"], s["t2"], "p21", 3)
        held_up(1, s["t2"], lambda i: (i - 1) // 2, s["e1"], 3)
        moved_rows(s["e1"], s["t1"], "p10", 4)

    def begun(x, z0, z1):
        inner = pl.ds(z0, z1 - z0)
        return s["w0"][x, inner] * s["b0"][x, inner]

    def corrected(x, z0, z1):
        e = s["t1"].at[x // 2]
        e = jnp.stack([e[z // 2] for z in range(z0, z1)])
        return s["v0"][1, x + 1, pl.ds(1 + z0, z1 - z0)] + e

    def coarse_kappa():
        moved_rows(s["t1"], s["f1"], "c01", 4)

        def pair_up(x, carry):
            s["f2"][x, pl.ds(0, 2)] = pair_sum(s["f1"][pl.ds(2 * x, 2)])[0]
            return carry

        loop(4, pair_up)
        start_exchange(1, 0, s["f1"])
        s["t3"][:, pl.ds(0, 2)] = moved(s["f2"][:, pl.ds(0, 2)], "c12")
        start_exchange(2, 0, s["t3"])

    def first_sums():
        def body(x, c):
            z = s["z"][0, x]
            b = s["flip"][x].reshape(8, 8, LANES)
            return c[0] + folded(b * z), c[1] + folded(z * s["q"][0, x])

        sum_start(loop(16, body, (jnp.zeros((8, LANES), F32),) * 2), 0)

    def cycle(n, carry):
        def meanwhile():
            pl.when(n == 1)(coarse_kappa)
            pl.when(n == 2)(first_sums)

        exchange(0, begun, meanwhile)
        exchange(1, swept(0))
        below(n)
        exchange(0, corrected)
        exchange(1, swept(0))
        exchange(2, swept(1))

        def apply(x, c):
            here, around = neighbours(2, x)
            q = s["d0"][x] * here - around
            s["z"][n - 1, x] = here
            s["q"][n - 1, x] = q
            return c

        loop(16, apply)

        @pl.when(n == 1)
        def _():
            def shift(x, c):
                s["flip"][x] = s["b0"][x].reshape(64, LANES)
                s["b0"][x] = s["q"][0, x]
                return c

            loop(16, shift)

        return carry

    lax.fori_loop(1, 3, cycle, 0)
    rz, zq = sum_finish(0, 2)
    step = jnp.broadcast_to(rz / zq, (8, LANES))
    zero = jnp.zeros((8, LANES), F32)

    def dots_second(x, c):
        q0 = s["q"][0, x]
        z0 = s["z"][0, x]
        r1 = s["flip"][x].reshape(8, 8, LANES) - step * q0
        z1 = z0 - step * s["z"][1, x]
        q1 = q0 - step * s["q"][1, x]
        s["z"][1, x] = z1
        pairs = (
            (r1, z1),
            (z1, q1),
            (z1, q0),
            (z0, q1),
            (r1, r1),
            (r1, q1),
            (r1, q0),
            (q1, q1),
            (q1, q0),
            (q0, q0),
        )
        return tuple(t + folded(u * v) for t, (u, v) in zip(c, pairs))

    sum_start(loop(16, dots_second, (zero,) * 10), 1)
    sum_middle(1)
    r1z1, z1q1, z1q0, z0q1, r1r1, r1q1, r1q0, q1q1, q1q0, q0q0 = sum_finish(1, 10)
    ratio = r1z1 / rz
    step2 = r1z1 / (z1q1 + ratio * (z1q0 + z0q1) + ratio * ratio * zq)
    squares = (
        r1r1
        - 2.0 * step2 * (r1q1 + ratio * r1q0)
        + step2 * step2 * (q1q1 + 2.0 * ratio * q1q0 + ratio * ratio * q0q0)
    )
    norm = jnp.sqrt(jnp.maximum(squares, 0.0) * (1.0 / cells))
    norm_ref[...] = jnp.broadcast_to(norm, (8, LANES))
    along_z0 = jnp.broadcast_to(step + step2 * ratio, (8, LANES))
    along_z1 = jnp.broadcast_to(step2, (8, LANES))

    def finish(x, c):
        value = along_z0 * s["z"][0, x] + along_z1 * s["z"][1, x]
        s["flip"][x] = value.reshape(64, LANES)
        return c

    loop(16, finish)

    def write(x, c):
        for p in range(PROBES):
            for h in range(2):
                row = h * PROBES + p
                solution_ref[p, x, pl.ds(8 * h, 8), :] = s["flip"][x, pl.ds(row, 8, stride=8), :]
        return c

    loop(16, write)


MATRICES = ("c01", "c12", "p10", "p21", "c230", "c231", "p320", "p321")


def scratch_list():
    def fields(*lead):
        return pltpu.VMEM((*lead[:-1], (lead[-1] + 3) // 4 * 4, 8, LANES), F32)

    out = {"flip": pltpu.VMEM((16, 64, LANES), F32), "lanes": pltpu.VMEM((8, LANES, LANES), jnp.bfloat16)}
    for name in ("b0", "d0", "w0"):
        out[name] = fields(16, 8)
    out["v0"] = fields(3, 18, 10)
    out["r0"] = fields(3, 2, 8)
    out["p0"] = fields(3, 2, 8)
    out["r0y"] = fields(3, 2)
    out["p0y"] = fields(3, 2)
    out["ends"] = fields(16, 1)
    out["f1"] = fields(8, 4)
    out["f2"] = fields(4, 2)
    out["f3"] = fields(2, 1)
    out["t3"] = fields(4, 2)
    for level in (1, 2):
        for name in (f"b{level}", f"w{level}", f"v{level}a", f"v{level}b"):
            out[name] = fields(*HELD[level])
        out[f"d{level}"] = fields(*CORE[level])
    out["e1"] = fields(8, 4)
    out["t1"] = fields(8, 4)
    out["e2"] = fields(6, 4)
    out["t2"] = fields(6, 4)
    out["e3"] = fields(6, 5)
    out["m1"] = fields(3, 3, 3, 4, 4)
    out["z1"] = fields(3, 3, 2, 2, 3)
    out["z1out"] = fields(3, 2, 2, 3)
    out["y1"] = fields(3, 3, 3, 2)
    out["y1out"] = fields(3, 2)
    out["m2"] = fields(3, 3, 3, 3, 2)
    out["z"] = fields(2, 16, 8)
    out["q"] = fields(2, 16, 8)
    out["g3"] = fields(3, 8, 4)
    out["a1"] = fields(2, 8, 4)
    out["a2"] = fields(2, 4)
    out["gw"] = fields(8, 4)
    out["gv"] = fields(2, 10, 6)
    out["count"] = fields(72)
    out["send"] = pltpu.SemaphoreType.DMA((3,))
    out["recv"] = pltpu.SemaphoreType.DMA((3,))
    out["xsend"] = pltpu.SemaphoreType.DMA((2, 3))
    out["xrecv"] = pltpu.SemaphoreType.DMA((2, 3))
    out["gsend"] = pltpu.SemaphoreType.DMA((7,))
    out["grecv"] = pltpu.SemaphoreType.DMA((7,))
    return out


def solution(mesh):
    counts = {a: mesh.shape[a] for a in ("gx", "gy", "gz")}

    def step(kappa_sq, probe_bits):
        cells = probe_bits[0].size * counts["gx"] * counts["gy"] * counts["gz"]
        whole, norms = pl.pallas_call(
            functools.partial(kernel_body, counts, cells),
            out_shape=(
                jax.ShapeDtypeStruct(probe_bits.shape, F32),
                jax.ShapeDtypeStruct((8, LANES), F32),
            ),
            in_specs=[pl.BlockSpec(memory_space=pltpu.VMEM)] * 2,
            out_specs=(pl.BlockSpec(memory_space=pltpu.VMEM),) * 2,
            scratch_shapes=list(scratch_list().values()),
            compiler_params=pltpu.CompilerParams(
                collective_id=0, has_side_effects=True, vmem_limit_bytes=40 * 2**20
            ),
            name="solve",
        )(kappa_sq, probe_bits)
        return whole, norms[:PROBES, 0]

    return jax.shard_map(
        step,
        mesh=mesh,
        in_specs=(P("gx", "gz", "gy"), P(None, "gx", "gz", "gy")),
        out_specs=(P(None, "gx", "gz", "gy"), P()),
        check_vma=False,
    )
```

```python
import functools

import jax
import jax.numpy as jnp
from jax import lax
from jax.experimental import pallas as pl
from jax.experimental.pallas import tpu as pltpu
from jax.sharding import PartitionSpec as P

LEVELS = 3
COARSE_SWEEPS = 8
PROBES = 4
LANES = 128
HALF = 4
MESH = pl.DeviceIdType.MESH
F32 = jnp.float32

OWN = {1: 32, 2: 48, 3: 24}
REACH = {1: 3, 2: 4}
HELD = {1: (14, 10), 2: (12, 10)}
CORE = {1: (8, 4), 2: (4, 2)}


def lanes_of(shape):
    return lax.broadcasted_iota(jnp.int32, shape, len(shape) - 1)


def rows_of(shape):
    return lax.broadcasted_iota(jnp.int32, shape, len(shape) - 2)


def turn(value, shift):
    return pltpu.roll(value, shift, len(value.shape) - 1)


def swap_halves(value):
    return pltpu.roll(value, HALF, len(value.shape) - 2)


def kernel_body(counts, cells, kappa_ref, bits_ref, solution_ref, norm_ref, *scratch):
    s = dict(zip(scratch_list(), scratch))
    axes = ("gx", "gz", "gy")
    me = {a: lax.axis_index(a) for a in axes}
    nx, nz = counts["gx"], counts["gz"]
    lane = lanes_of((8, LANES))

    def loop(count, body, init=0, unroll=1):
        return lax.fori_loop(0, count, body, init, unroll=count)

    def exists(steps):
        ok = None
        for a, d in zip(axes, steps):
            if d:
                one = me[a] > 0 if d < 0 else me[a] < counts[a] - 1
                ok = one if ok is None else ok & one
        return ok

    def device(steps):
        return {a: me[a] + d for a, d in zip(axes, steps)}

    around_me = sorted(
        (
            (i, j, k)
            for i in (-1, 0, 1)
            for j in (-1, 0, 1)
            for k in (-1, 0, 1)
            if (i, j, k) != (0, 0, 0)
        ),
        key=lambda steps: -sum(d * d for d in steps),
    )

    def clear_faces(i, carry):
        for x in (0, 17):
            s["v0"][i, x] = jnp.zeros(s["v0"].shape[2:], F32)
        for name in ("r0", "r0y"):
            s[name][i] = jnp.zeros(s[name].shape[1:], F32)
        return carry

    loop(3, clear_faces)
    for name in ("m1", "z1", "y1", "m2"):
        ref = s[name]

        def clear(i, carry, ref=ref):
            for j in range(ref.shape[2]):
                ref[i // 3, lax.rem(i, 3), j] = jnp.zeros(ref.shape[3:], F32)
            return carry

        loop(9, clear)

    def clear_coarse(i, carry):
        s["gv"][i // 10, lax.rem(i, 10)] = jnp.zeros(s["gv"].shape[2:], F32)
        return carry

    loop(20, clear_coarse)

    barrier = pltpu.get_barrier_semaphore()

    def greet(to):
        pl.semaphore_signal(barrier, inc=1, device_id=to, device_id_type=MESH)

    def wrapped(a, step):
        to = me[a] + step
        return jnp.where(to >= counts[a], to - counts[a], to)

    def plane_peer(i, j):
        return {"gx": wrapped("gx", i), "gz": wrapped("gz", j)}

    plane_offsets = sorted(
        ((i, j) for i in range(nx) for j in range(nz) if (i, j) != (0, 0)),
        key=lambda at: -min(at[0], nx - at[0]) - 2 * min(at[1], nz - at[1]),
    )
    for i, j in plane_offsets:
        greet(plane_peer(i, j))
    for o in range(1, counts["gy"]):
        greet({"gy": lax.rem(me["gy"] + o, counts["gy"])})
    for steps in around_me:
        if steps[2] and steps[:2] != (0, 0):
            pl.when(exists(steps))(functools.partial(greet, device(steps)))
    near = {
        a: (me[a] > 0).astype(jnp.int32) + (me[a] < counts[a] - 1).astype(jnp.int32) for a in axes
    }
    greeted = (
        nx * nz - 1 + counts["gy"] - 1 + ((near["gx"] + 1) * (near["gz"] + 1) - 1) * near["gy"]
    )

    row_at = rows_of((LANES, LANES))
    col_at = lanes_of((LANES, LANES))

    def halved(value):
        return (value + 256) // 2 - 128

    def keep(name, where, weight):
        s["lanes"][MATRICES.index(name)] = jnp.where(where, weight, 0.0).astype(jnp.bfloat16)

    keep("c01", col_at == 32 + row_at // 2, 0.125)
    keep("c12", (col_at == 48 + halved(row_at - 32)) & (row_at >= 32) & (row_at < 96), 0.125)
    inside = (row_at >= 18) & (row_at < 110)
    keep("p10", row_at == 32 + col_at // 2, 1.0)
    keep("p21", row_at == 48 + halved(col_at - 32), 1.0)
    for i in range(2):
        keep(f"c23{i}", (col_at == 64 * i + 24 + halved(row_at - 48)) & inside, 0.125)
        keep(f"p32{i}", row_at == 64 * i + 24 + halved(col_at - 48), 1.0)

    def moved(value, name):
        shape = value.shape
        rest = value.reshape(-1, LANES)
        matrix = s["lanes"][MATRICES.index(name)]
        total = None
        for _ in range(3):
            part = rest.astype(jnp.bfloat16)
            rest = rest - part.astype(F32)
            product = jnp.dot(part, matrix, preferred_element_type=F32)
            total = product if total is None else total + product
        return total.reshape(shape)

    def moved_rows(source, target, name, rows):
        def body(i, carry):
            at = pl.ds(i * rows, rows)
            target[at] = moved(source[at], name)
            return carry

        loop(source.shape[0] // rows, body)

    def load_x(x, carry):
        for p in range(PROBES):
            for h in range(2):
                row = h * PROBES + p
                s["flip"][x, pl.ds(row, 8, stride=8), :] = (
                    2.0 * bits_ref[p, x, pl.ds(8 * h, 8), :].astype(F32) - 1.0
                )
        return carry

    def take_x(x, carry):
        s["b0"][x] = s["flip"][x].reshape(8, 8, LANES)
        return carry

    def kappa_x(x, carry):
        for p in range(PROBES):
            for h in range(2):
                row = h * PROBES + p
                s["flip"][x, pl.ds(row, 8, stride=8), :] = kappa_ref[x, pl.ds(8 * h, 8), :]
        return carry

    def pair_sum(field):
        xs, zs = field.shape[0] // 2, field.shape[1] // 2
        split = field.reshape(xs, 2, zs, 2, 8, LANES)
        return (split[:, 0, :, 0] + split[:, 0, :, 1]) + (split[:, 1, :, 0] + split[:, 1, :, 1])

    def diag_x(x, carry):
        kappas = [s["flip"][2 * x + i].reshape(8, 8, LANES) for i in range(2)]
        for i in range(2):
            s["d0"][2 * x + i] = kappas[i] + 6.0
            s["w0"][2 * x + i] = 0.8 / (kappas[i] + 6.0)
        s["t1"][x] = pair_sum(jnp.stack(kappas))[0]
        return carry

    loop(16, load_x)
    loop(16, take_x)
    loop(16, kappa_x)
    loop(8, diag_x)

    def wait_for(count, send, recv):
        ref = s["count"].at[pl.ds(0, count)]
        c = pltpu.make_async_remote_copy(
            src_ref=ref,
            dst_ref=ref,
            send_sem=send,
            recv_sem=recv,
            device_id={"gx": lax.rem(me["gx"] + 1, nx)},
            device_id_type=MESH,
        )
        c.wait_recv()
        c.wait_send()

    def wait_near(count_of, send, recv):
        for x in (1, 2):
            for z in (1, 2):
                for y in (1, 2):
                    here = (near["gx"] == x) & (near["gz"] == z) & (near["gy"] == y)
                    pl.when(here)(functools.partial(wait_for, count_of(x, z, y), send, recv))

    def exchange(which, cell, meanwhile=None):
        v = s["v0"].at[which]
        got = s["r0"].at[which]
        pack = s["p0"].at[which]
        yin = s["r0y"].at[which]
        yout = s["p0y"].at[which]
        low_rows = rows_of((8, LANES)) < HALF
        inner = pl.ds(1, 8)

        def send(steps, src, dst):
            c = pltpu.make_async_remote_copy(
                src_ref=src,
                dst_ref=dst,
                send_sem=s["send"].at[which],
                recv_sem=s["recv"].at[which],
                device_id=device(steps),
                device_id_type=MESH,
            )
            pl.when(exists(steps))(c.start)

        def fill_z(x, carry):
            v[x + 1, pl.ds(1, 1)] = cell(x, 0, 1)
            v[x + 1, pl.ds(8, 1)] = cell(x, 7, 8)
            return carry

        loop(16, fill_z)

        def pack_z(x, carry):
            pack[0, x] = jnp.where(low_rows, v[x + 1, 1], swap_halves(v[x + 9, 1]))
            pack[1, x] = jnp.where(low_rows, swap_halves(v[x + 1, 8]), v[x + 9, 8])
            return carry

        loop(8, pack_z)
        send((0, -1, 0), pack.at[0], got.at[1])
        send((0, 1, 0), pack.at[1], got.at[0])
        for x in (0, 15):
            v[x + 1, pl.ds(2, 6)] = cell(x, 1, 7)
        send((-1, 0, 0), v.at[1, inner], v.at[17, inner])
        send((1, 0, 0), v.at[16, inner], v.at[0, inner])

        group = ((lane + 1) & (LANES - 1)) // 16

        def fill(x, carry):
            v[x + 2, pl.ds(2, 6)] = cell(x + 1, 1, 7)
            return carry

        loop(14, fill)

        def pack_y(x, carry):
            low, high = carry
            ends = v[x + 1, 1]
            for z in range(1, 8):
                ends = jnp.where(group == z, turn(v[x + 1, 1 + z], 16 * z), ends)
            ends = turn(ends, x)
            low = jnp.where((lane & 15) == x, ends, low)
            high = jnp.where((lane & 15) == ((x + 15) & 15), ends, high)
            return low, high

        zero = jnp.zeros((8, LANES), F32)
        yout[0], yout[1] = loop(16, pack_y, (zero, zero))
        send((0, 0, -1), yout.at[0], yin.at[1])
        send((0, 0, 1), yout.at[1], yin.at[0])
        if meanwhile is not None:
            meanwhile()
        wait_near(lambda x, z, y: 8 * (x + z) + y, s["send"].at[which], s["recv"].at[which])

        def unpack_z(x, carry):
            low, high = got[0, x], got[1, x]
            v[x + 1, 0] = jnp.where(low_rows, low, swap_halves(v[x + 1, 8]))
            v[x + 9, 0] = swap_halves(jnp.where(low_rows, v[x + 9, 8], low))
            v[x + 1, 9] = swap_halves(jnp.where(low_rows, high, v[x + 1, 1]))
            v[x + 9, 9] = jnp.where(low_rows, swap_halves(v[x + 9, 1]), high)
            return carry

        loop(8, unpack_z, 0, 4)

        def unpack_y(x, carry):
            before = turn(yin[0], (LANES + 1 - x) & (LANES - 1))
            after = turn(yin[1], LANES - 1 - x)
            s["ends"][x, 0] = jnp.where((lane & 15) == 0, before, after)
            return carry

        loop(16, unpack_y, 0, 8)

    def neighbours(which, x, z0=0, z1=8):
        v = s["v0"].at[which]
        inner = pl.ds(1 + z0, z1 - z0)
        here = v[x + 1, inner]
        total = v[x, inner] + v[x + 2, inner]
        total = total + (v[x + 1, pl.ds(z0, z1 - z0)] + v[x + 1, pl.ds(z0 + 2, z1 - z0)])
        ends = s["ends"][x, 0]
        ends = jnp.stack([turn(ends, LANES - 16 * z) if z else ends for z in range(z0, z1)])
        at_lane = lanes_of((z1 - z0, 8, LANES))
        before = jnp.where(at_lane == 0, ends, turn(here, 1))
        after = jnp.where(at_lane == LANES - 1, ends, turn(here, LANES - 1))
        return here, total + (before + after)

    def swept(which):
        def cell(x, z0, z1):
            inner = pl.ds(z0, z1 - z0)
            here, around = neighbours(which, x, z0, z1)
            return 0.2 * here + s["w0"][x, inner] * (s["b0"][x, inner] + around)

        return cell

    def start_exchange(level, n, field):
        if level == 1:

            def pack_x(i, carry):
                s["m1"][n, 1, 1, i] = turn(field[2 * i], LANES - 32) + turn(field[2 * i + 1], 32)
                return carry

            loop(4, pack_x, 0, 2)

            low_rows = rows_of((3, 8, LANES)) < HALF
            for i in range(2):
                one, two = (s["m1"].at[n, 1, 1, i + 2 * k] for k in range(2))
                s["z1out"][n, 0, i, pl.ds(0, 3)] = jnp.where(
                    low_rows, one[pl.ds(0, 3)], swap_halves(two[pl.ds(0, 3)])
                )
                s["z1out"][n, 1, i, pl.ds(0, 3)] = jnp.where(
                    low_rows, swap_halves(one[pl.ds(1, 3)]), two[pl.ds(1, 3)]
                )

            def pack_y(x, carry):
                low, high = carry
                for z in range(4):
                    at = 16 * x + 4 * z
                    slot = (lane >> 2) == 4 * x + z
                    value = field[x, z]
                    low = jnp.where(slot, turn(value, (at + LANES - 32) & (LANES - 1)), low)
                    high = jnp.where(slot, turn(value, (at + LANES - 92) & (LANES - 1)), high)
                return low, high

            zero = jnp.zeros((8, LANES), F32)
            low, high = loop(8, pack_y, (zero, zero), 2)
            s["y1out"][n, 0] = high
            s["y1out"][n, 1] = low
        else:
            both = pl.ds(0, 2)
            total = turn(field[0, both], LANES - 48)
            for x in range(1, 4):
                total = total + turn(field[x, both], (32 * x + LANES - 48) % LANES)
            s["m2"][n, 1, 1, 1, both] = total
        for steps in around_me:
            i, j, k = steps
            if level == 2:
                src = s["m2"].at[n, 1, 1, 1, pl.ds(0, 2)]
                dst = s["m2"].at[n, 1 - i, 1 - j, 1 - k, pl.ds(0, 2)]
            elif k:
                side = 0 if k > 0 else 1
                src = s["y1out"].at[n, side]
                dst = s["y1"].at[n, 1 - i, 1 - j, side]
            else:
                if j == 0:
                    part = pl.ds(0 if i < 0 else 2, 2)
                    src = s["m1"].at[n, 1, 1, part]
                    dst = s["m1"].at[n, 1 - i, 1 - j, part]
                else:
                    side = 0 if j < 0 else 1
                    if i == 0:
                        part = (slice(None), pl.ds(0, 3))
                    else:
                        part = (pl.ds(0 if i < 0 else 1, 1), pl.ds(0 if j < 0 else 1, 2))
                    src = s["z1out"].at[(n, side, *part)]
                    dst = s["z1"].at[(n, 1 - i, 1 - side, *part)]
            c = pltpu.make_async_remote_copy(
                src_ref=src,
                dst_ref=dst,
                send_sem=s["xsend"].at[level - 1, n],
                recv_sem=s["xrecv"].at[level - 1, n],
                device_id=device(steps),
                device_id_type=MESH,
            )
            pl.when(exists(steps))(c.start)

    def finish_exchange(level, n, out):
        def count_of(x, z, y):
            if level == 2:
                return 2 * ((x + 1) * (z + 1) * (y + 1) - 1)
            return 8 * x + 6 * z + 2 * x * z + (x + 1) * (z + 1) * y

        wait_near(count_of, s["xsend"].at[level - 1, n], s["xrecv"].at[level - 1, n])
        low_rows = rows_of((8, LANES)) < HALF
        reach = REACH[level]
        xs, zs = (8, 4) if level == 1 else (4, 2)

        def body(x, carry):
            far = (x + xs - reach) // xs
            at_x = lax.rem(x + xs - reach, xs)

            def source(j, z):
                if level == 1:
                    pair = at_x // 2
                    if j == 1:
                        mid = s["m1"][n, far, 1, pair, z]
                    else:
                        mid = s["z1"][n, far, j // 2, lax.rem(pair, 2), z - 1 if j == 0 else z]
                        there = (pair < 2) if j == 0 else (pair >= 2)
                        mid = jnp.where(there, swap_halves(mid), mid)
                    mid = turn(mid, 32 + 64 * lax.rem(at_x, 2))
                    at = 4 * (4 * at_x + z)
                    left = turn(s["y1"][n, far, j, 0], lax.rem(28 - at + 2 * LANES, LANES))
                    right = turn(s["y1"][n, far, j, 1], lax.rem(96 - at + 2 * LANES, LANES))
                    value = jnp.where((lane >= 28) & (lane < 32), left, 0.0)
                    value = jnp.where((lane >= 96) & (lane < 100), right, value)
                    return jnp.where((lane >= 32) & (lane < 96), mid, value)
                value = jnp.zeros((8, LANES), F32)
                for k in range(3):
                    start = 16 + 32 * k
                    part = turn(
                        s["m2"][n, far, j, k, z], lax.rem(start + 2 * LANES - 32 * at_x, LANES)
                    )
                    value = jnp.where((lane >= start) & (lane < start + 32), part, value)
                return value

            mine = [source(1, z) for z in range(zs)]
            if level == 1:
                down = [None] + [source(0, z) for z in (1, 2, 3)]
                over = [source(2, z) for z in (0, 1, 2)]
                below = [(down[z], mine[z]) for z in (1, 2, 3)]
                above = [(over[z], mine[z]) for z in (0, 1, 2)]
                outer_low, outer_high = [], []
            else:
                outer_low = [source(0, z) for z in range(2)]
                outer_high = [source(2, z) for z in range(2)]
                below = list(zip(outer_low, mine))
                above = list(zip(outer_high, mine))
            values = list(outer_low)
            values += [swap_halves(jnp.where(low_rows, own, other)) for other, own in below]
            values += mine
            values += [swap_halves(jnp.where(low_rows, other, own)) for other, own in above]
            values += outer_high
            out[x, pl.ds(0, len(values))] = jnp.stack(values)
            return carry

        loop(xs + 2 * reach, body, 0, 2)

    def held_row(src, x, z0, z1):
        inner = pl.ds(z0, z1 - z0)
        here = src[x, inner]
        total = (src[x - 1, inner] + src[x + 1, inner]) + (
            src[x, pl.ds(z0 - 1, z1 - z0)] + src[x, pl.ds(z0 + 1, z1 - z0)]
        )
        return here, total + (turn(here, 1) + turn(here, LANES - 1))

    def held_sweep(level, src, dst, margin, into=0):
        xs, zs = HELD[level]
        coupling = 0.25**level
        z0, z1 = margin, zs - margin

        def body(i, carry):
            x = i + margin
            here, around = held_row(src, x, z0, z1)
            inner = pl.ds(z0, z1 - z0)
            value = 0.2 * here + s[f"w{level}"][x, inner] * (
                s[f"b{level}"][x, inner] + coupling * around
            )
            if into:
                dst[i] = value
            else:
                dst[x, inner] = value
            return carry

        loop(xs - 2 * margin, body, 0, 2)

    def held_down(level):
        xs, zs = HELD[level]
        reach = REACH[level]
        coupling = 0.25**level

        def begin(x, carry):
            s[f"v{level}a"][x] = s[f"w{level}"][x] * s[f"b{level}"][x]
            return carry

        loop(xs, begin)
        held_sweep(level, s[f"v{level}a"], s[f"v{level}b"], reach - 1)
        z0, z1 = reach, zs - reach
        inner = pl.ds(z0, z1 - z0)

        def remainder(x):
            here, around = held_row(s[f"v{level}b"], x + reach, z0, z1)
            return s[f"b{level}"][x + reach, inner] - (
                s[f"d{level}"][x, pl.ds(0, CORE[level][1])] * here - coupling * around
            )

        def body(x, carry):
            pair = pair_sum(jnp.stack([remainder(2 * x), remainder(2 * x + 1)]))[0]
            s[f"f{level + 1}"][x, pl.ds(0, CORE[level][1] // 2)] = pair
            return carry

        loop((xs - 2 * reach) // 2, body, 0, 2)

    def held_rest(level):
        held_sweep(level, s[f"v{level}a"], s[f"v{level}b"], 1)

    def held_up(level, coarse, spread, out, last_margin):
        xs, zs = HELD[level]

        def add(i, carry):
            x = i + 1
            picked = jnp.stack([coarse[spread(x), spread(z)] for z in range(1, zs - 1)])
            s[f"v{level}a"][x, pl.ds(1, zs - 2)] = s[f"v{level}b"][x, pl.ds(1, zs - 2)] + picked
            return carry

        loop(xs - 2, add)
        held_sweep(level, s[f"v{level}a"], s[f"v{level}b"], 2)
        held_sweep(level, s[f"v{level}b"], out, 3, into=1)

    def own_of(level, ref):
        reach = REACH[level]
        xs, zs = HELD[level]
        return ref[pl.ds(reach, xs - 2 * reach), pl.ds(reach, zs - 2 * reach)]

    def coefficients(level, kappa):
        coupling = 6.0 * 0.25**level
        s[f"d{level}"][:, pl.ds(0, CORE[level][1])] = own_of(level, kappa) + coupling

        def body(x, carry):
            k = kappa[x]
            s[f"w{level}"][x] = jnp.where(k > 0.0, 0.8 / (k + coupling), 0.0)
            return carry

        loop(kappa.shape[0], body)

    def plane_start(ref, sems):
        at = ref.at[me["gx"], me["gz"]]
        for i, j in plane_offsets:
            pltpu.make_async_remote_copy(
                src_ref=at,
                dst_ref=at,
                send_sem=s["gsend"].at[sems],
                recv_sem=s["grecv"].at[sems],
                device_id=plane_peer(i, j),
                device_id_type=MESH,
            ).start()

    def plane_finish(sems):
        wait_for(nx * nz - 1, s["gsend"].at[sems], s["grecv"].at[sems])

    def gather_start(n):
        s["g3"][n, me["gx"], me["gz"]] = moved(s["f3"][0, 0], "c230") + moved(s["f3"][1, 0], "c231")
        plane_start(s["g3"].at[n], n)

    def gather_finish(n):
        plane_finish(n)

    def coarsest(n):
        coupling = 0.25**LEVELS
        inner = pl.ds(1, nz)
        s["gv"][0, pl.ds(1, nx), inner] = s["gw"][...] * s["g3"][n]
        glane, grow = lanes_of((nz, 8, LANES)), rows_of((nz, 8, LANES))

        def coarse_sweep(src, dst):
            def body(x, carry):
                here = src[x + 1, inner]
                along_x = turn(
                    here + jnp.where(glane >= 64, src[x, inner], src[x + 2, inner]), 64
                )
                along_z = swap_halves(
                    here
                    + jnp.where(grow >= HALF, src[x + 1, pl.ds(0, nz)], src[x + 1, pl.ds(2, nz)])
                )
                around = (along_x + along_z) + (turn(here, 1) + turn(here, LANES - 1))
                dst[x + 1, inner] = 0.2 * here + s["gw"][x] * (s["g3"][n, x] + coupling * around)
                return carry

            loop(nx, body, 0, nx)

        for i in range(COARSE_SWEEPS - 1):
            coarse_sweep(s["gv"].at[i % 2], s["gv"].at[1 - i % 2])
        done = s["gv"].at[(COARSE_SWEEPS - 1) % 2]
        low_rows = rows_of((8, LANES)) < HALF
        near_me = []
        for i in range(3):
            below, mine, above = (done[i + me["gx"], j + me["gz"]] for j in range(3))
            near_me += [
                below,
                swap_halves(jnp.where(low_rows, mine, below)),
                mine,
                swap_halves(jnp.where(low_rows, above, mine)),
                above,
            ]
        near_me = jnp.stack(near_me)
        for i in range(2):
            spread = moved(near_me, f"p32{i}")
            for x in range(3):
                s["e3"][2 * x + i, pl.ds(0, 5)] = spread[5 * x : 5 * x + 5]

    def sum_start(dots, n):
        packed = jnp.zeros((8, LANES), F32)
        for j, d in enumerate(dots):
            packed = jnp.where(lane == j, jnp.sum(d, axis=-1, keepdims=True), packed)
        s["a1"][n, me["gx"], me["gz"]] = packed + swap_halves(packed)
        plane_start(s["a1"].at[n], 3 + n)

    def folded(value):
        while value.shape[0] > 1:
            value = value[: value.shape[0] // 2] + value[value.shape[0] // 2 :]
        return value[0]

    def sum_middle(n):
        plane_finish(3 + n)
        s["a2"][n, me["gy"]] = folded(s["a1"][n].reshape(nx * nz, 8, LANES))
        at = s["a2"].at[n, me["gy"]]
        for o in range(1, counts["gy"]):
            pltpu.make_async_remote_copy(
                src_ref=at,
                dst_ref=at,
                send_sem=s["gsend"].at[5 + n],
                recv_sem=s["grecv"].at[5 + n],
                device_id={"gy": wrapped("gy", o)},
                device_id_type=MESH,
            ).start()

    def sum_finish(n, count):
        wait_for(counts["gy"] - 1, s["gsend"].at[5 + n], s["grecv"].at[5 + n])
        total = folded(s["a2"][n])
        return [total[:, j : j + 1] for j in range(count)]

    pl.semaphore_wait(barrier, greeted)

    def coefficients_held():
        finish_exchange(1, 0, s["v1a"])
        coefficients(1, s["v1a"])
        finish_exchange(2, 0, s["v2a"])
        coefficients(2, s["v2a"])
        s["f3"][:, pl.ds(0, 1)] = pair_sum(own_of(2, s["v2a"]))
        gather_start(0)

    def coarse_coefficients():
        gather_finish(0)
        kappa_3 = s["g3"][0]
        s["gw"][...] = jnp.where(kappa_3 > 0.0, 0.8 / (kappa_3 + 6.0 * 0.25**LEVELS), 0.0)

    def below(n):
        def remainder(x):
            here, around = neighbours(1, x)
            return s["b0"][x] - (s["d0"][x] * here - around)

        def body(x, carry):
            s["t1"][x] = pair_sum(jnp.stack([remainder(2 * x), remainder(2 * x + 1)]))[0]
            return carry

        loop(8, body, 0, 2)
        moved_rows(s["t1"], s["f1"], "c01", 4)
        start_exchange(1, n, s["f1"])
        pl.when(n == 1)(coefficients_held)
        pl.when(n == 2)(lambda: sum_middle(0))
        finish_exchange(1, n, s["b1"])
        held_down(1)
        s["t3"][:, pl.ds(0, 2)] = moved(s["f2"][:, pl.ds(0, 2)], "c12")
        start_exchange(2, n, s["t3"])
        held_rest(1)
        finish_exchange(2, n, s["b2"])
        held_down(2)
        gather_start(n)
        held_rest(2)
        pl.when(n == 1)(coarse_coefficients)
        gather_finish(n)
        coarsest(n)
        held_up(2, s["e3"], lambda i: i // 2, s["e2"], 3)
        moved_rows(s["e2"], s["t2"], "p21", 3)
        held_up(1, s["t2"], lambda i: (i - 1) // 2, s["e1"], 3)
        moved_rows(s["e1"], s["t1"], "p10", 4)

    def begun(x, z0, z1):
        inner = pl.ds(z0, z1 - z0)
        return s["w0"][x, inner] * s["b0"][x, inner]

    def corrected(x, z0, z1):
        e = s["t1"].at[x // 2]
        e = jnp.stack([e[z // 2] for z in range(z0, z1)])
        return s["v0"][1, x + 1, pl.ds(1 + z0, z1 - z0)] + e

    def coarse_kappa():
        moved_rows(s["t1"], s["f1"], "c01", 4)

        def pair_up(x, carry):
            s["f2"][x, pl.ds(0, 2)] = pair_sum(s["f1"][pl.ds(2 * x, 2)])[0]
            return carry

        loop(4, pair_up)
        start_exchange(1, 0, s["f1"])
        s["t3"][:, pl.ds(0, 2)] = moved(s["f2"][:, pl.ds(0, 2)], "c12")
        start_exchange(2, 0, s["t3"])

    def first_sums():
        def body(x, c):
            z = s["z"][0, x]
            b = s["flip"][x].reshape(8, 8, LANES)
            return c[0] + folded(b * z), c[1] + folded(z * s["q"][0, x])

        sum_start(loop(16, body, (jnp.zeros((8, LANES), F32),) * 2), 0)

    def cycle(n, carry):
        def meanwhile():
            pl.when(n == 1)(coarse_kappa)
            pl.when(n == 2)(first_sums)

        exchange(0, begun, meanwhile)
        exchange(1, swept(0))
        below(n)
        exchange(0, corrected)
        exchange(1, swept(0))
        exchange(2, swept(1))

        def apply(x, c):
            here, around = neighbours(2, x)
            q = s["d0"][x] * here - around
            s["z"][n - 1, x] = here
            s["q"][n - 1, x] = q
            return c

        loop(16, apply)

        @pl.when(n == 1)
        def _():
            def shift(x, c):
                s["flip"][x] = s["b0"][x].reshape(64, LANES)
                s["b0"][x] = s["q"][0, x]
                return c

            loop(16, shift)

        return carry

    lax.fori_loop(1, 3, cycle, 0)
    rz, zq = sum_finish(0, 2)
    step = jnp.broadcast_to(rz / zq, (8, LANES))
    zero = jnp.zeros((8, LANES), F32)

    def dots_second(x, c):
        q0 = s["q"][0, x]
        z0 = s["z"][0, x]
        r1 = s["flip"][x].reshape(8, 8, LANES) - step * q0
        z1 = z0 - step * s["z"][1, x]
        q1 = q0 - step * s["q"][1, x]
        s["z"][1, x] = z1
        pairs = (
            (r1, z1),
            (z1, q1),
            (z1, q0),
            (z0, q1),
            (r1, r1),
            (r1, q1),
            (r1, q0),
            (q1, q1),
            (q1, q0),
            (q0, q0),
        )
        return tuple(t + folded(u * v) for t, (u, v) in zip(c, pairs))

    sum_start(loop(16, dots_second, (zero,) * 10), 1)
    sum_middle(1)
    r1z1, z1q1, z1q0, z0q1, r1r1, r1q1, r1q0, q1q1, q1q0, q0q0 = sum_finish(1, 10)
    ratio = r1z1 / rz
    step2 = r1z1 / (z1q1 + ratio * (z1q0 + z0q1) + ratio * ratio * zq)
    squares = (
        r1r1
        - 2.0 * step2 * (r1q1 + ratio * r1q0)
        + step2 * step2 * (q1q1 + 2.0 * ratio * q1q0 + ratio * ratio * q0q0)
    )
    norm = jnp.sqrt(jnp.maximum(squares, 0.0) * (1.0 / cells))
    norm_ref[...] = jnp.broadcast_to(norm, (8, LANES))
    along_z0 = jnp.broadcast_to(step + step2 * ratio, (8, LANES))
    along_z1 = jnp.broadcast_to(step2, (8, LANES))

    def finish(x, c):
        value = along_z0 * s["z"][0, x] + along_z1 * s["z"][1, x]
        s["flip"][x] = value.reshape(64, LANES)
        return c

    loop(16, finish)

    def write(x, c):
        for p in range(PROBES):
            for h in range(2):
                row = h * PROBES + p
                solution_ref[p, x, pl.ds(8 * h, 8), :] = s["flip"][x, pl.ds(row, 8, stride=8), :]
        return c

    loop(16, write)


MATRICES = ("c01", "c12", "p10", "p21", "c230", "c231", "p320", "p321")


def scratch_list():
    def fields(*lead):
        return pltpu.VMEM((*lead[:-1], (lead[-1] + 3) // 4 * 4, 8, LANES), F32)

    out = {"flip": pltpu.VMEM((16, 64, LANES), F32), "lanes": pltpu.VMEM((8, LANES, LANES), jnp.bfloat16)}
    for name in ("b0", "d0", "w0"):
        out[name] = fields(16, 8)
    out["v0"] = fields(3, 18, 10)
    out["r0"] = fields(3, 2, 8)
    out["p0"] = fields(3, 2, 8)
    out["r0y"] = fields(3, 2)
    out["p0y"] = fields(3, 2)
    out["ends"] = fields(16, 1)
    out["f1"] = fields(8, 4)
    out["f2"] = fields(4, 2)
    out["f3"] = fields(2, 1)
    out["t3"] = fields(4, 2)
    for level in (1, 2):
        for name in (f"b{level}", f"w{level}", f"v{level}a", f"v{level}b"):
            out[name] = fields(*HELD[level])
        out[f"d{level}"] = fields(*CORE[level])
    out["e1"] = fields(8, 4)
    out["t1"] = fields(8, 4)
    out["e2"] = fields(6, 4)
    out["t2"] = fields(6, 4)
    out["e3"] = fields(6, 5)
    out["m1"] = fields(3, 3, 3, 4, 4)
    out["z1"] = fields(3, 3, 2, 2, 3)
    out["z1out"] = fields(3, 2, 2, 3)
    out["y1"] = fields(3, 3, 3, 2)
    out["y1out"] = fields(3, 2)
    out["m2"] = fields(3, 3, 3, 3, 2)
    out["z"] = fields(2, 16, 8)
    out["q"] = fields(2, 16, 8)
    out["g3"] = fields(3, 8, 4)
    out["a1"] = fields(2, 8, 4)
    out["a2"] = fields(2, 4)
    out["gw"] = fields(8, 4)
    out["gv"] = fields(2, 10, 6)
    out["count"] = fields(72)
    out["send"] = pltpu.SemaphoreType.DMA((3,))
    out["recv"] = pltpu.SemaphoreType.DMA((3,))
    out["xsend"] = pltpu.SemaphoreType.DMA((2, 3))
    out["xrecv"] = pltpu.SemaphoreType.DMA((2, 3))
    out["gsend"] = pltpu.SemaphoreType.DMA((7,))
    out["grecv"] = pltpu.SemaphoreType.DMA((7,))
    return out


def solution(mesh):
    counts = {a: mesh.shape[a] for a in ("gx", "gy", "gz")}

    def step(kappa_sq, probe_bits):
        cells = probe_bits[0].size * counts["gx"] * counts["gy"] * counts["gz"]
        whole, norms = pl.pallas_call(
            functools.partial(kernel_body, counts, cells),
            out_shape=(
                jax.ShapeDtypeStruct(probe_bits.shape, F32),
                jax.ShapeDtypeStruct((8, LANES), F32),
            ),
            in_specs=[pl.BlockSpec(memory_space=pltpu.VMEM)] * 2,
            out_specs=(pl.BlockSpec(memory_space=pltpu.VMEM),) * 2,
            scratch_shapes=list(scratch_list().values()),
            compiler_params=pltpu.CompilerParams(
                collective_id=0, has_side_effects=True, vmem_limit_bytes=40 * 2**20
            ),
            name="solve",
        )(kappa_sq, probe_bits)
        return whole, norms[:PROBES, 0]

    return jax.shard_map(
        step,
        mesh=mesh,
        in_specs=(P("gx", "gz", "gy"), P(None, "gx", "gz", "gy")),
        out_specs=(P(None, "gx", "gz", "gy"), P()),
        check_vma=False,
    )
```

```python
import functools

import jax
import jax.numpy as jnp
from jax import lax
from jax.experimental import pallas as pl
from jax.experimental.pallas import tpu as pltpu
from jax.sharding import PartitionSpec as P

LEVELS = 3
COARSE_SWEEPS = 8
PROBES = 4
LANES = 128
HALF = 4
MESH = pl.DeviceIdType.MESH
F32 = jnp.float32

OWN = {1: 32, 2: 48, 3: 24}
REACH = {1: 3, 2: 4}
HELD = {1: (14, 10), 2: (12, 10)}
CORE = {1: (8, 4), 2: (4, 2)}


def lanes_of(shape):
    return lax.broadcasted_iota(jnp.int32, shape, len(shape) - 1)


def rows_of(shape):
    return lax.broadcasted_iota(jnp.int32, shape, len(shape) - 2)


def turn(value, shift):
    return pltpu.roll(value, shift, len(value.shape) - 1)


def swap_halves(value):
    return pltpu.roll(value, HALF, len(value.shape) - 2)


def kernel_body(counts, cells, kappa_ref, bits_ref, solution_ref, norm_ref, *scratch):
    s = dict(zip(scratch_list(), scratch))
    axes = ("gx", "gz", "gy")
    me = {a: lax.axis_index(a) for a in axes}
    nx, nz = counts["gx"], counts["gz"]
    lane = lanes_of((8, LANES))

    def loop(count, body, init=0, unroll=1):
        return lax.fori_loop(0, count, body, init, unroll=count)

    def exists(steps):
        ok = None
        for a, d in zip(axes, steps):
            if d:
                one = me[a] > 0 if d < 0 else me[a] < counts[a] - 1
                ok = one if ok is None else ok & one
        return ok

    def device(steps):
        return {a: me[a] + d for a, d in zip(axes, steps)}

    around_me = sorted(
        (
            (i, j, k)
            for i in (-1, 0, 1)
            for j in (-1, 0, 1)
            for k in (-1, 0, 1)
            if (i, j, k) != (0, 0, 0)
        ),
        key=lambda steps: -sum(d * d for d in steps),
    )

    def clear_faces(i, carry):
        for x in (0, 17):
            s["v0"][i, x] = jnp.zeros(s["v0"].shape[2:], F32)
        for name in ("r0", "r0y"):
            s[name][i] = jnp.zeros(s[name].shape[1:], F32)
        return carry

    loop(3, clear_faces)
    for name in ("m1", "z1", "y1", "m2"):
        ref = s[name]

        def clear(i, carry, ref=ref):
            for j in range(ref.shape[2]):
                ref[i // 3, lax.rem(i, 3), j] = jnp.zeros(ref.shape[3:], F32)
            return carry

        loop(9, clear)

    def clear_coarse(i, carry):
        s["gv"][i // 10, lax.rem(i, 10)] = jnp.zeros(s["gv"].shape[2:], F32)
        return carry

    loop(20, clear_coarse)

    barrier = pltpu.get_barrier_semaphore()

    def greet(to):
        pl.semaphore_signal(barrier, inc=1, device_id=to, device_id_type=MESH)

    def wrapped(a, step):
        to = me[a] + step
        return jnp.where(to >= counts[a], to - counts[a], to)

    def plane_peer(i, j):
        return {"gx": wrapped("gx", i), "gz": wrapped("gz", j)}

    plane_offsets = sorted(
        ((i, j) for i in range(nx) for j in range(nz) if (i, j) != (0, 0)),
        key=lambda at: -min(at[0], nx - at[0]) - 2 * min(at[1], nz - at[1]),
    )
    for i, j in plane_offsets:
        greet(plane_peer(i, j))
    for o in range(1, counts["gy"]):
        greet({"gy": lax.rem(me["gy"] + o, counts["gy"])})
    for steps in around_me:
        if steps[2] and steps[:2] != (0, 0):
            pl.when(exists(steps))(functools.partial(greet, device(steps)))
    near = {
        a: (me[a] > 0).astype(jnp.int32) + (me[a] < counts[a] - 1).astype(jnp.int32) for a in axes
    }
    greeted = (
        nx * nz - 1 + counts["gy"] - 1 + ((near["gx"] + 1) * (near["gz"] + 1) - 1) * near["gy"]
    )

    row_at = rows_of((LANES, LANES))
    col_at = lanes_of((LANES, LANES))

    def halved(value):
        return (value + 256) // 2 - 128

    def keep(name, where, weight):
        s["lanes"][MATRICES.index(name)] = jnp.where(where, weight, 0.0).astype(jnp.bfloat16)

    keep("c01", col_at == 32 + row_at // 2, 0.125)
    keep("c12", (col_at == 48 + halved(row_at - 32)) & (row_at >= 32) & (row_at < 96), 0.125)
    inside = (row_at >= 18) & (row_at < 110)
    keep("p10", row_at == 32 + col_at // 2, 1.0)
    keep("p21", row_at == 48 + halved(col_at - 32), 1.0)
    for i in range(2):
        keep(f"c23{i}", (col_at == 64 * i + 24 + halved(row_at - 48)) & inside, 0.125)
        keep(f"p32{i}", row_at == 64 * i + 24 + halved(col_at - 48), 1.0)

    def moved(value, name):
        shape = value.shape
        rest = value.reshape(-1, LANES)
        matrix = s["lanes"][MATRICES.index(name)]
        total = None
        for _ in range(3):
            part = rest.astype(jnp.bfloat16)
            rest = rest - part.astype(F32)
            product = jnp.dot(part, matrix, preferred_element_type=F32)
            total = product if total is None else total + product
        return total.reshape(shape)

    def moved_rows(source, target, name, rows):
        def body(i, carry):
            at = pl.ds(i * rows, rows)
            target[at] = moved(source[at], name)
            return carry

        loop(source.shape[0] // rows, body)

    def load_x(x, carry):
        for p in range(PROBES):
            for h in range(2):
                row = h * PROBES + p
                s["flip"][x, pl.ds(row, 8, stride=8), :] = (
                    2.0 * bits_ref[p, x, pl.ds(8 * h, 8), :].astype(F32) - 1.0
                )
        return carry

    def take_x(x, carry):
        s["b0"][x] = s["flip"][x].reshape(8, 8, LANES)
        return carry

    def kappa_x(x, carry):
        for p in range(PROBES):
            for h in range(2):
                row = h * PROBES + p
                s["flip"][x, pl.ds(row, 8, stride=8), :] = kappa_ref[x, pl.ds(8 * h, 8), :]
        return carry

    def pair_sum(field):
        xs, zs = field.shape[0] // 2, field.shape[1] // 2
        split = field.reshape(xs, 2, zs, 2, 8, LANES)
        return (split[:, 0, :, 0] + split[:, 0, :, 1]) + (split[:, 1, :, 0] + split[:, 1, :, 1])

    def diag_x(x, carry):
        kappas = [s["flip"][2 * x + i].reshape(8, 8, LANES) for i in range(2)]
        for i in range(2):
            s["d0"][2 * x + i] = kappas[i] + 6.0
            s["w0"][2 * x + i] = 0.8 / (kappas[i] + 6.0)
        s["t1"][x] = pair_sum(jnp.stack(kappas))[0]
        return carry

    loop(16, load_x)
    loop(16, take_x)
    loop(16, kappa_x)
    loop(8, diag_x)

    def wait_for(count, send, recv):
        ref = s["count"].at[pl.ds(0, count)]
        c = pltpu.make_async_remote_copy(
            src_ref=ref,
            dst_ref=ref,
            send_sem=send,
            recv_sem=recv,
            device_id={"gx": lax.rem(me["gx"] + 1, nx)},
            device_id_type=MESH,
        )
        c.wait_recv()
        c.wait_send()

    def wait_near(count_of, send, recv):
        for x in (1, 2):
            for z in (1, 2):
                for y in (1, 2):
                    here = (near["gx"] == x) & (near["gz"] == z) & (near["gy"] == y)
                    pl.when(here)(functools.partial(wait_for, count_of(x, z, y), send, recv))

    def exchange(which, cell, meanwhile=None):
        v = s["v0"].at[which]
        got = s["r0"].at[which]
        pack = s["p0"].at[which]
        yin = s["r0y"].at[which]
        yout = s["p0y"].at[which]
        low_rows = rows_of((8, LANES)) < HALF
        inner = pl.ds(1, 8)

        def send(steps, src, dst):
            c = pltpu.make_async_remote_copy(
                src_ref=src,
                dst_ref=dst,
                send_sem=s["send"].at[which],
                recv_sem=s["recv"].at[which],
                device_id=device(steps),
                device_id_type=MESH,
            )
            pl.when(exists(steps))(c.start)

        def fill_z(x, carry):
            v[x + 1, pl.ds(1, 1)] = cell(x, 0, 1)
            v[x + 1, pl.ds(8, 1)] = cell(x, 7, 8)
            return carry

        loop(16, fill_z)

        def pack_z(x, carry):
            pack[0, x] = jnp.where(low_rows, v[x + 1, 1], swap_halves(v[x + 9, 1]))
            pack[1, x] = jnp.where(low_rows, swap_halves(v[x + 1, 8]), v[x + 9, 8])
            return carry

        loop(8, pack_z)
        send((0, -1, 0), pack.at[0], got.at[1])
        send((0, 1, 0), pack.at[1], got.at[0])
        for x in (0, 15):
            v[x + 1, pl.ds(2, 6)] = cell(x, 1, 7)
        send((-1, 0, 0), v.at[1, inner], v.at[17, inner])
        send((1, 0, 0), v.at[16, inner], v.at[0, inner])

        group = ((lane + 1) & (LANES - 1)) // 16

        def fill(x, carry):
            v[x + 2, pl.ds(2, 6)] = cell(x + 1, 1, 7)
            return carry

        loop(14, fill)

        def pack_y(x, carry):
            low, high = carry
            ends = v[x + 1, 1]
            for z in range(1, 8):
                ends = jnp.where(group == z, turn(v[x + 1, 1 + z], 16 * z), ends)
            ends = turn(ends, x)
            low = jnp.where((lane & 15) == x, ends, low)
            high = jnp.where((lane & 15) == ((x + 15) & 15), ends, high)
            return low, high

        zero = jnp.zeros((8, LANES), F32)
        yout[0], yout[1] = loop(16, pack_y, (zero, zero))
        send((0, 0, -1), yout.at[0], yin.at[1])
        send((0, 0, 1), yout.at[1], yin.at[0])
        if meanwhile is not None:
            meanwhile()
        wait_near(lambda x, z, y: 8 * (x + z) + y, s["send"].at[which], s["recv"].at[which])

        def unpack_z(x, carry):
            low, high = got[0, x], got[1, x]
            v[x + 1, 0] = jnp.where(low_rows, low, swap_halves(v[x + 1, 8]))
            v[x + 9, 0] = swap_halves(jnp.where(low_rows, v[x + 9, 8], low))
            v[x + 1, 9] = swap_halves(jnp.where(low_rows, high, v[x + 1, 1]))
            v[x + 9, 9] = jnp.where(low_rows, swap_halves(v[x + 9, 1]), high)
            return carry

        loop(8, unpack_z, 0, 4)

        def unpack_y(x, carry):
            before = turn(yin[0], (LANES + 1 - x) & (LANES - 1))
            after = turn(yin[1], LANES - 1 - x)
            s["ends"][x, 0] = jnp.where((lane & 15) == 0, before, after)
            return carry

        loop(16, unpack_y, 0, 8)

    def neighbours(which, x, z0=0, z1=8):
        v = s["v0"].at[which]
        inner = pl.ds(1 + z0, z1 - z0)
        here = v[x + 1, inner]
        total = v[x, inner] + v[x + 2, inner]
        total = total + (v[x + 1, pl.ds(z0, z1 - z0)] + v[x + 1, pl.ds(z0 + 2, z1 - z0)])
        ends = s["ends"][x, 0]
        ends = jnp.stack([turn(ends, LANES - 16 * z) if z else ends for z in range(z0, z1)])
        at_lane = lanes_of((z1 - z0, 8, LANES))
        before = jnp.where(at_lane == 0, ends, turn(here, 1))
        after = jnp.where(at_lane == LANES - 1, ends, turn(here, LANES - 1))
        return here, total + (before + after)

    def swept(which):
        def cell(x, z0, z1):
            inner = pl.ds(z0, z1 - z0)
            here, around = neighbours(which, x, z0, z1)
            return 0.2 * here + s["w0"][x, inner] * (s["b0"][x, inner] + around)

        return cell

    def start_exchange(level, n, field):
        if level == 1:

            def pack_x(i, carry):
                s["m1"][n, 1, 1, i] = turn(field[2 * i], LANES - 32) + turn(field[2 * i + 1], 32)
                return carry

            loop(4, pack_x, 0, 2)

            low_rows = rows_of((3, 8, LANES)) < HALF
            for i in range(2):
                one, two = (s["m1"].at[n, 1, 1, i + 2 * k] for k in range(2))
                s["z1out"][n, 0, i, pl.ds(0, 3)] = jnp.where(
                    low_rows, one[pl.ds(0, 3)], swap_halves(two[pl.ds(0, 3)])
                )
                s["z1out"][n, 1, i, pl.ds(0, 3)] = jnp.where(
                    low_rows, swap_halves(one[pl.ds(1, 3)]), two[pl.ds(1, 3)]
                )

            def pack_y(x, carry):
                low, high = carry
                for z in range(4):
                    at = 16 * x + 4 * z
                    slot = (lane >> 2) == 4 * x + z
                    value = field[x, z]
                    low = jnp.where(slot, turn(value, (at + LANES - 32) & (LANES - 1)), low)
                    high = jnp.where(slot, turn(value, (at + LANES - 92) & (LANES - 1)), high)
                return low, high

            zero = jnp.zeros((8, LANES), F32)
            low, high = loop(8, pack_y, (zero, zero), 2)
            s["y1out"][n, 0] = high
            s["y1out"][n, 1] = low
        else:
            both = pl.ds(0, 2)
            total = turn(field[0, both], LANES - 48)
            for x in range(1, 4):
                total = total + turn(field[x, both], (32 * x + LANES - 48) % LANES)
            s["m2"][n, 1, 1, 1, both] = total
        for steps in around_me:
            i, j, k = steps
            if level == 2:
                src = s["m2"].at[n, 1, 1, 1, pl.ds(0, 2)]
                dst = s["m2"].at[n, 1 - i, 1 - j, 1 - k, pl.ds(0, 2)]
            elif k:
                side = 0 if k > 0 else 1
                src = s["y1out"].at[n, side]
                dst = s["y1"].at[n, 1 - i, 1 - j, side]
            else:
                if j == 0:
                    part = pl.ds(0 if i < 0 else 2, 2)
                    src = s["m1"].at[n, 1, 1, part]
                    dst = s["m1"].at[n, 1 - i, 1 - j, part]
                else:
                    side = 0 if j < 0 else 1
                    if i == 0:
                        part = (slice(None), pl.ds(0, 3))
                    else:
                        part = (pl.ds(0 if i < 0 else 1, 1), pl.ds(0 if j < 0 else 1, 2))
                    src = s["z1out"].at[(n, side, *part)]
                    dst = s["z1"].at[(n, 1 - i, 1 - side, *part)]
            c = pltpu.make_async_remote_copy(
                src_ref=src,
                dst_ref=dst,
                send_sem=s["xsend"].at[level - 1, n],
                recv_sem=s["xrecv"].at[level - 1, n],
                device_id=device(steps),
                device_id_type=MESH,
            )
            pl.when(exists(steps))(c.start)

    def finish_exchange(level, n, out):
        def count_of(x, z, y):
            if level == 2:
                return 2 * ((x + 1) * (z + 1) * (y + 1) - 1)
            return 8 * x + 6 * z + 2 * x * z + (x + 1) * (z + 1) * y

        wait_near(count_of, s["xsend"].at[level - 1, n], s["xrecv"].at[level - 1, n])
        low_rows = rows_of((8, LANES)) < HALF
        reach = REACH[level]
        xs, zs = (8, 4) if level == 1 else (4, 2)

        def body(x, carry):
            far = (x + xs - reach) // xs
            at_x = lax.rem(x + xs - reach, xs)

            def source(j, z):
                if level == 1:
                    pair = at_x // 2
                    if j == 1:
                        mid = s["m1"][n, far, 1, pair, z]
                    else:
                        mid = s["z1"][n, far, j // 2, lax.rem(pair, 2), z - 1 if j == 0 else z]
                        there = (pair < 2) if j == 0 else (pair >= 2)
                        mid = jnp.where(there, swap_halves(mid), mid)
                    mid = turn(mid, 32 + 64 * lax.rem(at_x, 2))
                    at = 4 * (4 * at_x + z)
                    left = turn(s["y1"][n, far, j, 0], lax.rem(28 - at + 2 * LANES, LANES))
                    right = turn(s["y1"][n, far, j, 1], lax.rem(96 - at + 2 * LANES, LANES))
                    value = jnp.where((lane >= 28) & (lane < 32), left, 0.0)
                    value = jnp.where((lane >= 96) & (lane < 100), right, value)
                    return jnp.where((lane >= 32) & (lane < 96), mid, value)
                value = jnp.zeros((8, LANES), F32)
                for k in range(3):
                    start = 16 + 32 * k
                    part = turn(
                        s["m2"][n, far, j, k, z], lax.rem(start + 2 * LANES - 32 * at_x, LANES)
                    )
                    value = jnp.where((lane >= start) & (lane < start + 32), part, value)
                return value

            mine = [source(1, z) for z in range(zs)]
            if level == 1:
                down = [None] + [source(0, z) for z in (1, 2, 3)]
                over = [source(2, z) for z in (0, 1, 2)]
                below = [(down[z], mine[z]) for z in (1, 2, 3)]
                above = [(over[z], mine[z]) for z in (0, 1, 2)]
                outer_low, outer_high = [], []
            else:
                outer_low = [source(0, z) for z in range(2)]
                outer_high = [source(2, z) for z in range(2)]
                below = list(zip(outer_low, mine))
                above = list(zip(outer_high, mine))
            values = list(outer_low)
            values += [swap_halves(jnp.where(low_rows, own, other)) for other, own in below]
            values += mine
            values += [swap_halves(jnp.where(low_rows, other, own)) for other, own in above]
            values += outer_high
            out[x, pl.ds(0, len(values))] = jnp.stack(values)
            return carry

        loop(xs + 2 * reach, body, 0, 2)

    def held_row(src, x, z0, z1):
        inner = pl.ds(z0, z1 - z0)
        here = src[x, inner]
        total = (src[x - 1, inner] + src[x + 1, inner]) + (
            src[x, pl.ds(z0 - 1, z1 - z0)] + src[x, pl.ds(z0 + 1, z1 - z0)]
        )
        return here, total + (turn(here, 1) + turn(here, LANES - 1))

    def held_sweep(level, src, dst, margin, into=0):
        xs, zs = HELD[level]
        coupling = 0.25**level
        z0, z1 = margin, zs - margin

        def body(i, carry):
            x = i + margin
            here, around = held_row(src, x, z0, z1)
            inner = pl.ds(z0, z1 - z0)
            value = 0.2 * here + s[f"w{level}"][x, inner] * (
                s[f"b{level}"][x, inner] + coupling * around
            )
            if into:
                dst[i] = value
            else:
                dst[x, inner] = value
            return carry

        loop(xs - 2 * margin, body, 0, 2)

    def held_down(level):
        xs, zs = HELD[level]
        reach = REACH[level]
        coupling = 0.25**level

        def begin(x, carry):
            s[f"v{level}a"][x] = s[f"w{level}"][x] * s[f"b{level}"][x]
            return carry

        loop(xs, begin)
        held_sweep(level, s[f"v{level}a"], s[f"v{level}b"], reach - 1)
        z0, z1 = reach, zs - reach
        inner = pl.ds(z0, z1 - z0)

        def remainder(x):
            here, around = held_row(s[f"v{level}b"], x + reach, z0, z1)
            return s[f"b{level}"][x + reach, inner] - (
                s[f"d{level}"][x, pl.ds(0, CORE[level][1])] * here - coupling * around
            )

        def body(x, carry):
            pair = pair_sum(jnp.stack([remainder(2 * x), remainder(2 * x + 1)]))[0]
            s[f"f{level + 1}"][x, pl.ds(0, CORE[level][1] // 2)] = pair
            return carry

        loop((xs - 2 * reach) // 2, body, 0, 2)

    def held_rest(level):
        held_sweep(level, s[f"v{level}a"], s[f"v{level}b"], 1)

    def held_up(level, coarse, spread, out, last_margin):
        xs, zs = HELD[level]

        def add(i, carry):
            x = i + 1
            picked = jnp.stack([coarse[spread(x), spread(z)] for z in range(1, zs - 1)])
            s[f"v{level}a"][x, pl.ds(1, zs - 2)] = s[f"v{level}b"][x, pl.ds(1, zs - 2)] + picked
            return carry

        loop(xs - 2, add)
        held_sweep(level, s[f"v{level}a"], s[f"v{level}b"], 2)
        held_sweep(level, s[f"v{level}b"], out, 3, into=1)

    def own_of(level, ref):
        reach = REACH[level]
        xs, zs = HELD[level]
        return ref[pl.ds(reach, xs - 2 * reach), pl.ds(reach, zs - 2 * reach)]

    def coefficients(level, kappa):
        coupling = 6.0 * 0.25**level
        s[f"d{level}"][:, pl.ds(0, CORE[level][1])] = own_of(level, kappa) + coupling

        def body(x, carry):
            k = kappa[x]
            s[f"w{level}"][x] = jnp.where(k > 0.0, 0.8 / (k + coupling), 0.0)
            return carry

        loop(kappa.shape[0], body)

    def plane_start(ref, sems):
        at = ref.at[me["gx"], me["gz"]]
        for i, j in plane_offsets:
            pltpu.make_async_remote_copy(
                src_ref=at,
                dst_ref=at,
                send_sem=s["gsend"].at[sems],
                recv_sem=s["grecv"].at[sems],
                device_id=plane_peer(i, j),
                device_id_type=MESH,
            ).start()

    def plane_finish(sems):
        wait_for(nx * nz - 1, s["gsend"].at[sems], s["grecv"].at[sems])

    def gather_start(n):
        s["g3"][n, me["gx"], me["gz"]] = moved(s["f3"][0, 0], "c230") + moved(s["f3"][1, 0], "c231")
        plane_start(s["g3"].at[n], n)

    def gather_finish(n):
        plane_finish(n)

    def coarsest(n):
        coupling = 0.25**LEVELS
        inner = pl.ds(1, nz)
        s["gv"][0, pl.ds(1, nx), inner] = s["gw"][...] * s["g3"][n]
        glane, grow = lanes_of((nz, 8, LANES)), rows_of((nz, 8, LANES))

        def coarse_sweep(src, dst):
            def body(x, carry):
                here = src[x + 1, inner]
                along_x = turn(
                    here + jnp.where(glane >= 64, src[x, inner], src[x + 2, inner]), 64
                )
                along_z = swap_halves(
                    here
                    + jnp.where(grow >= HALF, src[x + 1, pl.ds(0, nz)], src[x + 1, pl.ds(2, nz)])
                )
                around = (along_x + along_z) + (turn(here, 1) + turn(here, LANES - 1))
                dst[x + 1, inner] = 0.2 * here + s["gw"][x] * (s["g3"][n, x] + coupling * around)
                return carry

            loop(nx, body, 0, nx)

        for i in range(COARSE_SWEEPS - 1):
            coarse_sweep(s["gv"].at[i % 2], s["gv"].at[1 - i % 2])
        done = s["gv"].at[(COARSE_SWEEPS - 1) % 2]
        low_rows = rows_of((8, LANES)) < HALF
        near_me = []
        for i in range(3):
            below, mine, above = (done[i + me["gx"], j + me["gz"]] for j in range(3))
            near_me += [
                below,
                swap_halves(jnp.where(low_rows, mine, below)),
                mine,
                swap_halves(jnp.where(low_rows, above, mine)),
                above,
            ]
        near_me = jnp.stack(near_me)
        for i in range(2):
            spread = moved(near_me, f"p32{i}")
            for x in range(3):
                s["e3"][2 * x + i, pl.ds(0, 5)] = spread[5 * x : 5 * x + 5]

    def sum_start(dots, n):
        packed = jnp.zeros((8, LANES), F32)
        for j, d in enumerate(dots):
            packed = jnp.where(lane == j, jnp.sum(d, axis=-1, keepdims=True), packed)
        s["a1"][n, me["gx"], me["gz"]] = packed + swap_halves(packed)
        plane_start(s["a1"].at[n], 3 + n)

    def folded(value):
        while value.shape[0] > 1:
            value = value[: value.shape[0] // 2] + value[value.shape[0] // 2 :]
        return value[0]

    def sum_middle(n):
        plane_finish(3 + n)
        s["a2"][n, me["gy"]] = folded(s["a1"][n].reshape(nx * nz, 8, LANES))
        at = s["a2"].at[n, me["gy"]]
        for o in range(1, counts["gy"]):
            pltpu.make_async_remote_copy(
                src_ref=at,
                dst_ref=at,
                send_sem=s["gsend"].at[5 + n],
                recv_sem=s["grecv"].at[5 + n],
                device_id={"gy": wrapped("gy", o)},
                device_id_type=MESH,
            ).start()

    def sum_finish(n, count):
        wait_for(counts["gy"] - 1, s["gsend"].at[5 + n], s["grecv"].at[5 + n])
        total = folded(s["a2"][n])
        return [total[:, j : j + 1] for j in range(count)]

    pl.semaphore_wait(barrier, greeted)

    def coefficients_held():
        finish_exchange(1, 0, s["v1a"])
        coefficients(1, s["v1a"])
        finish_exchange(2, 0, s["v2a"])
        coefficients(2, s["v2a"])
        s["f3"][:, pl.ds(0, 1)] = pair_sum(own_of(2, s["v2a"]))
        gather_start(0)

    def coarse_coefficients():
        gather_finish(0)
        kappa_3 = s["g3"][0]
        s["gw"][...] = jnp.where(kappa_3 > 0.0, 0.8 / (kappa_3 + 6.0 * 0.25**LEVELS), 0.0)

    def below(n):
        def remainder(x):
            here, around = neighbours(1, x)
            return s["b0"][x] - (s["d0"][x] * here - around)

        def body(x, carry):
            s["t1"][x] = pair_sum(jnp.stack([remainder(2 * x), remainder(2 * x + 1)]))[0]
            return carry

        loop(8, body, 0, 2)
        moved_rows(s["t1"], s["f1"], "c01", 4)
        start_exchange(1, n, s["f1"])
        pl.when(n == 1)(coefficients_held)
        pl.when(n == 2)(lambda: sum_middle(0))
        finish_exchange(1, n, s["b1"])
        held_down(1)
        s["t3"][:, pl.ds(0, 2)] = moved(s["f2"][:, pl.ds(0, 2)], "c12")
        start_exchange(2, n, s["t3"])
        held_rest(1)
        finish_exchange(2, n, s["b2"])
        held_down(2)
        gather_start(n)
        held_rest(2)
        pl.when(n == 1)(coarse_coefficients)
        gather_finish(n)
        coarsest(n)
        held_up(2, s["e3"], lambda i: i // 2, s["e2"], 3)
        moved_rows(s["e2"], s["t2"], "p21", 3)
        held_up(1, s["t2"], lambda i: (i - 1) // 2, s["e1"], 3)
        moved_rows(s["e1"], s["t1"], "p10", 4)

    def begun(x, z0, z1):
        inner = pl.ds(z0, z1 - z0)
        return s["w0"][x, inner] * s["b0"][x, inner]

    def corrected(x, z0, z1):
        e = s["t1"].at[x // 2]
        e = jnp.stack([e[z // 2] for z in range(z0, z1)])
        return s["v0"][1, x + 1, pl.ds(1 + z0, z1 - z0)] + e

    def coarse_kappa():
        moved_rows(s["t1"], s["f1"], "c01", 4)

        def pair_up(x, carry):
            s["f2"][x, pl.ds(0, 2)] = pair_sum(s["f1"][pl.ds(2 * x, 2)])[0]
            return carry

        loop(4, pair_up)
        start_exchange(1, 0, s["f1"])
        s["t3"][:, pl.ds(0, 2)] = moved(s["f2"][:, pl.ds(0, 2)], "c12")
        start_exchange(2, 0, s["t3"])

        def keep_b(x, carry):
            s["flip"][x] = s["b0"][x].reshape(64, LANES)
            return carry

        loop(16, keep_b)

    def first_sums():
        def body(x, c):
            z = s["z"][1, x]
            q = s["q"][1, x]
            s["z"][0, x] = z
            s["q"][0, x] = q
            b = s["flip"][x].reshape(8, 8, LANES)
            return c[0] + folded(b * z), c[1] + folded(z * q)

        sum_start(loop(16, body, (jnp.zeros((8, LANES), F32),) * 2), 0)

    def cycle(n, carry):
        def meanwhile():
            pl.when(n == 1)(coarse_kappa)
            pl.when(n == 2)(first_sums)

        exchange(0, begun, meanwhile)
        exchange(1, swept(0))
        below(n)
        exchange(0, corrected)
        exchange(1, swept(0))
        exchange(2, swept(1))

        def apply(x, c):
            here, around = neighbours(2, x)
            q = s["d0"][x] * here - around
            s["z"][1, x] = here
            s["q"][1, x] = q
            return c

        loop(16, apply)

        @pl.when(n == 1)
        def _():
            def shift(x, c):
                s["b0"][x] = s["q"][1, x]
                return c

            loop(16, shift)

        return carry

    lax.fori_loop(1, 3, cycle, 0)
    rz, zq = sum_finish(0, 2)
    step = jnp.broadcast_to(rz / zq, (8, LANES))
    zero = jnp.zeros((8, LANES), F32)

    def dots_second(x, c):
        q0 = s["q"][0, x]
        z0 = s["z"][0, x]
        r1 = s["flip"][x].reshape(8, 8, LANES) - step * q0
        z1 = z0 - step * s["z"][1, x]
        q1 = q0 - step * s["q"][1, x]
        s["z"][1, x] = z1
        pairs = (
            (r1, z1),
            (z1, q1),
            (z1, q0),
            (z0, q1),
            (r1, r1),
            (r1, q1),
            (r1, q0),
            (q1, q1),
            (q1, q0),
            (q0, q0),
        )
        return tuple(t + folded(u * v) for t, (u, v) in zip(c, pairs))

    sum_start(loop(16, dots_second, (zero,) * 10), 1)
    sum_middle(1)
    r1z1, z1q1, z1q0, z0q1, r1r1, r1q1, r1q0, q1q1, q1q0, q0q0 = sum_finish(1, 10)
    ratio = r1z1 / rz
    step2 = r1z1 / (z1q1 + ratio * (z1q0 + z0q1) + ratio * ratio * zq)
    squares = (
        r1r1
        - 2.0 * step2 * (r1q1 + ratio * r1q0)
        + step2 * step2 * (q1q1 + 2.0 * ratio * q1q0 + ratio * ratio * q0q0)
    )
    norm = jnp.sqrt(jnp.maximum(squares, 0.0) * (1.0 / cells))
    norm_ref[...] = jnp.broadcast_to(norm, (8, LANES))
    along_z0 = jnp.broadcast_to(step + step2 * ratio, (8, LANES))
    along_z1 = jnp.broadcast_to(step2, (8, LANES))

    def finish(x, c):
        value = along_z0 * s["z"][0, x] + along_z1 * s["z"][1, x]
        s["flip"][x] = value.reshape(64, LANES)
        return c

    loop(16, finish)

    def write(x, c):
        for p in range(PROBES):
            for h in range(2):
                row = h * PROBES + p
                solution_ref[p, x, pl.ds(8 * h, 8), :] = s["flip"][x, pl.ds(row, 8, stride=8), :]
        return c

    loop(16, write)


MATRICES = ("c01", "c12", "p10", "p21", "c230", "c231", "p320", "p321")


def scratch_list():
    def fields(*lead):
        return pltpu.VMEM((*lead[:-1], (lead[-1] + 3) // 4 * 4, 8, LANES), F32)

    out = {"flip": pltpu.VMEM((16, 64, LANES), F32), "lanes": pltpu.VMEM((8, LANES, LANES), jnp.bfloat16)}
    for name in ("b0", "d0", "w0"):
        out[name] = fields(16, 8)
    out["v0"] = fields(3, 18, 10)
    out["r0"] = fields(3, 2, 8)
    out["p0"] = fields(3, 2, 8)
    out["r0y"] = fields(3, 2)
    out["p0y"] = fields(3, 2)
    out["ends"] = fields(16, 1)
    out["f1"] = fields(8, 4)
    out["f2"] = fields(4, 2)
    out["f3"] = fields(2, 1)
    out["t3"] = fields(4, 2)
    for level in (1, 2):
        for name in (f"b{level}", f"w{level}", f"v{level}a", f"v{level}b"):
            out[name] = fields(*HELD[level])
        out[f"d{level}"] = fields(*CORE[level])
    out["e1"] = fields(8, 4)
    out["t1"] = fields(8, 4)
    out["e2"] = fields(6, 4)
    out["t2"] = fields(6, 4)
    out["e3"] = fields(6, 5)
    out["m1"] = fields(3, 3, 3, 4, 4)
    out["z1"] = fields(3, 3, 2, 2, 3)
    out["z1out"] = fields(3, 2, 2, 3)
    out["y1"] = fields(3, 3, 3, 2)
    out["y1out"] = fields(3, 2)
    out["m2"] = fields(3, 3, 3, 3, 2)
    out["z"] = fields(2, 16, 8)
    out["q"] = fields(2, 16, 8)
    out["g3"] = fields(3, 8, 4)
    out["a1"] = fields(2, 8, 4)
    out["a2"] = fields(2, 4)
    out["gw"] = fields(8, 4)
    out["gv"] = fields(2, 10, 6)
    out["count"] = fields(72)
    out["send"] = pltpu.SemaphoreType.DMA((3,))
    out["recv"] = pltpu.SemaphoreType.DMA((3,))
    out["xsend"] = pltpu.SemaphoreType.DMA((2, 3))
    out["xrecv"] = pltpu.SemaphoreType.DMA((2, 3))
    out["gsend"] = pltpu.SemaphoreType.DMA((7,))
    out["grecv"] = pltpu.SemaphoreType.DMA((7,))
    return out


def solution(mesh):
    counts = {a: mesh.shape[a] for a in ("gx", "gy", "gz")}

    def step(kappa_sq, probe_bits):
        cells = probe_bits[0].size * counts["gx"] * counts["gy"] * counts["gz"]
        whole, norms = pl.pallas_call(
            functools.partial(kernel_body, counts, cells),
            out_shape=(
                jax.ShapeDtypeStruct(probe_bits.shape, F32),
                jax.ShapeDtypeStruct((8, LANES), F32),
            ),
            in_specs=[pl.BlockSpec(memory_space=pltpu.VMEM)] * 2,
            out_specs=(pl.BlockSpec(memory_space=pltpu.VMEM),) * 2,
            scratch_shapes=list(scratch_list().values()),
            compiler_params=pltpu.CompilerParams(
                collective_id=0, has_side_effects=True, vmem_limit_bytes=40 * 2**20
            ),
            name="solve",
        )(kappa_sq, probe_bits)
        return whole, norms[:PROBES, 0]

    return jax.shard_map(
        step,
        mesh=mesh,
        in_specs=(P("gx", "gz", "gy"), P(None, "gx", "gz", "gy")),
        out_specs=(P(None, "gx", "gz", "gy"), P()),
        check_vma=False,
    )
```
